32 devices in a mesh: rows: 8 (over z, y), cols: 4 (over x, core).
Axes of the slice: x: 2, y: 2, z: 4, core: 2. Of those that a mesh axis runs over, the one named last changes fastest.
Arguments:
- slab: float32 [1536, 6144], P('rows', 'cols'), may hold values from -6 to 6
- factor: float32 [6144, 6144], P('cols', 'rows'), may hold values from -0.078125 to 0.078125
- block_inverse: float32 [6144, 1536], P('cols'), may hold values from -2 to 2, as said below
- pivot_order: int32 [6144], replicated, may hold values from 0 to 6143, as said below
- row_count: int32 [8], P('rows'), may hold values from 1 to 192, 1075 in all
Outputs:
- vectors: float32 [1536, 6144], P('rows', 'cols')
- mean_square: float32 [1536], P('rows')
The draws below stay inside these ranges and needn't reach their ends.
Inputs may be any that keep to these rules, and one draw needn't show every extreme that they name: `pivot_order`: each of 0 to 6143 appears once. Of the 1536 pivots of one block, at most 768 have slab columns in any one block of 1536 slab columns, and exactly 768 in some. `row_count`: slots at or beyond the count hold entries that are ignored. `block_inverse`: each block of 1536 rows is lower triangular, with diagonal entries from 0.6 to 1.4.
All inputs are finite; a program needn't handle non-finite values. No bound on the sum of `row_count` on one device may be relied on, other than what follows from the above.
Results may differ from the reference program's by a relative error of at most 0.0001.
Values sent between devices are 32-bit elements; how exact they have to be, the bound alone decides.
A program may use at most 192 MiB of HBM per device.

```python
import math
import jax
import jax.numpy as jnp
import numpy as np
from jax import lax

K = 6144
ROWS_DEV = 192
BLOCK = 1536
ROWS = 1536
N_ROWS = 8
N_COLS = 4


def draw_block_inverse(key, part):
    first_key, second_key = jax.random.split(key)
    local_rows = jnp.arange(K, dtype=jnp.int32) % BLOCK
    local_cols = jnp.arange(BLOCK, dtype=jnp.int32)
    spread = jnp.clip(jax.random.normal(first_key, (K, BLOCK), jnp.float32), -4.0, 4.0)
    spread = spread / jnp.sqrt(jnp.float32(BLOCK))
    diagonal = jax.random.uniform(second_key, (K, 1), jnp.float32, 0.6, 1.4)
    lower = jnp.where(local_cols[None, :] < local_rows[:, None], spread, jnp.float32(0.0))
    return lower + jnp.where(local_cols[None, :] == local_rows[:, None], diagonal, jnp.float32(0.0))


def draw_pivot_order(key, part):
    keys = jax.random.split(jax.random.fold_in(key, 17), 4)
    group_count = K // BLOCK
    base = BLOCK // group_count
    shift = jax.random.randint(keys[0], (), 0, group_count, dtype=jnp.int32)
    extra = jax.random.randint(keys[1], (), 0, base // 2 + 1, dtype=jnp.int32)
    source = jnp.arange(group_count, dtype=jnp.int32)[:, None]
    target = jnp.arange(group_count, dtype=jnp.int32)[None, :]
    offset = (target - source - shift) % group_count
    counts = base + base * (offset == 0).astype(jnp.int32) - base * (offset == 1).astype(jnp.int32)
    counts = counts + extra * (offset == 2).astype(jnp.int32) - extra * (offset == 3).astype(jnp.int32)
    inclusive = jnp.cumsum(counts, axis=1)
    columns = jnp.arange(K, dtype=jnp.int32)
    column_block = columns // BLOCK
    first_perm = jax.random.permutation(keys[2], K).astype(jnp.int32)
    order = jnp.argsort(column_block * K + first_perm).astype(jnp.int32)
    position = jnp.argsort(order).astype(jnp.int32)
    local_rank = position - column_block * BLOCK
    bounds = jnp.take(inclusive, column_block, axis=0)
    destination = jnp.sum((bounds <= local_rank[:, None]).astype(jnp.int32), axis=1)
    second_perm = jax.random.permutation(keys[3], K).astype(jnp.int32)
    return jnp.argsort(destination * K + second_perm).astype(jnp.int32)


def block_levels(own_key, shape, cuts, least, high):
    def one(axis_at, blocks):
        steps = jax.random.uniform(jax.random.fold_in(jax.random.fold_in(own_key, 6), axis_at), (blocks,), jnp.float32, least / len(cuts), high / len(cuts))
        return jnp.repeat(jnp.exp(steps), shape[axis_at] // blocks).reshape((-1,) + (1,) * (len(shape) - axis_at - 1))

    factor_of = one(*cuts[0])
    for cut in cuts[1:]:
        factor_of = factor_of * one(*cut)
    return factor_of


def length_profile(number_of, total, most, lean):
    loads = [(1 << 20) // math.isqrt(rank ** lean) + 1 for rank in range(2, number_of + 1)]
    surplus, holding = total - most - (number_of - 1), [1] * (number_of - 1)
    while surplus > 0:
        candidates = [i for i in range(number_of - 1) if holding[i] < most]
        mass, remaining = sum([loads[i] for i in candidates]), surplus
        for i in candidates:
            addition = min(most - holding[i], max(1, remaining * loads[i] // mass), surplus)
            holding[i] = holding[i] + addition
            surplus = surplus - addition
    return np.array([most] + holding)


def uneven(stream_key, amount, total, limit, slope):
    if amount == 2:
        one = jax.random.randint(stream_key, (), max(1, total - limit), min(limit, total - 1) + 1)
        return jnp.stack([one, total - one])
    sizes = jnp.asarray(length_profile(amount, total, limit, slope), jnp.int32)
    couples = (amount - 1) // 2
    giver, sink = sizes[1:1 + 2 * couples:2], sizes[2:2 + 2 * couples:2]
    margin = jnp.minimum(giver - 1, limit - sink)
    passed = jax.random.randint(jax.random.fold_in(stream_key, 1), (couples,), 0, 1 << 20) % (margin + 1)
    sizes = sizes.at[1:1 + 2 * couples:2].set(giver - passed).at[2:2 + 2 * couples:2].set(sink + passed)
    return sizes[jax.random.permutation(jax.random.fold_in(stream_key, 2), amount)]


def scatter_about(rng, shape, scale, bound, shards=(), held_as=jnp.bfloat16):
    gain = block_levels(rng, shape, shards, -0.22, 0.18) if shards else 1.0
    drawn = jax.random.normal(rng, shape, jnp.float32) * scale * gain
    return jnp.minimum(jnp.maximum(drawn, -bound), bound).astype(held_as)


def setup_inputs(seed: int = 0) -> dict:
    key_list = jax.random.split(jax.random.key(seed), 6)
    slab = scatter_about(key_list[0], (ROWS, K), 1.0, 6.0, ((0, 8), (1, 4)), jnp.float32)
    factor = scatter_about(key_list[1], (K, K), K ** -0.5, 0.078125, ((0, 4), (1, 8)), jnp.float32)
    block_inverse = draw_block_inverse(jax.random.fold_in(key_list[5], 71), 0)
    pivot_order = draw_pivot_order(jax.random.fold_in(key_list[5], 71), 0)
    row_count = uneven(key_list[4], N_ROWS, (7 * ROWS) // 10, ROWS_DEV, 2).astype(jnp.int32)
    return dict(slab=slab, factor=factor, block_inverse=block_inverse, pivot_order=pivot_order, row_count=row_count)


def reference(slab, factor, block_inverse, pivot_order, row_count):
    ordered = jnp.take(slab, pivot_order, axis=1)
    slot_index = jnp.arange(ROWS, dtype=jnp.int32) % ROWS_DEV
    owner = jnp.arange(ROWS, dtype=jnp.int32) // ROWS_DEV
    live_rows = slot_index < row_count[owner]
    ordered = jnp.where(live_rows[:, None], ordered, jnp.float32(0.0))
    block_width = K // N_COLS
    finished = []
    for column_block in range(N_COLS):
        low = column_block * block_width
        remainder = ordered[:, low:low + block_width]
        for earlier in range(column_block):
            weights = factor[low:low + block_width, earlier * block_width:(earlier + 1) * block_width]
            remainder = remainder - jnp.dot(finished[earlier], weights.T, precision=lax.Precision.HIGHEST, preferred_element_type=jnp.float32)
        inverse = block_inverse[low:low + block_width]
        finished.append(jnp.dot(remainder, inverse.T, precision=lax.Precision.HIGHEST, preferred_element_type=jnp.float32))
    vectors = jnp.concatenate(finished, axis=1)
    mean_square = jnp.sum(vectors * vectors, axis=1) / K
    return vectors, mean_square
```

```python
import functools
import jax
import jax.numpy as jnp
from jax import lax
from jax.experimental import pallas as pl
from jax.experimental.pallas import tpu as pltpu
from jax.sharding import PartitionSpec as P

MESH = pl.DeviceIdType.MESH


def times_transposed(left, right):
    return lax.dot_general(
        left,
        right,
        (((1,), (1,)), ((), ())),
        precision=lax.Precision.HIGH,
        preferred_element_type=jnp.float32,
    )


def gather_kernel(groups, side, chunks, part_ref, row_ref, mine, in_sem, keep_sem, right_sem, left_sem, hop_sem, side_sem, cross_sem):
    row, column = lax.axis_index("rows"), lax.axis_index("cols")
    a, b = row // side, row % side
    depth, width = part_ref.shape
    tall = depth // chunks

    def at(a_to, b_to):
        return (a_to * side + b_to, column)

    barrier = pltpu.get_barrier_semaphore()
    for step in (1, groups - 1):
        pl.semaphore_signal(barrier, inc=1, device_id=at((a + step) % groups, b), device_id_type=MESH)
    for step in range(1, side):
        pl.semaphore_signal(barrier, inc=1, device_id=at(a, (b + step) % side), device_id_type=MESH)
    pl.semaphore_wait(barrier, 2 + side - 1)

    def rows_of(i):
        return pl.ds(pl.multiple_of(i * tall, tall), tall)

    def place(k, b_of, i):
        return row_ref.at[k * side + b_of, rows_of(i), :]

    def right(k, i, source):
        return pltpu.make_async_remote_copy(source, place(k, b, i), right_sem.at[k, i], hop_sem.at[k, i], device_id=at(jnp.minimum(a + 1, groups - 1), b), device_id_type=MESH)

    def left(k, i, source):
        return pltpu.make_async_remote_copy(source, place(k, b, i), left_sem.at[k, i], hop_sem.at[k, i], device_id=at(jnp.maximum(a - 1, 0), b), device_id_type=MESH)

    def across(k, step, i, source):
        return pltpu.make_async_remote_copy(source, place(k, b, i), side_sem.at[step - 1, k, i], cross_sem.at[step - 1, k, i], device_id=at(a, (b + step) % side), device_id_type=MESH)

    def load(i):
        return pltpu.make_async_copy(part_ref.at[rows_of(i), :], mine.at[rows_of(i), :], in_sem.at[i])

    def keep(i):
        return pltpu.make_async_copy(mine.at[rows_of(i), :], place(a, b, i), keep_sem.at[i])

    @pl.when(a < column)
    def _():
        @pl.loop(0, chunks)
        def _(i):
            load(i).start()

        @pl.loop(0, chunks)
        def _(i):
            source = mine.at[rows_of(i), :]
            load(i).wait()

            @pl.when(a < groups - 1)
            def _():
                right(a, i, source).start()

            @pl.when(a > 0)
            def _():
                left(a, i, source).start()

            for step in range(1, side):
                across(a, step, i, source).start()
            keep(i).start()

    for hop in range(1, groups):
        @pl.loop(0, chunks)
        def _(i):
            k = a - hop

            @pl.when((k >= 0) & (k < column))
            def _():
                source = place(k, b, i)
                right(k, i, source).wait_recv()

                @pl.when(a < groups - 1)
                def _():
                    right(k, i, source).start()

                for step in range(1, side):
                    across(k, step, i, source).start()

            h = a + hop

            @pl.when((h <= groups - 1) & (h < column))
            def _():
                source = place(h, b, i)
                left(h, i, source).wait_recv()

                @pl.when(a > 0)
                def _():
                    left(h, i, source).start()

                for step in range(1, side):
                    across(h, step, i, source).start()

    for k in range(groups - 1):
        @pl.when(k < column)
        def _():
            @pl.loop(0, chunks)
            def _(i):
                source = place(k, b, i)
                for step in range(1, side):
                    came = place(k, (b + side - step) % side, i)
                    pltpu.make_async_remote_copy(came, came, side_sem.at[step - 1, k, i], cross_sem.at[step - 1, k, i], device_id=at(a, (b + step) % side), device_id_type=MESH).wait_recv()
                    across(k, step, i, source).wait_send()

                @pl.when((k <= a) & (a < groups - 1))
                def _():
                    right(k, i, source).wait_send()

                @pl.when((k >= a) & (a > 0))
                def _():
                    left(k, i, source).wait_send()

                @pl.when(k == a)
                def _():
                    keep(i).wait()


def gather_factor(factor, rows, groups):
    side = rows // groups
    depth, width = factor.shape
    chunks = max(1, depth // 256)
    sem = pltpu.SemaphoreType.DMA
    return pl.pallas_call(
        functools.partial(gather_kernel, groups, side, chunks),
        out_shape=jax.ShapeDtypeStruct(((groups - 1) * side, depth, width), jnp.float32),
        in_specs=[pl.BlockSpec(memory_space=pl.ANY)],
        out_specs=pl.BlockSpec(memory_space=pl.ANY),
        scratch_shapes=[
            pltpu.VMEM((depth, width), jnp.float32),
            sem((chunks,)),
            sem((chunks,)),
            sem((groups, chunks)),
            sem((groups, chunks)),
            sem((groups, chunks)),
            sem((side - 1, groups, chunks)),
            sem((side - 1, groups, chunks)),
        ],
        compiler_params=pltpu.CompilerParams(collective_id=0, has_side_effects=True, vmem_limit_bytes=60000 * 1024),
        cost_estimate=pl.CostEstimate(flops=0, bytes_accessed=600000000, transcendentals=0),
    )(factor)


def plain_device(slab, factor, block_inverse, pivot_order, row_count):
    rows_here, block_width = slab.shape
    row_devices = lax.axis_size("rows")
    column_count = lax.axis_size("cols")
    column = lax.axis_index("cols")
    total_width = block_width * column_count
    side = row_devices // column_count
    chosen = lax.dynamic_slice_in_dim(pivot_order, column * block_width, block_width)
    gathered = lax.all_gather(slab, "cols", axis=1, tiled=True)
    parts = gather_factor(factor, row_devices, column_count)
    gathered, parts = lax.optimization_barrier((gathered, parts))
    ordered = jnp.take(gathered, chosen, axis=1)
    live_rows = jnp.arange(rows_here, dtype=jnp.int32) < row_count[0]
    pending = jnp.where(live_rows[:, None], ordered, jnp.float32(0.0))

    def finish(values):
        return times_transposed(values, block_inverse)

    def nothing(values):
        return jnp.zeros_like(values)

    width = factor.shape[1]
    vectors = jnp.zeros_like(pending)
    for k in range(column_count):
        finished = lax.cond(column == k, finish, nothing, pending)
        vectors = vectors + finished
        if k + 1 < column_count:
            arrived = moving = finished
            for to in range(k + 1, column_count):
                moving = lax.ppermute(moving, "cols", [(to - 1, to)])
                arrived = jnp.where(column == to, moving, arrived)
            update = jnp.zeros_like(pending)
            for b in range(side):
                update += times_transposed(arrived[:, b * width : (b + 1) * width], parts[k * side + b])
            pending = pending - jnp.where(k < column, update, jnp.float32(0.0))
    row_sums = lax.psum(jnp.sum(vectors * vectors, axis=1), "cols")
    return (vectors, row_sums / total_width)


TALL = 128
WIDE = 256


def target_of(j, k):
    if j % 2 == 0:
        return k
    return j - 1 if k == 0 and j > 1 else j


def halves(values):
    high = values.astype(jnp.bfloat16)
    return high, (values - high.astype(jnp.float32)).astype(jnp.bfloat16)


def nt(left, right):
    return lax.dot_general(left, right, (((1,), (1,)), ((), ())), preferred_element_type=jnp.float32)


def nt3(stacked, right):
    rows = stacked.shape[0] // 2
    high, low = halves(right)
    both = nt(stacked, high)
    return both[:rows] + (both[rows:] + nt(stacked[:rows], low))


def chain_kernel(
    groups,
    side,
    slab_ref,
    factor_ref,
    inverse_ref,
    order_ref,
    live_ref,
    out_ref,
    mean_ref,
    buf,
    inverse,
    slabs,
    rest,
    vec,
    stack,
    vec_in,
    part_in,
    part_out,
    sums,
    ones,
    load_sem,
    recv_sem,
    up_sem,
    down_sem,
    side_sem,
    entry_sem,
    inverse_sem,
    own_sem,
    slab_send,
    slab_recv,
    pass_send,
    vec_send,
    vec_recv,
    part_send,
    part_recv,
    sum_send,
    sum_recv,
    out_sem,
):
    columns = groups
    row, column = lax.axis_index("rows"), lax.axis_index("cols")
    a, b = row // side, row % side
    height, width = rest.shape
    depth, part = factor_ref.shape
    chunks = depth // TALL
    pieces = width // WIDE
    chips = columns // 2
    chip, core = column // 2, column % 2
    all_blocks = [(j, k) for j in range(1, columns) for k in range(j)]
    blocks = [[jk for jk in all_blocks if target_of(*jk) == c] for c in range(columns)]
    before = [[jk for jk in blocks[c] if jk[1] < c] for c in range(columns)]
    after = [[jk for jk in blocks[c] if jk[1] == c] for c in range(columns)]
    vec_from = [sorted({k for _, k in before[c]}) for c in range(columns)]
    vec_to = [[u for u in range(columns) if c in vec_from[u]] for c in range(columns)]
    part_from = [[k for k in range(c) if target_of(c, k) != c] for c in range(columns)]
    part_made = [[jk for jk in blocks[c] if jk[0] != c] for c in range(columns)]

    def there(c):
        return (row, c)

    def remote(source, target, send, recv, device):
        return pltpu.make_async_remote_copy(source, target, send, recv, device_id=device, device_id_type=MESH)

    def tall(i):
        return pl.ds(pl.multiple_of(i * TALL, TALL), TALL)

    def wide(q):
        return pl.ds(pl.multiple_of(q * WIDE, WIDE), WIDE)

    barrier = pltpu.get_barrier_semaphore()
    for step in (1, groups - 1):
        pl.semaphore_signal(barrier, inc=1, device_id=((a + step) % groups * side + b, column), device_id_type=MESH)
    for step in range(1, side):
        pl.semaphore_signal(barrier, inc=1, device_id=(a * side + (b + step) % side, column), device_id_type=MESH)
    for step in range(1, columns):
        pl.semaphore_signal(barrier, inc=1, device_id=(row, (column + step) % columns), device_id_type=MESH)
    pl.semaphore_wait(barrier, 2 + side - 1 + columns - 1)

    def source_of(d, f):
        return (chip + d) % chips * 2 + (core + f) % 2

    partner = source_of(0, 1)
    own_load = pltpu.make_async_copy(slab_ref, slabs.at[column], own_sem)
    own_load.start()
    inverse_load = pltpu.make_async_copy(inverse_ref, inverse, inverse_sem)

    def slab_out(d):
        to = source_of(d, 0) if d else partner
        return remote(slab_ref, slabs.at[column], slab_send.at[d], slab_recv.at[column], there(to))

    def slab_pass(d):
        place = slabs.at[source_of(d, 0)]
        return remote(place, place, pass_send.at[d - 1], slab_recv.at[source_of(d, 0)], there(partner))

    def slab_wait(s):
        place = slabs.at[s]
        remote(place, place, slab_send.at[0], slab_recv.at[s], there(partner)).wait_recv()

    for d in list(range(1, chips)) + [0]:
        slab_out(d).start()

    def load(slot, i):
        return pltpu.make_async_copy(factor_ref.at[tall(i), :], buf.at[slot, b, tall(i), :], load_sem.at[i])

    def place(slot, half, i):
        return buf.at[slot, half, tall(i), :]

    def entry(slot, i, to):
        return remote(factor_ref.at[tall(i), :], place(slot, b, i), entry_sem.at[i], recv_sem.at[slot, b, i], there(to))

    def up(slot, i):
        return remote(place(slot, b, i), place(slot, b, i), up_sem.at[slot, i], recv_sem.at[slot, b, i], (jnp.minimum(a + 1, groups - 1) * side + b, column))

    def down(slot, i):
        return remote(place(slot, b, i), place(slot, b, i), down_sem.at[slot, i], recv_sem.at[slot, b, i], (jnp.maximum(a - 1, 0) * side + b, column))

    def across(slot, step, i):
        return remote(place(slot, b, i), place(slot, b, i), side_sem.at[step - 1, slot, i], recv_sem.at[slot, b, i], (a * side + (b + step) % side, column))

    def arrived(slot, half, i):
        remote(place(slot, half, i), place(slot, half, i), up_sem.at[slot, i], recv_sem.at[slot, half, i], there(column)).wait_recv()

    def others(slot, i):
        for step in range(1, side):
            arrived(slot, (b + step) % side, i)

    def serve(slot, block, i):
        j, k = block
        if target_of(j, k) == j:

            @pl.when(a == k)
            def _():
                load(slot, i).wait()

            @pl.when(a != k)
            def _():
                arrived(slot, b, i)
        else:
            arrived(slot, b, i)

        @pl.when((a >= k) & (a < groups - 1))
        def _():
            up(slot, i).start()

        @pl.when((a <= k) & (a > 0))
        def _():
            down(slot, i).start()

        for step in range(1, side):
            across(slot, step, i).start()

    def sent(slot, block, i):
        k = block[1]

        @pl.when((a >= k) & (a < groups - 1))
        def _():
            up(slot, i).wait_send()

        @pl.when((a <= k) & (a > 0))
        def _():
            down(slot, i).wait_send()

        for step in range(1, side):
            across(slot, step, i).wait_send()

    for j, k in all_blocks:
        t = target_of(j, k)
        slot = blocks[t].index((j, k))

        @pl.when((column == j) & (a == k))
        def _():
            @pl.loop(0, chunks)
            def _(i):
                if t == j:
                    load(slot, i).start()
                else:
                    entry(slot, i, t).start()

    inverse_load.start()

    def on(c, work):
        pl.when(column == c)(work)

    rest[...] = jnp.zeros_like(rest)
    ones[...] = jnp.ones_like(ones)
    for turn in range(columns):
        d, f = turn // 2, turn % 2
        s = source_of(d, f)
        for c in range(columns):
            low, high = turn * chunks // columns, (turn + 1) * chunks // columns
            if before[c] and high > low:

                def work(c=c, low=low, high=high):
                    @pl.loop(low, high)
                    def _(i):
                        for block in before[c]:
                            serve(blocks[c].index(block), block, i)

                on(c, work)
        if turn == 0:
            own_load.wait()
        else:
            slab_wait(s)
            if f == 0:
                slab_pass(d).start()
        high, low = halves(slabs[s] * live_ref[...])
        stack[:height] = high
        stack[height:] = low

        @pl.loop(0, pieces)
        def _(q):
            index = lax.broadcasted_iota(jnp.int32, (width, WIDE), 0) + s * width
            chosen = jnp.where(index == order_ref[:, wide(q)], 1.0, 0.0).astype(jnp.bfloat16)
            both = jnp.dot(stack[...], chosen, preferred_element_type=jnp.float32)
            rest[:, wide(q)] += both[:height] + both[height:]

    def vec_wait(slot, q):
        here = vec_in.at[slot, :, wide(q)]
        remote(here, here, vec_send.at[0, q], vec_recv.at[slot, q], there(column)).wait_recv()

    def part_wait(slot, q):
        here = part_in.at[slot, :, wide(q)]
        remote(here, here, part_send.at[0, q], part_recv.at[slot, q], there(column)).wait_recv()

    def vec_out(c, n, q):
        u = vec_to[c][n]
        here = vec.at[:, wide(q)]
        return remote(here, vec_in.at[vec_from[u].index(c), :, wide(q)], vec_send.at[n, q], vec_recv.at[vec_from[u].index(c), q], there(u))

    def part_to(block, made, q):
        j, k = block
        slot = part_from[j].index(k)
        return remote(part_out.at[made, :, wide(q)], part_in.at[slot, :, wide(q)], part_send.at[made, q], part_recv.at[slot, q], there(j))

    per_piece = WIDE // TALL

    def make_part(c, block, served):
        slot, made = blocks[c].index(block), part_made[c].index(block)

        @pl.loop(0, pieces)
        def _(q):
            for n in range(per_piece):
                if served:
                    serve(slot, block, q * per_piece + n)
            for n in range(per_piece):
                others(slot, q * per_piece + n)
            total = jnp.zeros((height, WIDE), jnp.float32)
            for half in range(side):
                total += nt3(stack[:, half * part : (half + 1) * part], buf[slot, half, wide(q), :])
            part_out[made, :, wide(q)] = total
            part_to(block, made, q).start()

    def take_before(c):
        for k in vec_from[c]:
            coming = vec_from[c].index(k)
            for block in [jk for jk in before[c] if jk[1] == k and jk[0] != c]:
                for q in range(pieces):
                    vec_wait(coming, q)
                high, low = halves(vec_in[coming])
                stack[:height] = high
                stack[height:] = low
                make_part(c, block, False)
            for block in [jk for jk in before[c] if jk[1] == k and jk[0] == c]:
                slot = blocks[c].index(block)

                @pl.loop(0, chunks)
                def _(i):
                    others(slot, i)

                for q in range(pieces):
                    if not [jk for jk in before[c] if jk[1] == k and jk[0] != c]:
                        vec_wait(coming, q)
                    high, low = halves(vec_in[coming, :, q * WIDE : (q + 1) * WIDE])
                    stack[:height, :WIDE] = high
                    stack[height:, :WIDE] = low
                    half, at = q * WIDE // part, q * WIDE % part

                    @pl.loop(0, pieces)
                    def _(n):
                        rest[:, wide(n)] -= nt3(stack[:, :WIDE], buf[slot, half, wide(n), at : at + WIDE])

    for c in range(columns):
        if before[c]:
            on(c, functools.partial(take_before, c))

    inverse_load.wait()
    squares = jnp.zeros((8, height), jnp.float32)
    for q in range(pieces):
        here = slice(q * WIDE, (q + 1) * WIDE)
        for c in range(columns):
            if part_from[c]:

                def work(c=c):
                    for slot in range(len(part_from[c])):
                        part_wait(slot, q)
                        rest[:, here] -= part_in[slot, :, here]

                on(c, work)
        high, low = halves(rest[:, here])
        stack[:height, here] = high
        stack[height:, here] = low
        done = nt3(stack[:, : (q + 1) * WIDE], inverse[here, : (q + 1) * WIDE])
        vec[:, here] = done
        high, low = halves(done * done)
        squares += nt(ones[...], high) + nt(ones[...], low)
        for c in range(columns):
            if vec_to[c]:

                def work(c=c):
                    for n in range(len(vec_to[c])):
                        vec_out(c, n, q).start()

                on(c, work)
    store = pltpu.make_async_copy(vec, out_ref, out_sem)
    store.start()
    sums[column] = squares

    def sum_out(step):
        to = (column + step) % columns
        return remote(sums.at[column], sums.at[column], sum_send.at[step - 1], sum_recv.at[column], there(to))

    for step in range(1, columns):
        sum_out(step).start()

    def give_after(c):
        high, low = halves(vec[...])
        stack[:height] = high
        stack[height:] = low
        for block in after[c]:
            make_part(c, block, True)

    for c in range(columns):
        if after[c]:
            on(c, functools.partial(give_after, c))

    for d in range(chips):
        slab_out(d).wait_send()
    for d in range(1, chips):
        slab_pass(d).wait_send()
    for j, k in all_blocks:
        t = target_of(j, k)
        if t != j:
            slot = blocks[t].index((j, k))

            @pl.when((column == j) & (a == k))
            def _():
                @pl.loop(0, chunks)
                def _(i):
                    entry(slot, i, t).wait_send()

    for c in range(columns):

        def work(c=c):
            for slot, block in enumerate(blocks[c]):

                @pl.loop(0, chunks)
                def _(i):
                    sent(slot, block, i)

            for q in range(pieces):
                for n in range(len(vec_to[c])):
                    vec_out(c, n, q).wait_send()
                for made, block in enumerate(part_made[c]):
                    part_to(block, made, q).wait_send()

        on(c, work)
    for step in range(1, columns):
        came = sums.at[(column + step) % columns]
        remote(came, came, sum_send.at[step - 1], sum_recv.at[(column + step) % columns], there(column)).wait_recv()
    total = sums[0]
    for c in range(1, columns):
        total += sums[c]
    mean_ref[...] = total[:1] / (width * columns)
    for step in range(1, columns):
        sum_out(step).wait_send()
    store.wait()


def chain_device(slab, factor, block_inverse, pivot_order, row_count):
    height, width = slab.shape
    depth, part = factor.shape
    groups = lax.axis_size("cols")
    side = lax.axis_size("rows") // groups
    column = lax.axis_index("cols")
    order = lax.dynamic_slice_in_dim(pivot_order, column * width, width)[None, :]
    live = (jnp.arange(height, dtype=jnp.int32) < row_count[0]).astype(jnp.float32)[:, None]
    slots = max([sum(target_of(j, k) == c for j in range(groups) for k in range(j)) for c in range(groups)])
    chunks, pieces, chips = depth // TALL, width // WIDE, groups // 2
    sem, space = pltpu.SemaphoreType.DMA, pltpu.VMEM
    f32, bf16 = jnp.float32, jnp.bfloat16
    held = pl.BlockSpec(memory_space=pltpu.VMEM)
    away = pl.BlockSpec(memory_space=pl.ANY)
    vectors, mean = pl.pallas_call(
        functools.partial(chain_kernel, groups, side),
        out_shape=(jax.ShapeDtypeStruct((height, width), f32), jax.ShapeDtypeStruct((1, height), f32)),
        in_specs=[away, away, away, held, held],
        out_specs=(away, held),
        scratch_shapes=[
            space((slots, side, depth, part), f32),
            space((width, width), f32),
            space((groups, height, width), f32),
            space((height, width), f32),
            space((height, width), f32),
            space((2 * height, width), bf16),
            space((groups - 2, height, width), f32),
            space((groups - 2, height, width), f32),
            space((max(1, groups // 2 - 1), height, width), f32),
            space((groups, 8, height), f32),
            space((8, WIDE), bf16),
            sem((chunks,)),
            sem((slots, side, chunks)),
            sem((slots, chunks)),
            sem((slots, chunks)),
            sem((side - 1, slots, chunks)),
            sem((chunks,)),
            sem(()),
            sem(()),
            sem((chips,)),
            sem((groups,)),
            sem((chips - 1,)),
            sem((groups, pieces)),
            sem((groups, pieces)),
            sem((groups, pieces)),
            sem((groups, pieces)),
            sem((groups,)),
            sem((groups,)),
            sem(()),
        ],
        compiler_params=pltpu.CompilerParams(collective_id=0, has_side_effects=True, vmem_limit_bytes=60000 * 1024),
    )(slab, factor, block_inverse, order, live)
    return vectors, mean[0]


def per_device(slab, factor, block_inverse, pivot_order, row_count):
    groups, rows = lax.axis_size("cols"), lax.axis_size("rows")
    depth, part = factor.shape
    fits = groups % 2 == 0 and rows % groups == 0 and rows > groups and part % WIDE == 0 and depth % WIDE == 0
    one = chain_device if fits else plain_device
    return one(slab, factor, block_inverse, pivot_order, row_count)


def solution(mesh):
    placed = (P("rows", "cols"), P("cols", "rows"), P("cols", None), P(), P("rows"))
    return jax.shard_map(
        per_device,
        mesh=mesh,
        in_specs=placed,
        out_specs=(P("rows", "cols"), P("rows")),
        check_vma=False,
    )
```

```python
import functools
import jax
import jax.numpy as jnp
from jax import lax
from jax.experimental import pallas as pl
from jax.experimental.pallas import tpu as pltpu
from jax.sharding import PartitionSpec as P

MESH = pl.DeviceIdType.MESH


def times_transposed(left, right):
    return lax.dot_general(
        left,
        right,
        (((1,), (1,)), ((), ())),
        precision=lax.Precision.HIGH,
        preferred_element_type=jnp.float32,
    )


def gather_kernel(groups, side, chunks, part_ref, row_ref, mine, in_sem, keep_sem, right_sem, left_sem, hop_sem, side_sem, cross_sem):
    row, column = lax.axis_index("rows"), lax.axis_index("cols")
    a, b = row // side, row % side
    depth, width = part_ref.shape
    tall = depth // chunks

    def at(a_to, b_to):
        return (a_to * side + b_to, column)

    barrier = pltpu.get_barrier_semaphore()
    for step in (1, groups - 1):
        pl.semaphore_signal(barrier, inc=1, device_id=at((a + step) % groups, b), device_id_type=MESH)
    for step in range(1, side):
        pl.semaphore_signal(barrier, inc=1, device_id=at(a, (b + step) % side), device_id_type=MESH)
    pl.semaphore_wait(barrier, 2 + side - 1)

    def rows_of(i):
        return pl.ds(pl.multiple_of(i * tall, tall), tall)

    def place(k, b_of, i):
        return row_ref.at[k * side + b_of, rows_of(i), :]

    def right(k, i, source):
        return pltpu.make_async_remote_copy(source, place(k, b, i), right_sem.at[k, i], hop_sem.at[k, i], device_id=at(jnp.minimum(a + 1, groups - 1), b), device_id_type=MESH)

    def left(k, i, source):
        return pltpu.make_async_remote_copy(source, place(k, b, i), left_sem.at[k, i], hop_sem.at[k, i], device_id=at(jnp.maximum(a - 1, 0), b), device_id_type=MESH)

    def across(k, step, i, source):
        return pltpu.make_async_remote_copy(source, place(k, b, i), side_sem.at[step - 1, k, i], cross_sem.at[step - 1, k, i], device_id=at(a, (b + step) % side), device_id_type=MESH)

    def load(i):
        return pltpu.make_async_copy(part_ref.at[rows_of(i), :], mine.at[rows_of(i), :], in_sem.at[i])

    def keep(i):
        return pltpu.make_async_copy(mine.at[rows_of(i), :], place(a, b, i), keep_sem.at[i])

    @pl.when(a < column)
    def _():
        @pl.loop(0, chunks)
        def _(i):
            load(i).start()

        @pl.loop(0, chunks)
        def _(i):
            source = mine.at[rows_of(i), :]
            load(i).wait()

            @pl.when(a < groups - 1)
            def _():
                right(a, i, source).start()

            @pl.when(a > 0)
            def _():
                left(a, i, source).start()

            for step in range(1, side):
                across(a, step, i, source).start()
            keep(i).start()

    for hop in range(1, groups):
        @pl.loop(0, chunks)
        def _(i):
            k = a - hop

            @pl.when((k >= 0) & (k < column))
            def _():
                source = place(k, b, i)
                right(k, i, source).wait_recv()

                @pl.when(a < groups - 1)
                def _():
                    right(k, i, source).start()

                for step in range(1, side):
                    across(k, step, i, source).start()

            h = a + hop

            @pl.when((h <= groups - 1) & (h < column))
            def _():
                source = place(h, b, i)
                left(h, i, source).wait_recv()

                @pl.when(a > 0)
                def _():
                    left(h, i, source).start()

                for step in range(1, side):
                    across(h, step, i, source).start()

    for k in range(groups - 1):
        @pl.when(k < column)
        def _():
            @pl.loop(0, chunks)
            def _(i):
                source = place(k, b, i)
                for step in range(1, side):
                    came = place(k, (b + side - step) % side, i)
                    pltpu.make_async_remote_copy(came, came, side_sem.at[step - 1, k, i], cross_sem.at[step - 1, k, i], device_id=at(a, (b + step) % side), device_id_type=MESH).wait_recv()
                    across(k, step, i, source).wait_send()

                @pl.when((k <= a) & (a < groups - 1))
                def _():
                    right(k, i, source).wait_send()

                @pl.when((k >= a) & (a > 0))
                def _():
                    left(k, i, source).wait_send()

                @pl.when(k == a)
                def _():
                    keep(i).wait()


def gather_factor(factor, rows, groups):
    side = rows // groups
    depth, width = factor.shape
    chunks = max(1, depth // 256)
    sem = pltpu.SemaphoreType.DMA
    return pl.pallas_call(
        functools.partial(gather_kernel, groups, side, chunks),
        out_shape=jax.ShapeDtypeStruct(((groups - 1) * side, depth, width), jnp.float32),
        in_specs=[pl.BlockSpec(memory_space=pl.ANY)],
        out_specs=pl.BlockSpec(memory_space=pl.ANY),
        scratch_shapes=[
            pltpu.VMEM((depth, width), jnp.float32),
            sem((chunks,)),
            sem((chunks,)),
            sem((groups, chunks)),
            sem((groups, chunks)),
            sem((groups, chunks)),
            sem((side - 1, groups, chunks)),
            sem((side - 1, groups, chunks)),
        ],
        compiler_params=pltpu.CompilerParams(collective_id=0, has_side_effects=True, vmem_limit_bytes=58 * 1024 * 1024),
        cost_estimate=pl.CostEstimate(flops=0, bytes_accessed=600000000, transcendentals=0),
    )(factor)


def plain_device(slab, factor, block_inverse, pivot_order, row_count):
    rows_here, block_width = slab.shape
    row_devices = lax.axis_size("rows")
    column_count = lax.axis_size("cols")
    column = lax.axis_index("cols")
    total_width = block_width * column_count
    side = row_devices // column_count
    chosen = lax.dynamic_slice_in_dim(pivot_order, column * block_width, block_width)
    gathered = lax.all_gather(slab, "cols", axis=1, tiled=True)
    parts = gather_factor(factor, row_devices, column_count)
    gathered, parts = lax.optimization_barrier((gathered, parts))
    ordered = jnp.take(gathered, chosen, axis=1)
    live_rows = jnp.arange(rows_here, dtype=jnp.int32) < row_count[0]
    pending = jnp.where(live_rows[:, None], ordered, jnp.float32(0.0))

    def finish(values):
        return times_transposed(values, block_inverse)

    def nothing(values):
        return jnp.zeros_like(values)

    width = factor.shape[1]
    vectors = jnp.zeros_like(pending)
    for k in range(column_count):
        finished = lax.cond(column == k, finish, nothing, pending)
        vectors = vectors + finished
        if k + 1 < column_count:
            arrived = moving = finished
            for to in range(k + 1, column_count):
                moving = lax.ppermute(moving, "cols", [(to - 1, to)])
                arrived = jnp.where(column == to, moving, arrived)
            update = jnp.zeros_like(pending)
            for b in range(side):
                update += times_transposed(arrived[:, b * width : (b + 1) * width], parts[k * side + b])
            pending = pending - jnp.where(k < column, update, jnp.float32(0.0))
    row_sums = lax.psum(jnp.sum(vectors * vectors, axis=1), "cols")
    return (vectors, row_sums / total_width)


TALL = 128
WIDE = 256
ROUND = 64
LAG = 2


def target_of(j, k):
    if k == j - 1:
        return j if j % 2 else j - 2
    return j - 1 if j % 2 and k == 0 else None


def halves(values):
    high = values.astype(jnp.bfloat16)
    return high, (values - high.astype(jnp.float32)).astype(jnp.bfloat16)


def nt(left, right):
    return lax.dot_general(left, right, (((1,), (1,)), ((), ())), preferred_element_type=jnp.float32)


def nt3(stacked, right):
    rows = stacked.shape[0] // 2
    high, low = halves(right)
    both = nt(stacked, high)
    return both[:rows] + (both[rows:] + nt(stacked[:rows], low))


def chain_kernel(
    groups,
    side,
    slab_ref,
    factor_ref,
    inverse_ref,
    order_ref,
    live_ref,
    out_ref,
    mean_ref,
    buf,
    inverse,
    slabs,
    rest,
    vec,
    stack,
    vec_in,
    part_in,
    part_out,
    sums,
    ones,
    stay,
    guest,
    guest_stack,
    guest_part,
    load_sem,
    recv_sem,
    up_sem,
    down_sem,
    side_sem,
    entry_sem,
    inverse_sem,
    own_sem,
    slab_send,
    slab_recv,
    pass_send,
    vec_send,
    vec_recv,
    part_send,
    part_recv,
    sum_send,
    sum_recv,
    out_sem,
    stay_load,
    stay_send,
    stay_recv,
    guest_send,
    guest_recv,
    back_send,
    back_recv,
):
    columns = groups
    row, column = lax.axis_index("rows"), lax.axis_index("cols")
    a, b = row // side, row % side
    height, width = rest.shape
    depth, part = factor_ref.shape
    chunks = depth // TALL
    pieces = width // WIDE
    rounds = height // ROUND
    chips = columns // 2
    chip, core = column // 2, column % 2
    all_blocks = [(j, k) for j in range(1, columns) for k in range(j)]
    moving = [jk for jk in all_blocks if target_of(*jk) is not None]
    staying = [jk for jk in all_blocks if target_of(*jk) is None]
    blocks = [[jk for jk in moving if target_of(*jk) == c] for c in range(columns)]
    before = [[jk for jk in blocks[c] if jk[1] < c] for c in range(columns)]
    after = [[jk for jk in blocks[c] if jk[1] > c] for c in range(columns)]
    vec_from = [sorted({k for _, k in blocks[c] if k != c}) for c in range(columns)]
    vec_to = [[u for u in range(columns) if c in vec_from[u]] for c in range(columns)]
    part_from = [[k for k in range(c) if target_of(c, k) != c] for c in range(columns)]
    part_made = [[jk for jk in blocks[c] if jk[0] != c] for c in range(columns)]

    def there(c):
        return (row, c)

    def level(z, c):
        return (z * side + b, c)

    def beside(step):
        return (a * side + (b + step) % side, column)

    def remote(source, target, send, recv, device):
        return pltpu.make_async_remote_copy(source, target, send, recv, device_id=device, device_id_type=MESH)

    def landed(here, recv):
        remote(here, here, out_sem, recv, there(column)).wait_recv()

    def tall(i):
        return pl.ds(pl.multiple_of(i * TALL, TALL), TALL)

    def wide(q):
        return pl.ds(pl.multiple_of(q * WIDE, WIDE), WIDE)

    def few(r):
        return pl.ds(pl.multiple_of(r * ROUND, ROUND), ROUND)

    def on(c, work):
        pl.when(column == c)(work)

    barrier = pltpu.get_barrier_semaphore()
    for step in range(1, side):
        pl.semaphore_signal(barrier, inc=1, device_id=beside(step), device_id_type=MESH)
    for up_by in range(groups):
        for right_by in range(columns):
            if up_by or right_by:
                pl.semaphore_signal(barrier, inc=1, device_id=level((a + up_by) % groups, (column + right_by) % columns), device_id_type=MESH)
    pl.semaphore_wait(barrier, side - 1 + groups * columns - 1)

    def source_of(d, f):
        return (chip + d) % chips * 2 + (core + f) % 2

    partner = source_of(0, 1)
    own_load = pltpu.make_async_copy(slab_ref, slabs.at[column], own_sem)
    own_load.start()
    inverse_load = pltpu.make_async_copy(inverse_ref, inverse, inverse_sem)

    def slab_out(d):
        to = source_of(d, 0) if d else partner
        return remote(slab_ref, slabs.at[column], slab_send.at[d], slab_recv.at[column], there(to))

    def slab_pass(d):
        place = slabs.at[source_of(d, 0)]
        return remote(place, place, pass_send.at[d - 1], slab_recv.at[source_of(d, 0)], there(partner))

    for d in list(range(1, chips)) + [0]:
        slab_out(d).start()

    def place(slot, half, i):
        return buf.at[slot, half, tall(i), :]

    def load(slot, i):
        return pltpu.make_async_copy(factor_ref.at[tall(i), :], place(slot, b, i), load_sem.at[i])

    def entry(slot, i, to):
        return remote(factor_ref.at[tall(i), :], place(slot, b, i), entry_sem.at[i], recv_sem.at[slot, b, i], there(to))

    def up(slot, i):
        return remote(place(slot, b, i), place(slot, b, i), up_sem.at[slot, i], recv_sem.at[slot, b, i], level(jnp.minimum(a + 1, groups - 1), column))

    def down(slot, half, i):
        return remote(place(slot, half, i), place(slot, half, i), down_sem.at[slot, half, i], recv_sem.at[slot, half, i], level(jnp.maximum(a - 1, 0), column))

    def across(slot, step, i):
        return remote(place(slot, b, i), place(slot, b, i), side_sem.at[step - 1, slot, i], recv_sem.at[slot, b, i], beside(step))

    def arrived(slot, half, i):
        landed(place(slot, half, i), recv_sem.at[slot, half, i])

    def both_down(block):
        return block[1] >= 2

    def flows(slot, block, i, act):
        k = block[1]

        @pl.when((a >= k) & (a < groups - 1))
        def _():
            act(up(slot, i))

        @pl.when((a <= k) & (a > 0))
        def _():
            act(down(slot, b, i))

        if both_down(block):

            @pl.when(a >= k)
            def _():
                for step in range(1, side):
                    act(across(slot, step, i))
        else:
            for step in range(1, side):
                act(across(slot, step, i))

    def other_flows(slot, block, i, act):
        @pl.when((a <= block[1]) & (a > 0))
        def _():
            for step in range(1, side):
                act(down(slot, (b + step) % side, i))

    def serve(slot, block, i):
        j, k = block
        if target_of(j, k) == j:

            @pl.when(a == k)
            def _():
                load(slot, i).wait()

            @pl.when(a != k)
            def _():
                arrived(slot, b, i)
        else:
            arrived(slot, b, i)
        flows(slot, block, i, lambda copy: copy.start())
        if both_down(block):

            @pl.when(i >= LAG)
            def _():
                serve_others(slot, block, i - LAG)

    def serve_others(slot, block, i):
        for step in range(1, side):
            arrived(slot, (b + step) % side, i)
        other_flows(slot, block, i, lambda copy: copy.start())

    def others(slot, block, i):
        if not both_down(block):
            for step in range(1, side):
                arrived(slot, (b + step) % side, i)

    def stay_out(step, q):
        return remote(factor_ref.at[wide(q), :], stay.at[b, wide(q), :], stay_send.at[step - 1, q], stay_recv.at[b, q], beside(step))

    def stay_in():
        return pltpu.make_async_copy(factor_ref, stay.at[b], stay_load)

    for j, k in all_blocks:
        t = target_of(j, k)

        @pl.when((column == j) & (a == k))
        def _():
            if t is None:
                for q in range(pieces):
                    for step in range(1, side):
                        stay_out(step, q).start()
                stay_in().start()
            else:
                slot = blocks[t].index((j, k))

                @pl.loop(0, chunks)
                def _(i):
                    if t == j:
                        load(slot, i).start()
                    else:
                        entry(slot, i, t).start()

    inverse_load.start()

    rest[...] = jnp.zeros_like(rest)
    ones[...] = jnp.ones_like(ones)
    for turn in range(columns):
        d, f = turn // 2, turn % 2
        s = source_of(d, f)
        for c in range(columns):
            low, high = turn * chunks // columns, (turn + 1) * chunks // columns
            if before[c] and high > low:

                def work(c=c, low=low, high=high):
                    @pl.loop(low, high)
                    def _(i):
                        for block in before[c]:
                            serve(blocks[c].index(block), block, i)

                on(c, work)
        if turn == 0:
            own_load.wait()
        else:
            landed(slabs.at[s], slab_recv.at[s])
            if f == 0:
                slab_pass(d).start()
        high, low = halves(slabs[s] * live_ref[...])
        stack[:height] = high
        stack[height:] = low

        @pl.loop(0, pieces)
        def _(q):
            index = lax.broadcasted_iota(jnp.int32, (width, WIDE), 0) + s * width
            chosen = jnp.where(index == order_ref[:, wide(q)], 1.0, 0.0).astype(jnp.bfloat16)
            both = jnp.dot(stack[...], chosen, preferred_element_type=jnp.float32)
            rest[:, wide(q)] += both[:height] + both[height:]

    def finish_serving(c):
        for block in before[c]:
            if both_down(block):

                @pl.loop(chunks - LAG, chunks)
                def _(i):
                    serve_others(blocks[c].index(block), block, i)

    def vec_wait(slot, q):
        landed(vec_in.at[slot, :, wide(q)], vec_recv.at[slot, q])

    def part_wait(slot, q):
        landed(part_in.at[slot, :, wide(q)], part_recv.at[slot, q])

    def vec_out(c, n, q):
        u = vec_to[c][n]
        slot = vec_from[u].index(c)
        return remote(vec.at[:, wide(q)], vec_in.at[slot, :, wide(q)], vec_send.at[n, q], vec_recv.at[slot, q], there(u))

    def part_to(block, made, q):
        j, k = block
        slot = part_from[j].index(k)
        return remote(part_out.at[made, :, wide(q)], part_in.at[slot, :, wide(q)], part_send.at[made, q], part_recv.at[slot, q], there(j))

    def put(values):
        high, low = halves(values)
        stack[:height] = high
        stack[height:] = low

    def known(j, k):
        return k in vec_from[j]

    def guest_out(n, j, k, r):
        return remote(vec.at[few(r), :], guest.at[a, few(r), :], guest_send.at[n, r], guest_recv.at[a, r], level(k, j))

    def back(j, k, z, r):
        slot = part_from[j].index(k)
        source = guest_part.at[r, z * ROUND : (z + 1) * ROUND, :]
        return remote(source, part_in.at[slot, few(r), :], back_send.at[z, r], back_recv.at[slot, r], level(z, j))

    def host(j, k):
        slot = part_from[j].index(k)
        if known(j, k):
            for q in range(pieces):
                vec_wait(vec_from[j].index(k), q)
        stay_in().wait()
        for step in range(1, side):
            half = (b + step) % side
            for q in range(pieces):
                landed(stay.at[half, wide(q), :], stay_recv.at[half, q])

        @pl.loop(0, rounds)
        def _(r):
            for z in range(groups):
                if z == k and known(j, k):
                    high, low = halves(vec_in[vec_from[j].index(k), few(r), :])
                else:
                    landed(guest.at[z, few(r), :], guest_recv.at[z, r])
                    high, low = halves(guest[z, few(r), :])
                guest_stack[z * ROUND : (z + 1) * ROUND] = high
                guest_stack[(groups + z) * ROUND : (groups + z + 1) * ROUND] = low

            @pl.loop(0, pieces)
            def _(q):
                total = jnp.zeros((groups * ROUND, WIDE), jnp.float32)
                for half in range(side):
                    total += nt3(guest_stack[:, half * part : (half + 1) * part], stay[half, wide(q), :])
                guest_part[r, :, wide(q)] = total
                part_in[slot, few(r), wide(q)] = total[k * ROUND : (k + 1) * ROUND]

            for z in range(groups):
                if z != k:
                    back(j, k, z, r).start()

    def make_part(c, block, q):
        slot, made = blocks[c].index(block), part_made[c].index(block)
        for n in range(WIDE // TALL):
            others(slot, block, q * (WIDE // TALL) + n)
        total = jnp.zeros((height, WIDE), jnp.float32)
        for half in range(side):
            total += nt3(stack[:, half * part : (half + 1) * part], buf[slot, half, wide(q), :])
        part_out[made, :, wide(q)] = total
        part_to(block, made, q).start()

    def take_before(c):
        finish_serving(c)
        for j, k in staying:
            if j == c:
                pl.when(a == k)(functools.partial(host, j, k))
        for block in before[c]:
            j, k = block
            slot, coming = blocks[c].index(block), vec_from[c].index(k)
            if j != c:

                def work(k=k):
                    for q in range(pieces):
                        vec_wait(coming, q)

                if known(c, k) and (c, k) in staying:
                    pl.when(a != k)(work)
                else:
                    work()
                put(vec_in[coming])

                @pl.loop(0, pieces)
                def _(q):
                    make_part(c, block, q)
            else:

                @pl.loop(0, chunks)
                def _(i):
                    others(slot, block, i)

                for q in range(pieces):
                    vec_wait(coming, q)
                    high, low = halves(vec_in[coming, :, q * WIDE : (q + 1) * WIDE])
                    stack[:height, :WIDE] = high
                    stack[height:, :WIDE] = low
                    half, at = q * WIDE // part, q * WIDE % part

                    @pl.loop(0, pieces)
                    def _(n):
                        rest[:, wide(n)] -= nt3(stack[:, :WIDE], buf[slot, half, wide(n), at : at + WIDE])

    for c in range(columns):
        if before[c]:
            on(c, functools.partial(take_before, c))

    inverse_load.wait()
    squares = jnp.zeros((8, height), jnp.float32)
    for q in range(pieces):
        here = slice(q * WIDE, (q + 1) * WIDE)
        for c in range(columns):
            if part_from[c]:

                def work(c=c):
                    for slot, k in enumerate(part_from[c]):
                        if (c, k) not in staying:
                            part_wait(slot, q)
                        elif q == 0:

                            @pl.when(a != k)
                            def _():
                                for r in range(rounds):
                                    landed(part_in.at[slot, few(r), :], back_recv.at[slot, r])

                        rest[:, here] -= part_in[slot, :, here]

                on(c, work)
        high, low = halves(rest[:, here])
        stack[:height, here] = high
        stack[height:, here] = low
        done = nt3(stack[:, : (q + 1) * WIDE], inverse[here, : (q + 1) * WIDE])
        vec[:, here] = done
        high, low = halves(done * done)
        squares += nt(ones[...], high) + nt(ones[...], low)
        for c in range(columns):
            if vec_to[c]:

                def work(c=c):
                    for n in range(len(vec_to[c])):
                        vec_out(c, n, q).start()

                on(c, work)

    def guests(c, act):
        for n, (j, k) in enumerate([jk for jk in staying if jk[1] == c]):

            def work():
                for r in range(rounds):
                    act(guest_out(n, j, k, r))

            if known(j, k):
                pl.when(a != k)(work)
            else:
                work()

    for c in range(columns):
        on(c, functools.partial(guests, c, lambda copy: copy.start()))
    store = pltpu.make_async_copy(vec, out_ref, out_sem)
    store.start()
    sums[column] = squares

    def sum_out(step):
        to = (column + step) % columns
        return remote(sums.at[column], sums.at[column], sum_send.at[step - 1], sum_recv.at[column], there(to))

    for step in range(1, columns):
        sum_out(step).start()

    def give_after(c):
        for block in after[c]:
            slot, coming = blocks[c].index(block), vec_from[c].index(block[1])

            @pl.loop(0, chunks - pieces)
            def _(i):
                serve(slot, block, i)

            for q in range(pieces):
                vec_wait(coming, q)
            put(vec_in[coming])

            @pl.loop(0, pieces)
            def _(q):
                serve(slot, block, chunks - pieces + q)
                make_part(c, block, q)

    for c in range(columns):
        if after[c]:
            on(c, functools.partial(give_after, c))

    for d in range(chips):
        slab_out(d).wait_send()
    for d in range(1, chips):
        slab_pass(d).wait_send()
    for j, k in all_blocks:
        t = target_of(j, k)

        @pl.when((column == j) & (a == k))
        def _():
            if t is None:
                for q in range(pieces):
                    for step in range(1, side):
                        stay_out(step, q).wait_send()
                for r in range(rounds):
                    for z in range(groups):
                        if z != k:
                            back(j, k, z, r).wait_send()
            elif t != j:

                @pl.loop(0, chunks)
                def _(i):
                    entry(blocks[t].index((j, k)), i, t).wait_send()

    for c in range(columns):

        def work(c=c):
            for slot, block in enumerate(blocks[c]):

                @pl.loop(0, chunks)
                def _(i):
                    flows(slot, block, i, lambda copy: copy.wait_send())
                    if both_down(block):
                        other_flows(slot, block, i, lambda copy: copy.wait_send())

            for q in range(pieces):
                for n in range(len(vec_to[c])):
                    vec_out(c, n, q).wait_send()
                for made, block in enumerate(part_made[c]):
                    part_to(block, made, q).wait_send()
            guests(c, lambda copy: copy.wait_send())

        on(c, work)
    for step in range(1, columns):
        came = (column + step) % columns
        landed(sums.at[came], sum_recv.at[came])
    total = sums[0]
    for c in range(1, columns):
        total += sums[c]
    mean_ref[...] = total[:1] / (width * columns)
    for step in range(1, columns):
        sum_out(step).wait_send()
    store.wait()


def chain_device(slab, factor, block_inverse, pivot_order, row_count):
    height, width = slab.shape
    depth, part = factor.shape
    groups = lax.axis_size("cols")
    side = lax.axis_size("rows") // groups
    column = lax.axis_index("cols")
    order = lax.dynamic_slice_in_dim(pivot_order, column * width, width)[None, :]
    live = (jnp.arange(height, dtype=jnp.int32) < row_count[0]).astype(jnp.float32)[:, None]
    slots = max([sum(target_of(j, k) == c for j in range(groups) for k in range(j)) for c in range(groups)])
    chunks, pieces, rounds, chips = depth // TALL, width // WIDE, height // ROUND, groups // 2
    sem, space = pltpu.SemaphoreType.DMA, pltpu.VMEM
    f32, bf16 = jnp.float32, jnp.bfloat16
    held = pl.BlockSpec(memory_space=pltpu.VMEM)
    away = pl.BlockSpec(memory_space=pl.ANY)
    vectors, mean = pl.pallas_call(
        functools.partial(chain_kernel, groups, side),
        out_shape=(jax.ShapeDtypeStruct((height, width), f32), jax.ShapeDtypeStruct((1, height), f32)),
        in_specs=[away, away, away, held, held],
        out_specs=(away, held),
        scratch_shapes=[
            space((slots, side, depth, part), f32),
            space((width, width), f32),
            space((groups, height, width), f32),
            space((height, width), f32),
            space((height, width), f32),
            space((2 * height, width), bf16),
            space((1, height, width), f32),
            space((groups - 2, height, width), f32),
            space((1, height, width), f32),
            space((groups, 8, height), f32),
            space((8, WIDE), bf16),
            space((side, depth, part), f32),
            space((groups, height, width), f32),
            space((2 * groups * ROUND, width), bf16),
            space((rounds, groups * ROUND, width), f32),
            sem((chunks,)),
            sem((slots, side, chunks)),
            sem((slots, chunks)),
            sem((slots, side, chunks)),
            sem((side - 1, slots, chunks)),
            sem((chunks,)),
            sem(()),
            sem(()),
            sem((chips,)),
            sem((groups,)),
            sem((chips - 1,)),
            sem((groups, pieces)),
            sem((groups, pieces)),
            sem((groups, pieces)),
            sem((groups, pieces)),
            sem((groups,)),
            sem((groups,)),
            sem(()),
            sem(()),
            sem((side - 1, pieces)),
            sem((side, pieces)),
            sem((groups, rounds)),
            sem((groups, rounds)),
            sem((groups, rounds)),
            sem((groups, rounds)),
        ],
        compiler_params=pltpu.CompilerParams(collective_id=0, has_side_effects=True, vmem_limit_bytes=60 * 1024 * 1024),
    )(slab, factor, block_inverse, order, live)
    return vectors, mean[0]


def per_device(slab, factor, block_inverse, pivot_order, row_count):
    groups, rows = lax.axis_size("cols"), lax.axis_size("rows")
    depth, part = factor.shape
    fits = groups // 2 == 2 and rows % groups == 0 and rows > groups and part % WIDE == 0 and depth % WIDE == 0 and slab.shape[0] % ROUND == 0
    one = chain_device if fits else plain_device
    return one(slab, factor, block_inverse, pivot_order, row_count)


def solution(mesh):
    placed = (P("rows", "cols"), P("cols", "rows"), P("cols", None), P(), P("rows"))
    return jax.shard_map(
        per_device,
        mesh=mesh,
        in_specs=placed,
        out_specs=(P("rows", "cols"), P("rows")),
        check_vma=False,
    )
```

```python
import functools
import jax
import jax.numpy as jnp
from jax import lax
from jax.experimental import pallas as pl
from jax.experimental.pallas import tpu as pltpu
from jax.sharding import PartitionSpec as P

MESH = pl.DeviceIdType.MESH


def times_transposed(left, right):
    return lax.dot_general(
        left,
        right,
        (((1,), (1,)), ((), ())),
        precision=lax.Precision.HIGH,
        preferred_element_type=jnp.float32,
    )


def gather_kernel(groups, side, chunks, part_ref, row_ref, mine, in_sem, keep_sem, right_sem, left_sem, hop_sem, side_sem, cross_sem):
    row, column = lax.axis_index("rows"), lax.axis_index("cols")
    a, b = row // side, row % side
    depth, width = part_ref.shape
    tall = depth // chunks

    def at(a_to, b_to):
        return (a_to * side + b_to, column)

    barrier = pltpu.get_barrier_semaphore()
    for step in (1, groups - 1):
        pl.semaphore_signal(barrier, inc=1, device_id=at((a + step) % groups, b), device_id_type=MESH)
    for step in range(1, side):
        pl.semaphore_signal(barrier, inc=1, device_id=at(a, (b + step) % side), device_id_type=MESH)
    pl.semaphore_wait(barrier, 2 + side - 1)

    def rows_of(i):
        return pl.ds(pl.multiple_of(i * tall, tall), tall)

    def place(k, b_of, i):
        return row_ref.at[k * side + b_of, rows_of(i), :]

    def right(k, i, source):
        return pltpu.make_async_remote_copy(source, place(k, b, i), right_sem.at[k, i], hop_sem.at[k, i], device_id=at(jnp.minimum(a + 1, groups - 1), b), device_id_type=MESH)

    def left(k, i, source):
        return pltpu.make_async_remote_copy(source, place(k, b, i), left_sem.at[k, i], hop_sem.at[k, i], device_id=at(jnp.maximum(a - 1, 0), b), device_id_type=MESH)

    def across(k, step, i, source):
        return pltpu.make_async_remote_copy(source, place(k, b, i), side_sem.at[step - 1, k, i], cross_sem.at[step - 1, k, i], device_id=at(a, (b + step) % side), device_id_type=MESH)

    def load(i):
        return pltpu.make_async_copy(part_ref.at[rows_of(i), :], mine.at[rows_of(i), :], in_sem.at[i])

    def keep(i):
        return pltpu.make_async_copy(mine.at[rows_of(i), :], place(a, b, i), keep_sem.at[i])

    @pl.when(a < column)
    def _():
        @pl.loop(0, chunks)
        def _(i):
            load(i).start()

        @pl.loop(0, chunks)
        def _(i):
            source = mine.at[rows_of(i), :]
            load(i).wait()

            @pl.when(a < groups - 1)
            def _():
                right(a, i, source).start()

            @pl.when(a > 0)
            def _():
                left(a, i, source).start()

            for step in range(1, side):
                across(a, step, i, source).start()
            keep(i).start()

    for hop in range(1, groups):
        @pl.loop(0, chunks)
        def _(i):
            k = a - hop

            @pl.when((k >= 0) & (k < column))
            def _():
                source = place(k, b, i)
                right(k, i, source).wait_recv()

                @pl.when(a < groups - 1)
                def _():
                    right(k, i, source).start()

                for step in range(1, side):
                    across(k, step, i, source).start()

            h = a + hop

            @pl.when((h <= groups - 1) & (h < column))
            def _():
                source = place(h, b, i)
                left(h, i, source).wait_recv()

                @pl.when(a > 0)
                def _():
                    left(h, i, source).start()

                for step in range(1, side):
                    across(h, step, i, source).start()

    for k in range(groups - 1):
        @pl.when(k < column)
        def _():
            @pl.loop(0, chunks)
            def _(i):
                source = place(k, b, i)
                for step in range(1, side):
                    came = place(k, (b + side - step) % side, i)
                    pltpu.make_async_remote_copy(came, came, side_sem.at[step - 1, k, i], cross_sem.at[step - 1, k, i], device_id=at(a, (b + step) % side), device_id_type=MESH).wait_recv()
                    across(k, step, i, source).wait_send()

                @pl.when((k <= a) & (a < groups - 1))
                def _():
                    right(k, i, source).wait_send()

                @pl.when((k >= a) & (a > 0))
                def _():
                    left(k, i, source).wait_send()

                @pl.when(k == a)
                def _():
                    keep(i).wait()


def gather_factor(factor, rows, groups):
    side = rows // groups
    depth, width = factor.shape
    chunks = max(1, depth // 256)
    sem = pltpu.SemaphoreType.DMA
    return pl.pallas_call(
        functools.partial(gather_kernel, groups, side, chunks),
        out_shape=jax.ShapeDtypeStruct(((groups - 1) * side, depth, width), jnp.float32),
        in_specs=[pl.BlockSpec(memory_space=pl.ANY)],
        out_specs=pl.BlockSpec(memory_space=pl.ANY),
        scratch_shapes=[
            pltpu.VMEM((depth, width), jnp.float32),
            sem((chunks,)),
            sem((chunks,)),
            sem((groups, chunks)),
            sem((groups, chunks)),
            sem((groups, chunks)),
            sem((side - 1, groups, chunks)),
            sem((side - 1, groups, chunks)),
        ],
        compiler_params=pltpu.CompilerParams(collective_id=0, has_side_effects=True, vmem_limit_bytes=58 * 1024 * 1024),
        cost_estimate=pl.CostEstimate(flops=0, bytes_accessed=600000000, transcendentals=0),
    )(factor)


def plain_device(slab, factor, block_inverse, pivot_order, row_count):
    rows_here, block_width = slab.shape
    row_devices = lax.axis_size("rows")
    column_count = lax.axis_size("cols")
    column = lax.axis_index("cols")
    total_width = block_width * column_count
    side = row_devices // column_count
    chosen = lax.dynamic_slice_in_dim(pivot_order, column * block_width, block_width)
    gathered = lax.all_gather(slab, "cols", axis=1, tiled=True)
    parts = gather_factor(factor, row_devices, column_count)
    gathered, parts = lax.optimization_barrier((gathered, parts))
    ordered = jnp.take(gathered, chosen, axis=1)
    live_rows = jnp.arange(rows_here, dtype=jnp.int32) < row_count[0]
    pending = jnp.where(live_rows[:, None], ordered, jnp.float32(0.0))

    def finish(values):
        return times_transposed(values, block_inverse)

    def nothing(values):
        return jnp.zeros_like(values)

    width = factor.shape[1]
    vectors = jnp.zeros_like(pending)
    for k in range(column_count):
        finished = lax.cond(column == k, finish, nothing, pending)
        vectors = vectors + finished
        if k + 1 < column_count:
            arrived = moving = finished
            for to in range(k + 1, column_count):
                moving = lax.ppermute(moving, "cols", [(to - 1, to)])
                arrived = jnp.where(column == to, moving, arrived)
            update = jnp.zeros_like(pending)
            for b in range(side):
                update += times_transposed(arrived[:, b * width : (b + 1) * width], parts[k * side + b])
            pending = pending - jnp.where(k < column, update, jnp.float32(0.0))
    row_sums = lax.psum(jnp.sum(vectors * vectors, axis=1), "cols")
    return (vectors, row_sums / total_width)


TALL = 128
WIDE = 256
EARLY = (5, 7, 9)
LATER = 4


def target_of(j, k):
    if k == j - 1:
        return j if j % 2 else j - 2
    return j - 1 if j % 2 and k == 0 else None


def host_of(j, k):
    return j - 1 if j % 2 else j


def halves(values):
    high = values.astype(jnp.bfloat16)
    return high, (values - high.astype(jnp.float32)).astype(jnp.bfloat16)


def nt(left, right):
    return lax.dot_general(left, right, (((1,), (1,)), ((), ())), preferred_element_type=jnp.float32)


def nt3(stacked, right):
    rows = stacked.shape[0] // 2
    high, low = halves(right)
    both = nt(stacked, high)
    return both[:rows] + (both[rows:] + nt(stacked[:rows], low))


def chain_kernel(
    groups,
    side,
    slab_ref,
    factor_ref,
    inverse_ref,
    order_ref,
    live_ref,
    out_ref,
    mean_ref,
    buf,
    inverse,
    slabs,
    rest,
    vec,
    stack,
    vec_in,
    part_in,
    part_out,
    sums,
    ones,
    stay,
    guest,
    guest_stack,
    guest_part,
    load_sem,
    recv_sem,
    up_sem,
    down_sem,
    side_sem,
    entry_sem,
    inverse_sem,
    own_sem,
    slab_send,
    slab_recv,
    pass_send,
    vec_send,
    vec_recv,
    part_send,
    part_recv,
    sum_send,
    sum_recv,
    out_sem,
    stay_load,
    stay_send,
    stay_recv,
    guest_send,
    guest_recv,
    back_send,
    back_recv,
    lift_send,
    lift_back_send,
    gate,
):
    columns = groups
    row, column = lax.axis_index("rows"), lax.axis_index("cols")
    a, b = row // side, row % side
    height, width = rest.shape
    depth, part = factor_ref.shape
    chunks = depth // TALL
    pieces = width // WIDE
    rounds = groups - 1
    share = height // rounds
    chips = columns // 2
    chip, core = column // 2, column % 2
    all_blocks = [(j, k) for j in range(1, columns) for k in range(j)]
    moving = [jk for jk in all_blocks if target_of(*jk) is not None]
    staying = [jk for jk in all_blocks if target_of(*jk) is None]
    blocks = [[jk for jk in moving if target_of(*jk) == c] for c in range(columns)]
    before = [[jk for jk in blocks[c] if jk[1] < c] for c in range(columns)]
    after = [[jk for jk in blocks[c] if jk[1] > c] for c in range(columns)]
    heir = [host_of(*[jk for jk in staying if jk[1] == k][0]) if [jk for jk in staying if jk[1] == k] else None for k in range(columns)]
    hosted = [[k for j, k in staying if host_of(j, k) == c] for c in range(columns)]
    vec_from = [sorted({k for _, k in blocks[c] if k != c}) for c in range(columns)]
    vec_to = [[u for u in range(columns) if c in vec_from[u]] for c in range(columns)]
    part_from = [[k for k in range(c) if target_of(c, k) != c] for c in range(columns)]
    part_made = [[jk for jk in blocks[c] if jk[0] != c] for c in range(columns)]

    def there(c):
        return (row, c)

    def level(z, c):
        return (z * side + b, c)

    def beside(step):
        return (a * side + (b + step) % side, column)

    def remote(source, target, send, recv, device):
        return pltpu.make_async_remote_copy(source, target, send, recv, device_id=device, device_id_type=MESH)

    def landed(here, recv):
        remote(here, here, out_sem, recv, there(column)).wait_recv()

    def tall(i):
        return pl.ds(pl.multiple_of(i * TALL, TALL), TALL)

    def wide(q):
        return pl.ds(pl.multiple_of(q * WIDE, WIDE), WIDE)

    def few(r):
        return pl.ds(pl.multiple_of(r * share, share), share)

    def on(c, work):
        pl.when(column == c)(work)

    barrier = pltpu.get_barrier_semaphore()
    for step in range(1, side):
        pl.semaphore_signal(barrier, inc=1, device_id=beside(step), device_id_type=MESH)
        for right_by in range(1, columns):
            pl.semaphore_signal(barrier, inc=1, device_id=(a * side + (b + step) % side, (column + right_by) % columns), device_id_type=MESH)
    for up_by in range(groups):
        for right_by in range(columns):
            if up_by or right_by:
                pl.semaphore_signal(barrier, inc=1, device_id=level((a + up_by) % groups, (column + right_by) % columns), device_id_type=MESH)
    pl.semaphore_wait(barrier, (side - 1) * columns + groups * columns - 1)

    def source_of(d, f):
        return (chip + d) % chips * 2 + (core + f) % 2

    partner = source_of(0, 1)
    own_load = pltpu.make_async_copy(slab_ref, slabs.at[column], own_sem)
    own_load.start()
    inverse_load = pltpu.make_async_copy(inverse_ref, inverse, inverse_sem)

    def slab_out(d):
        to = source_of(d, 0) if d else partner
        return remote(slab_ref, slabs.at[column], slab_send.at[d], slab_recv.at[column], there(to))

    def slab_pass(d):
        place = slabs.at[source_of(d, 0)]
        return remote(place, place, pass_send.at[d - 1], slab_recv.at[source_of(d, 0)], there(partner))

    for d in list(range(1, chips)) + [0]:
        slab_out(d).start()

    def place(slot, half, i):
        return buf.at[slot, half, tall(i), :]

    def load(slot, i):
        return pltpu.make_async_copy(factor_ref.at[tall(i), :], place(slot, b, i), load_sem.at[i])

    def entry(slot, i, to):
        return remote(factor_ref.at[tall(i), :], place(slot, b, i), entry_sem.at[i], recv_sem.at[slot, b, i], there(to))

    def up(slot, i):
        return remote(place(slot, b, i), place(slot, b, i), up_sem.at[slot, i], recv_sem.at[slot, b, i], level(jnp.minimum(a + 1, groups - 1), column))

    def down(slot, half, i):
        return remote(place(slot, half, i), place(slot, half, i), down_sem.at[slot, half, i], recv_sem.at[slot, half, i], level(jnp.maximum(a - 1, 0), column))

    def across(slot, step, i):
        return remote(place(slot, b, i), place(slot, b, i), side_sem.at[step - 1, slot, i], recv_sem.at[slot, b, i], beside(step))

    def arrived(slot, half, i):
        landed(place(slot, half, i), recv_sem.at[slot, half, i])

    def both_down(block):
        return block[1] >= 2

    def lifted(block):
        return block[0] % 2 == 0

    def free_level(block):
        return functools.reduce(jnp.logical_and, [a != k for k in hosted[target_of(*block)]], a >= 0)

    def line_flows(slot, block, i, act):
        k = block[1]

        @pl.when((a >= k) & (a < groups - 1))
        def _():
            act(up(slot, i))

        if not lifted(block):

            @pl.when((a <= k) & (a > 0))
            def _():
                act(down(slot, b, i))

    def side_flows(slot, block, i, act):
        if both_down(block) or lifted(block):

            @pl.when(a >= block[1])
            def _():
                for step in range(1, side):
                    act(across(slot, step, i))
        else:
            for step in range(1, side):
                act(across(slot, step, i))

    def other_flows(slot, block, i, act):
        @pl.when((a <= block[1]) & (a > 0))
        def _():
            for step in range(1, side):
                act(down(slot, (b + step) % side, i))

    def serve(slot, block, i):
        j, k = block
        if target_of(j, k) == j:

            @pl.when(a == k)
            def _():
                load(slot, i).wait()

            @pl.when(a != k)
            def _():
                arrived(slot, b, i)
        else:
            arrived(slot, b, i)
        line_flows(slot, block, i, lambda copy: copy.start())

        @pl.when(free_level(block))
        def _():
            side_flows(slot, block, i, lambda copy: copy.start())


    def serve_ahead(slot, block, q, ahead):
        for n in range(WIDE // TALL):
            i = ahead + q * (WIDE // TALL) + n

            @pl.when(i < chunks)
            def _():
                serve(slot, block, i)

    def serve_others(slot, block, i):
        for step in range(1, side):
            arrived(slot, (b + step) % side, i)
        other_flows(slot, block, i, lambda copy: copy.start())

    def others(slot, block, i):
        def work():
            for step in range(1, side):
                arrived(slot, (b + step) % side, i)

        if both_down(block):
            pl.when((a > block[1]) | (a == 0))(work)
        else:
            work()

    def stay_out(step, q, to):
        return remote(factor_ref.at[wide(q), :], stay.at[b, wide(q), :], stay_send.at[step, q], stay_recv.at[b, q], (a * side + (b + step) % side, to))

    def stay_in():
        return pltpu.make_async_copy(factor_ref, stay.at[b], stay_load)

    for j, k in all_blocks:
        t = target_of(j, k)

        @pl.when((column == j) & (a == k))
        def _():
            if t is None:
                for step in range(0 if host_of(j, k) != j else 1, side):
                    for q in range(pieces):
                        stay_out(step, q, host_of(j, k)).start()
                if host_of(j, k) == j:
                    stay_in().start()
            else:
                slot = blocks[t].index((j, k))

                @pl.loop(0, chunks)
                def _(i):
                    if t == j:
                        load(slot, i).start()
                    else:
                        entry(slot, i, t).start()

    inverse_load.start()

    rest[...] = jnp.zeros_like(rest)
    ones[...] = jnp.ones_like(ones)

    def serving(c, low, high):
        for block in before[c]:

            def work(block=block):
                @pl.loop(low(block), high(block))
                def _(i):
                    serve(blocks[c].index(block), block, i)

            pl.when(a != block[1])(work)

    def early(n):
        return lambda block: jnp.maximum(EARLY[n] - jnp.abs(a - block[1]), 0)

    def serve_source(c):
        for block in before[c]:

            def work(block=block):
                @pl.loop(0, chunks)
                def _(i):
                    serve(blocks[c].index(block), block, i)

            pl.when(a == block[1])(work)

    for c in range(columns):
        if before[c]:
            on(c, functools.partial(serve_source, c))
    for turn in range(columns):
        d, f = turn // 2, turn % 2
        s = source_of(d, f)
        if turn >= 2:
            for c in range(columns):
                if before[c]:
                    on(c, functools.partial(serving, c, early(turn - 3) if turn > 2 else lambda block: 0, early(turn - 2)))
        if turn == 0:
            own_load.wait()
        else:
            landed(slabs.at[s], slab_recv.at[s])
            if f == 0:
                slab_pass(d).start()
        high, low = halves(slabs[s] * live_ref[...])
        stack[:height] = high
        stack[height:] = low

        @pl.loop(0, pieces)
        def _(q):
            index = lax.broadcasted_iota(jnp.int32, (width, WIDE), 0) + s * width
            chosen = jnp.where(index == order_ref[:, wide(q)], 1.0, 0.0).astype(jnp.bfloat16)
            both = jnp.dot(stack[...], chosen, preferred_element_type=jnp.float32)
            rest[:, wide(q)] += both[:height] + both[height:]

    def vec_wait(slot, q):
        landed(vec_in.at[slot, :, wide(q)], vec_recv.at[slot, q])

    def part_wait(slot, q):
        landed(part_in.at[slot, :, wide(q)], part_recv.at[slot, q])

    def vec_out(c, n, q):
        u = vec_to[c][n]
        slot = vec_from[u].index(c)
        return remote(vec.at[:, wide(q)], vec_in.at[slot, :, wide(q)], vec_send.at[n, q], vec_recv.at[slot, q], there(u))

    def vec_outs(c, q, act):
        for n, u in enumerate(vec_to[c]):
            lifting = [jk for jk in after[u] if jk[1] == c]

            def work():
                act(vec_out(c, n, q))

            if lifting:
                pl.when(a >= c)(work)
            else:
                work()

    def lift_to(c):
        return [jk for u in range(columns) for jk in after[u] if jk[1] == c]

    def lift_out(block, r):
        j, k = block
        return remote(vec.at[few(r), :], guest.at[a, few(r), :], lift_send.at[r], guest_recv.at[a, r], level(k, target_of(j, k)))

    def lift_back(block, z, q):
        j, k = block
        slot = part_from[j].index(k)
        return remote(guest.at[groups - 1 - z, :, wide(q)], part_in.at[slot, :, wide(q)], lift_back_send.at[z, q], part_recv.at[slot, q], level(z, j))

    def part_to(block, made, q):
        j, k = block
        slot = part_from[j].index(k)
        return remote(part_out.at[made, :, wide(q)], part_in.at[slot, :, wide(q)], part_send.at[made, q], part_recv.at[slot, q], there(j))

    def put(values):
        high, low = halves(values)
        stack[:height] = high
        stack[height:] = low

    def known(k):
        return k in vec_from[heir[k]]

    def guest_out(k, r):
        return remote(vec.at[few(r), :], guest.at[a, few(r), :], guest_send.at[r], guest_recv.at[a, r], level(k, heir[k]))

    def back(j, k, z, r):
        slot = part_from[j].index(k)
        n = z - (z > k)
        source = guest_part.at[r, n * share : (n + 1) * share, :] if z != k else guest_part.at[rounds, few(r), :]
        return remote(source, part_in.at[slot, few(r), :], back_send.at[z, r], back_recv.at[slot, r], level(z, j))

    def products(rows, q):
        total = jnp.zeros((rows, WIDE), jnp.float32)
        for half in range(side):
            total += nt3(guest_stack[:, half * part : (half + 1) * part], stay[half, wide(q), :])
        return total

    def host(j, k):
        c = host_of(j, k)
        if c == j:
            stay_in().wait()
        for step in range(1 if c == j else 0, side):
            half = (b + step) % side
            for q in range(pieces):
                landed(stay.at[half, wide(q), :], stay_recv.at[half, q])
        for block in blocks[c]:

            @pl.loop(0, chunks)
            def _(i):
                side_flows(blocks[c].index(block), block, i, lambda copy: copy.start())

        away = [z for z in range(groups) if z != k]
        tall_of = len(away) * share

        @pl.loop(0, rounds)
        def _(r):
            for n, z in enumerate(away):
                landed(guest.at[z, few(r), :], guest_recv.at[z, r])
                high, low = halves(guest[z, few(r), :])
                guest_stack[n * share : (n + 1) * share] = high
                guest_stack[tall_of + n * share : tall_of + (n + 1) * share] = low

            @pl.loop(0, pieces)
            def _(q):
                guest_part[r, :, wide(q)] = products(tall_of, q)

            for n, z in enumerate(away):
                back(j, k, z, r).start()

        if c == j:
            host_own(j, k)

    def host_own(j, k):
        c = host_of(j, k)
        if known(k):
            for q in range(pieces):
                vec_wait(vec_from[c].index(k), q)
            own = vec_in.at[vec_from[c].index(k)]
        else:
            for r in range(rounds):
                landed(guest.at[k, few(r), :], guest_recv.at[k, r])
            own = guest.at[k]
        high, low = halves(own[...])
        guest_stack[:height] = high
        guest_stack[height:] = low

        @pl.loop(0, pieces)
        def _(q):
            if c == j:
                part_in[part_from[j].index(k), :, wide(q)] = products(height, q)
            else:
                guest_part[rounds, :, wide(q)] = products(height, q)

        if c != j:
            for r in range(rounds):
                back(j, k, k, r).start()

    def make_part(c, block, q):
        slot, made = blocks[c].index(block), part_made[c].index(block)
        for n in range(WIDE // TALL):
            others(slot, block, q * (WIDE // TALL) + n)
        total = jnp.zeros((height, WIDE), jnp.float32)
        for half in range(side):
            total += nt3(stack[:, half * part : (half + 1) * part], buf[slot, half, wide(q), :])
        part_out[made, :, wide(q)] = total
        part_to(block, made, q).start()

    def take_before(c):
        for block in before[c]:
            j, k = block
            slot, coming = blocks[c].index(block), vec_from[c].index(k)
            if both_down(block):
                serving(c, early(columns - 3), lambda block: chunks)

                @pl.when((a <= k) & (a > 0))
                def _():
                    @pl.loop(0, chunks)
                    def _(i):
                        serve_others(slot, block, i)

                @pl.loop(0, chunks)
                def _(i):
                    others(slot, block, i)

                for q in range(pieces):
                    vec_wait(coming, q)
                    high, low = halves(vec_in[coming, :, q * WIDE : (q + 1) * WIDE])
                    stack[:height, :WIDE] = high
                    stack[height:, :WIDE] = low
                    half, at = q * WIDE // part, q * WIDE % part

                    @pl.loop(0, pieces)
                    def _(n):
                        rest[:, wide(n)] -= nt3(stack[:, :WIDE], buf[slot, half, wide(n), at : at + WIDE])
            elif j != c:
                serving(c, early(columns - 3), lambda block: chunks)
                for jj, kk in staying:
                    if host_of(jj, kk) == c:
                        pl.when(a == kk)(functools.partial(host, jj, kk))

                def work():
                    for q in range(pieces):
                        vec_wait(coming, q)

                if c == heir[k]:
                    pl.when(a != k)(work)
                else:
                    work()
                put(vec_in[coming])

                @pl.loop(0, pieces)
                def _(q):
                    make_part(c, block, q)
            else:
                serving(c, early(columns - 3), early(columns - 2))
                for q in range(pieces):
                    vec_wait(coming, q)
                put(vec_in[coming])

                @pl.loop(0, pieces)
                def _(q):
                    @pl.when(a != k)
                    def _():
                        serve_ahead(slot, block, q, early(columns - 2)(block))

                    for u in range(columns):
                        for jj, kk in after[u]:
                            if kk == c:

                                @pl.when((a == kk) & (q == (chunks - EARLY[columns - 2] + 1) * TALL // WIDE + 1))
                                def _():
                                    pl.semaphore_signal(gate, inc=1, device_id=there(u), device_id_type=MESH)

                    for n in range(WIDE // TALL):
                        others(slot, block, q * (WIDE // TALL) + n)
                    total = jnp.zeros((height, WIDE), jnp.float32)
                    for half in range(side):
                        total += nt3(stack[:, half * part : (half + 1) * part], buf[slot, half, wide(q), :])
                    rest[:, wide(q)] -= total

    for c in range(columns):
        if before[c]:
            on(c, functools.partial(take_before, c))

    inverse_load.wait()
    squares = jnp.zeros((8, height), jnp.float32)
    for q in range(pieces):
        here = slice(q * WIDE, (q + 1) * WIDE)
        for c in range(columns):
            if part_from[c]:

                def work(c=c):
                    for slot, k in enumerate(part_from[c]):
                        if (c, k) not in staying:
                            part_wait(slot, q)
                        elif q == 0:

                            def back_wait(slot=slot):
                                for r in range(rounds):
                                    landed(part_in.at[slot, few(r), :], back_recv.at[slot, r])

                            if host_of(c, k) == c:
                                pl.when(a != k)(back_wait)
                            else:
                                back_wait()

                        rest[:, here] -= part_in[slot, :, here]

                on(c, work)
        high, low = halves(rest[:, here])
        stack[:height, here] = high
        stack[height:, here] = low
        done = nt3(stack[:, : (q + 1) * WIDE], inverse[here, : (q + 1) * WIDE])
        vec[:, here] = done
        high, low = halves(done * done)
        squares += nt(ones[...], high) + nt(ones[...], low)
        for c in range(columns):
            if vec_to[c]:

                on(c, functools.partial(vec_outs, c, q, lambda copy: copy.start()))

    def guest_round(c, r):
        def work():
            if r:
                guest_out(c, r - 1).wait_send()
            if r < rounds:
                guest_out(c, r).start()

        if known(c):
            pl.when(a != c)(work)
        else:
            work()

    def guests(c):
        for block in lift_to(c):

            @pl.when(a < c)
            def _():
                for r in range(rounds):
                    lift_out(block, r).start()

        if heir[c] is not None:
            for r in range(1 if after[c] else rounds + 1):
                guest_round(c, r)

    for c in range(columns):
        on(c, functools.partial(guests, c))
    store = pltpu.make_async_copy(vec, out_ref, out_sem)
    store.start()
    sums[column] = squares

    def sum_out(step):
        to = (column + step) % columns
        return remote(sums.at[column], sums.at[column], sum_send.at[step - 1], sum_recv.at[column], there(to))

    for step in range(1, columns):
        sum_out(step).start()

    for j, k in staying:
        if host_of(j, k) != j:
            pl.when((column == host_of(j, k)) & (a == k))(functools.partial(host_own, j, k))

    def give_after(c):
        for block in after[c]:
            j, k = block
            slot, coming = blocks[c].index(block), vec_from[c].index(k)

            if heir[c] is not None:
                for r in range(1, rounds + 1):
                    guest_round(c, r)

                    @pl.when(a == k)
                    def _():
                        if r == 1:
                            pl.semaphore_wait(gate, 1)

                    @pl.when(a >= k)
                    def _():
                        @pl.loop((r - 1) * LATER // rounds, r * LATER // rounds)
                        def _(i):
                            serve(slot, block, i)

            @pl.when(a >= k)
            def _():
                for q in range(pieces):
                    vec_wait(coming, q)
                put(vec_in[coming])

                @pl.loop(0, pieces)
                def _(q):
                    serve_ahead(slot, block, q, LATER)
                    make_part(c, block, q)

            @pl.when(a == k)
            def _():
                for z in range(k):
                    for r in range(rounds):
                        landed(guest.at[z, few(r), :], guest_recv.at[z, r])
                    high, low = halves(guest[z])
                    stack[:height] = high
                    stack[height:] = low

                    @pl.loop(0, pieces)
                    def _(q):
                        total = jnp.zeros((height, WIDE), jnp.float32)
                        for half in range(side):
                            total += nt3(stack[:, half * part : (half + 1) * part], buf[slot, half, wide(q), :])
                        guest[groups - 1 - z, :, wide(q)] = total
                        lift_back(block, z, q).start()

    for c in range(columns):
        if after[c]:
            on(c, functools.partial(give_after, c))

    for d in range(chips):
        slab_out(d).wait_send()
    for d in range(1, chips):
        slab_pass(d).wait_send()
    for j, k in all_blocks:
        t = target_of(j, k)

        @pl.when((column == j) & (a == k))
        def _():
            if t is not None and t != j:

                @pl.loop(0, chunks)
                def _(i):
                    entry(blocks[t].index((j, k)), i, t).wait_send()

    for j, k in staying:

        @pl.when((column == j) & (a == k))
        def _():
            for q in range(pieces):
                for step in range(0 if host_of(j, k) != j else 1, side):
                    stay_out(step, q, host_of(j, k)).wait_send()

        @pl.when((column == host_of(j, k)) & (a == k))
        def _():
            for r in range(rounds):
                for z in range(groups):
                    if z != k or host_of(j, k) != j:
                        back(j, k, z, r).wait_send()

    for c in range(columns):

        def work(c=c):
            for slot, block in enumerate(blocks[c]):

                @pl.loop(0, chunks)
                def _(i):
                    line_flows(slot, block, i, lambda copy: copy.wait_send())
                    side_flows(slot, block, i, lambda copy: copy.wait_send())
                    if both_down(block):
                        other_flows(slot, block, i, lambda copy: copy.wait_send())

            for q in range(pieces):
                vec_outs(c, q, lambda copy: copy.wait_send())
                for made, block in enumerate(part_made[c]):
                    if lifted(block):

                        @pl.when(a >= block[1])
                        def _():
                            part_to(block, made, q).wait_send()

                        @pl.when(a == block[1])
                        def _():
                            for z in range(block[1]):
                                lift_back(block, z, q).wait_send()
                    else:
                        part_to(block, made, q).wait_send()
            for block in lift_to(c):

                @pl.when(a < c)
                def _():
                    for r in range(rounds):
                        lift_out(block, r).wait_send()


        on(c, work)
    for step in range(1, columns):
        came = (column + step) % columns
        landed(sums.at[came], sum_recv.at[came])
    total = sums[0]
    for c in range(1, columns):
        total += sums[c]
    mean_ref[...] = total[:1] / (width * columns)
    for step in range(1, columns):
        sum_out(step).wait_send()
    store.wait()


def chain_device(slab, factor, block_inverse, pivot_order, row_count):
    height, width = slab.shape
    depth, part = factor.shape
    groups = lax.axis_size("cols")
    side = lax.axis_size("rows") // groups
    column = lax.axis_index("cols")
    order = lax.dynamic_slice_in_dim(pivot_order, column * width, width)[None, :]
    live = (jnp.arange(height, dtype=jnp.int32) < row_count[0]).astype(jnp.float32)[:, None]
    slots = max([sum(target_of(j, k) == c for j in range(groups) for k in range(j)) for c in range(groups)])
    chunks, pieces, rounds, chips = depth // TALL, width // WIDE, groups - 1, groups // 2
    sem, space = pltpu.SemaphoreType.DMA, pltpu.VMEM
    f32, bf16 = jnp.float32, jnp.bfloat16
    held = pl.BlockSpec(memory_space=pltpu.VMEM)
    away = pl.BlockSpec(memory_space=pl.ANY)
    vectors, mean = pl.pallas_call(
        functools.partial(chain_kernel, groups, side),
        out_shape=(jax.ShapeDtypeStruct((height, width), f32), jax.ShapeDtypeStruct((1, height), f32)),
        in_specs=[away, away, away, held, held],
        out_specs=(away, held),
        scratch_shapes=[
            space((slots, side, depth, part), f32),
            space((width, width), f32),
            space((groups, height, width), f32),
            space((height, width), f32),
            space((height, width), f32),
            space((2 * height, width), bf16),
            space((1, height, width), f32),
            space((groups - 2, height, width), f32),
            space((1, height, width), f32),
            space((groups, 8, height), f32),
            space((8, WIDE), bf16),
            space((side, depth, part), f32),
            space((groups, height, width), f32),
            space((2 * height, width), bf16),
            space((rounds + 1, height, width), f32),
            sem((chunks,)),
            sem((slots, side, chunks)),
            sem((slots, chunks)),
            sem((slots, side, chunks)),
            sem((side - 1, slots, chunks)),
            sem((chunks,)),
            sem(()),
            sem(()),
            sem((chips,)),
            sem((groups,)),
            sem((chips - 1,)),
            sem((groups, pieces)),
            sem((groups, pieces)),
            sem((groups, pieces)),
            sem((groups, pieces)),
            sem((groups,)),
            sem((groups,)),
            sem(()),
            sem(()),
            sem((side, pieces)),
            sem((side, pieces)),
            sem((rounds,)),
            sem((groups, rounds)),
            sem((groups, rounds)),
            sem((groups, rounds)),
            sem((rounds,)),
            sem((groups, pieces)),
            pltpu.SemaphoreType.REGULAR,
        ],
        compiler_params=pltpu.CompilerParams(collective_id=0, has_side_effects=True, vmem_limit_bytes=60 * 1024 * 1024),
    )(slab, factor, block_inverse, order, live)
    return vectors, mean[0]


def per_device(slab, factor, block_inverse, pivot_order, row_count):
    groups, rows = lax.axis_size("cols"), lax.axis_size("rows")
    depth, part = factor.shape
    fits = groups // 2 == 2 and rows % groups == 0 and rows > groups and part % WIDE == 0 and depth % WIDE == 0 and slab.shape[0] % (8 * (groups - 1)) == 0
    one = chain_device if fits else plain_device
    return one(slab, factor, block_inverse, pivot_order, row_count)


def solution(mesh):
    placed = (P("rows", "cols"), P("cols", "rows"), P("cols", None), P(), P("rows"))
    return jax.shard_map(
        per_device,
        mesh=mesh,
        in_specs=placed,
        out_specs=(P("rows", "cols"), P("rows")),
        check_vma=False,
    )
```

```python
import functools
import jax
import jax.numpy as jnp
from jax import lax
from jax.experimental import pallas as pl
from jax.experimental.pallas import tpu as pltpu
from jax.sharding import PartitionSpec as P

MESH = pl.DeviceIdType.MESH


def times_transposed(left, right):
    return lax.dot_general(
        left,
        right,
        (((1,), (1,)), ((), ())),
        precision=lax.Precision.HIGH,
        preferred_element_type=jnp.float32,
    )


def gather_kernel(groups, side, chunks, part_ref, row_ref, mine, in_sem, keep_sem, right_sem, left_sem, hop_sem, side_sem, cross_sem):
    row, column = lax.axis_index("rows"), lax.axis_index("cols")
    a, b = row // side, row % side
    depth, width = part_ref.shape
    tall = depth // chunks

    def at(a_to, b_to):
        return (a_to * side + b_to, column)

    barrier = pltpu.get_barrier_semaphore()
    for step in (1, groups - 1):
        pl.semaphore_signal(barrier, inc=1, device_id=at((a + step) % groups, b), device_id_type=MESH)
    for step in range(1, side):
        pl.semaphore_signal(barrier, inc=1, device_id=at(a, (b + step) % side), device_id_type=MESH)
    pl.semaphore_wait(barrier, 2 + side - 1)

    def rows_of(i):
        return pl.ds(pl.multiple_of(i * tall, tall), tall)

    def place(k, b_of, i):
        return row_ref.at[k * side + b_of, rows_of(i), :]

    def right(k, i, source):
        return pltpu.make_async_remote_copy(source, place(k, b, i), right_sem.at[k, i], hop_sem.at[k, i], device_id=at(jnp.minimum(a + 1, groups - 1), b), device_id_type=MESH)

    def left(k, i, source):
        return pltpu.make_async_remote_copy(source, place(k, b, i), left_sem.at[k, i], hop_sem.at[k, i], device_id=at(jnp.maximum(a - 1, 0), b), device_id_type=MESH)

    def across(k, step, i, source):
        return pltpu.make_async_remote_copy(source, place(k, b, i), side_sem.at[step - 1, k, i], cross_sem.at[step - 1, k, i], device_id=at(a, (b + step) % side), device_id_type=MESH)

    def load(i):
        return pltpu.make_async_copy(part_ref.at[rows_of(i), :], mine.at[rows_of(i), :], in_sem.at[i])

    def keep(i):
        return pltpu.make_async_copy(mine.at[rows_of(i), :], place(a, b, i), keep_sem.at[i])

    @pl.when(a < column)
    def _():
        @pl.loop(0, chunks)
        def _(i):
            load(i).start()

        @pl.loop(0, chunks)
        def _(i):
            source = mine.at[rows_of(i), :]
            load(i).wait()

            @pl.when(a < groups - 1)
            def _():
                right(a, i, source).start()

            @pl.when(a > 0)
            def _():
                left(a, i, source).start()

            for step in range(1, side):
                across(a, step, i, source).start()
            keep(i).start()

    for hop in range(1, groups):
        @pl.loop(0, chunks)
        def _(i):
            k = a - hop

            @pl.when((k >= 0) & (k < column))
            def _():
                source = place(k, b, i)
                right(k, i, source).wait_recv()

                @pl.when(a < groups - 1)
                def _():
                    right(k, i, source).start()

                for step in range(1, side):
                    across(k, step, i, source).start()

            h = a + hop

            @pl.when((h <= groups - 1) & (h < column))
            def _():
                source = place(h, b, i)
                left(h, i, source).wait_recv()

                @pl.when(a > 0)
                def _():
                    left(h, i, source).start()

                for step in range(1, side):
                    across(h, step, i, source).start()

    for k in range(groups - 1):
        @pl.when(k < column)
        def _():
            @pl.loop(0, chunks)
            def _(i):
                source = place(k, b, i)
                for step in range(1, side):
                    came = place(k, (b + side - step) % side, i)
                    pltpu.make_async_remote_copy(came, came, side_sem.at[step - 1, k, i], cross_sem.at[step - 1, k, i], device_id=at(a, (b + step) % side), device_id_type=MESH).wait_recv()
                    across(k, step, i, source).wait_send()

                @pl.when((k <= a) & (a < groups - 1))
                def _():
                    right(k, i, source).wait_send()

                @pl.when((k >= a) & (a > 0))
                def _():
                    left(k, i, source).wait_send()

                @pl.when(k == a)
                def _():
                    keep(i).wait()


def gather_factor(factor, rows, groups):
    side = rows // groups
    depth, width = factor.shape
    chunks = max(1, depth // 256)
    sem = pltpu.SemaphoreType.DMA
    return pl.pallas_call(
        functools.partial(gather_kernel, groups, side, chunks),
        out_shape=jax.ShapeDtypeStruct(((groups - 1) * side, depth, width), jnp.float32),
        in_specs=[pl.BlockSpec(memory_space=pl.ANY)],
        out_specs=pl.BlockSpec(memory_space=pl.ANY),
        scratch_shapes=[
            pltpu.VMEM((depth, width), jnp.float32),
            sem((chunks,)),
            sem((chunks,)),
            sem((groups, chunks)),
            sem((groups, chunks)),
            sem((groups, chunks)),
            sem((side - 1, groups, chunks)),
            sem((side - 1, groups, chunks)),
        ],
        compiler_params=pltpu.CompilerParams(collective_id=0, has_side_effects=True, vmem_limit_bytes=60000 * 1024),
        cost_estimate=pl.CostEstimate(flops=0, bytes_accessed=600000000, transcendentals=0),
    )(factor)


def plain_device(slab, factor, block_inverse, pivot_order, row_count):
    rows_here, block_width = slab.shape
    row_devices = lax.axis_size("rows")
    column_count = lax.axis_size("cols")
    column = lax.axis_index("cols")
    total_width = block_width * column_count
    side = row_devices // column_count
    chosen = lax.dynamic_slice_in_dim(pivot_order, column * block_width, block_width)
    gathered = lax.all_gather(slab, "cols", axis=1, tiled=True)
    parts = gather_factor(factor, row_devices, column_count)
    gathered, parts = lax.optimization_barrier((gathered, parts))
    ordered = jnp.take(gathered, chosen, axis=1)
    live_rows = jnp.arange(rows_here, dtype=jnp.int32) < row_count[0]
    pending = jnp.where(live_rows[:, None], ordered, jnp.float32(0.0))

    def finish(values):
        return times_transposed(values, block_inverse)

    def nothing(values):
        return jnp.zeros_like(values)

    width = factor.shape[1]
    vectors = jnp.zeros_like(pending)
    for k in range(column_count):
        finished = lax.cond(column == k, finish, nothing, pending)
        vectors = vectors + finished
        if k + 1 < column_count:
            arrived = moving = finished
            for to in range(k + 1, column_count):
                moving = lax.ppermute(moving, "cols", [(to - 1, to)])
                arrived = jnp.where(column == to, moving, arrived)
            update = jnp.zeros_like(pending)
            for b in range(side):
                update += times_transposed(arrived[:, b * width : (b + 1) * width], parts[k * side + b])
            pending = pending - jnp.where(k < column, update, jnp.float32(0.0))
    row_sums = lax.psum(jnp.sum(vectors * vectors, axis=1), "cols")
    return (vectors, row_sums / total_width)


TALL = 128
WIDE = 256
EARLY = (5, 7, 9)
LATER = 4


def target_of(j, k):
    if k == j - 1:
        return j if j % 2 else j - 2
    return j - 1 if j % 2 and k == 0 else None


def host_of(j, k):
    return j - 1 if j % 2 else j


def halves(values):
    high = values.astype(jnp.bfloat16)
    return high, (values - high.astype(jnp.float32)).astype(jnp.bfloat16)


def nt(left, right):
    return lax.dot_general(left, right, (((1,), (1,)), ((), ())), preferred_element_type=jnp.float32)


def nt3(stacked, right):
    rows = stacked.shape[0] // 2
    high, low = halves(right)
    both = nt(stacked, high)
    return both[:rows] + (both[rows:] + nt(stacked[:rows], low))


def chain_kernel(
    groups,
    side,
    slab_ref,
    factor_ref,
    inverse_ref,
    order_ref,
    count_ref,
    out_ref,
    mean_ref,
    buf,
    inverse,
    slabs,
    rest,
    vec,
    stack,
    vec_in,
    part_in,
    part_out,
    sums,
    ones,
    stay,
    guest,
    guest_stack,
    guest_part,
    help_stack,
    load_sem,
    recv_sem,
    up_sem,
    down_sem,
    side_sem,
    entry_sem,
    inverse_sem,
    own_sem,
    slab_send,
    slab_recv,
    pass_send,
    vec_send,
    vec_recv,
    part_send,
    part_recv,
    sum_send,
    sum_recv,
    out_sem,
    stay_load,
    stay_send,
    stay_recv,
    guest_send,
    guest_recv,
    back_send,
    back_recv,
    lift_send,
    lift_back_send,
    relayed_send,
    relay_send,
    own_back_send,
    gate,
):
    columns = groups
    row, column = lax.axis_index("rows"), lax.axis_index("cols")
    a, b = row // side, row % side
    height, width = rest.shape
    depth, part = factor_ref.shape
    chunks = depth // TALL
    pieces = width // WIDE
    rounds = groups - 1
    share = height // rounds
    chips = columns // 2
    chip, core = column // 2, column % 2
    all_blocks = [(j, k) for j in range(1, columns) for k in range(j)]
    moving = [jk for jk in all_blocks if target_of(*jk) is not None]
    staying = [jk for jk in all_blocks if target_of(*jk) is None]
    blocks = [[jk for jk in moving if target_of(*jk) == c] for c in range(columns)]
    before = [[jk for jk in blocks[c] if jk[1] < c] for c in range(columns)]
    after = [[jk for jk in blocks[c] if jk[1] > c] for c in range(columns)]
    heir = [host_of(*[jk for jk in staying if jk[1] == k][0]) if [jk for jk in staying if jk[1] == k] else None for k in range(columns)]
    hosted = [[k for j, k in staying if host_of(j, k) == c] for c in range(columns)]
    vec_from = [sorted({k for _, k in blocks[c] if k != c}) for c in range(columns)]
    vec_to = [[u for u in range(columns) if c in vec_from[u]] for c in range(columns)]
    part_from = [[k for k in range(c) if target_of(c, k) != c] for c in range(columns)]
    part_made = [[jk for jk in blocks[c] if jk[0] != c] for c in range(columns)]

    def there(c):
        return (row, c)

    def level(z, c):
        return (z * side + b, c)

    def beside(step):
        return (a * side + (b + step) % side, column)

    def remote(source, target, send, recv, device):
        return pltpu.make_async_remote_copy(source, target, send, recv, device_id=device, device_id_type=MESH)

    def landed(here, recv):
        remote(here, here, out_sem, recv, there(column)).wait_recv()

    def tall(i):
        return pl.ds(pl.multiple_of(i * TALL, TALL), TALL)

    def wide(q):
        return pl.ds(pl.multiple_of(q * WIDE, WIDE), WIDE)

    def few(r):
        return pl.ds(pl.multiple_of(r * share, share), share)

    def on(c, work):
        pl.when(column == c)(work)

    barrier = pltpu.get_barrier_semaphore()
    for step in range(1, side):
        pl.semaphore_signal(barrier, inc=1, device_id=beside(step), device_id_type=MESH)
        for right_by in range(1, columns):
            pl.semaphore_signal(barrier, inc=1, device_id=(a * side + (b + step) % side, (column + right_by) % columns), device_id_type=MESH)
    for up_by in range(groups):
        for right_by in range(columns):
            if up_by or right_by:
                pl.semaphore_signal(barrier, inc=1, device_id=level((a + up_by) % groups, (column + right_by) % columns), device_id_type=MESH)
    pl.semaphore_wait(barrier, (side - 1) * columns + groups * columns - 1)

    def source_of(d, f):
        return (chip + d) % chips * 2 + (core + f) % 2

    partner = source_of(0, 1)
    own_load = pltpu.make_async_copy(slab_ref, slabs.at[column], own_sem)
    own_load.start()
    inverse_load = pltpu.make_async_copy(inverse_ref, inverse, inverse_sem)

    def slab_out(d):
        to = source_of(d, 0) if d else partner
        return remote(slab_ref, slabs.at[column], slab_send.at[d], slab_recv.at[column], there(to))

    def slab_pass(d):
        place = slabs.at[source_of(d, 0)]
        return remote(place, place, pass_send.at[d - 1], slab_recv.at[source_of(d, 0)], there(partner))

    for d in list(range(1, chips)) + [0]:
        slab_out(d).start()

    def place(slot, half, i):
        return buf.at[slot, half] if i is None else buf.at[slot, half, tall(i), :]

    def came(slot, half, i):
        return recv_sem.at[slot, half, 0 if i is None else i]

    def load(slot, i):
        return pltpu.make_async_copy(factor_ref.at[tall(i), :], place(slot, b, i), load_sem.at[i])

    def entry(slot, i, to):
        return remote(factor_ref if i is None else factor_ref.at[tall(i), :], place(slot, b, i), entry_sem, came(slot, b, i), there(to))

    def up(slot, i):
        return remote(place(slot, b, i), place(slot, b, i), up_sem.at[slot], came(slot, b, i), level(jnp.minimum(a + 1, groups - 1), column))

    def down(slot, half, i):
        return remote(place(slot, half, i), place(slot, half, i), down_sem.at[slot, half], came(slot, half, i), level(jnp.maximum(a - 1, 0), column))

    def across(slot, step, i):
        return remote(place(slot, b, i), place(slot, b, i), side_sem.at[step - 1, slot], came(slot, b, i), beside(step))

    def arrived(slot, half, i):
        landed(place(slot, half, i), recv_sem.at[slot, half, i])

    def both_down(block):
        return block[1] >= 2

    def lifted(block):
        return block[0] % 2 == 0

    top = groups - 1

    def crosses(block):
        return target_of(*block) != block[0]

    def active(block):
        if not crosses(block):
            return a >= 0
        return a >= block[1] if lifted(block) else a < top

    def helper(block):
        return block[1] if lifted(block) else top - 1

    def helped_level(block):
        return block[1] - 1 if lifted(block) else top

    def helping(block):
        return a == helper(block)

    def free_level(block):
        return functools.reduce(jnp.logical_and, [a != k for k in hosted[target_of(*block)]], a >= 0)

    def line_flows(slot, block, i, act):
        k = block[1]

        @pl.when((a >= k) & (a < (top - 1 if crosses(block) and not lifted(block) else top)))
        def _():
            act(up(slot, i))

        if not lifted(block):

            @pl.when((a <= k) & (a > 0))
            def _():
                act(down(slot, b, i))

    def side_flows(slot, block, i, act):
        @pl.when((a >= block[1]) if both_down(block) else active(block))
        def _():
            for step in range(1, side):
                act(across(slot, step, i))

    def other_flows(slot, block, i, act):
        @pl.when((a <= block[1]) & (a > 0))
        def _():
            for step in range(1, side):
                act(down(slot, (b + step) % side, i))

    def serve(slot, block, i):
        j, k = block
        if target_of(j, k) == j:

            @pl.when(a == k)
            def _():
                load(slot, i).wait()

            @pl.when(a != k)
            def _():
                arrived(slot, b, i)
        else:
            arrived(slot, b, i)
        line_flows(slot, block, i, lambda copy: copy.start())

        @pl.when(free_level(block))
        def _():
            side_flows(slot, block, i, lambda copy: copy.start())


    def serve_ahead(slot, block, q, ahead):
        for n in range(WIDE // TALL):
            i = ahead + q * (WIDE // TALL) + n

            @pl.when(i < chunks)
            def _():
                serve(slot, block, i)

    def serve_others(slot, block, i):
        for step in range(1, side):
            arrived(slot, (b + step) % side, i)
        other_flows(slot, block, i, lambda copy: copy.start())

    def others(slot, block, i):
        def work():
            for step in range(1, side):
                arrived(slot, (b + step) % side, i)

        if both_down(block):
            pl.when((a > block[1]) | (a == 0))(work)
        else:
            work()

    def stay_out(step, q, to):
        here = factor_ref if q is None else factor_ref.at[wide(q), :]
        return remote(here, stay.at[b] if q is None else stay.at[b, wide(q), :], stay_send.at[step], stay_recv.at[b], (a * side + (b + step) % side, to))

    def stay_in():
        return pltpu.make_async_copy(factor_ref, stay.at[b], stay_load)

    for j, k in all_blocks:
        t = target_of(j, k)

        @pl.when((column == j) & (a == k))
        def _():
            if t is None:
                for step in range(0 if host_of(j, k) != j else 1, side):
                    for q in range(pieces):
                        stay_out(step, q, host_of(j, k)).start()
                if host_of(j, k) == j:
                    stay_in().start()
            else:
                slot = blocks[t].index((j, k))

                @pl.loop(0, chunks)
                def _(i):
                    if t == j:
                        load(slot, i).start()
                    else:
                        entry(slot, i, t).start()

    inverse_load.start()

    rest[...] = jnp.zeros_like(rest)
    live = lax.broadcasted_iota(jnp.int32, (height, 1), 0) < count_ref[0]
    ones[...] = jnp.ones_like(ones)

    def serving(c, low, high):
        for block in before[c]:

            def work(block=block):
                @pl.loop(low(block), high(block))
                def _(i):
                    serve(blocks[c].index(block), block, i)

            pl.when((a != block[1]) & active(block))(work)

    def early(n):
        return lambda block: jnp.maximum(EARLY[n] - jnp.abs(a - block[1]), 0)

    def serve_source(c):
        for block in before[c]:

            def work(block=block):
                @pl.loop(0, chunks)
                def _(i):
                    serve(blocks[c].index(block), block, i)

            pl.when(a == block[1])(work)

    for c in range(columns):
        if before[c]:
            on(c, functools.partial(serve_source, c))
    for turn in range(columns):
        d, f = turn // 2, turn % 2
        s = source_of(d, f)
        if turn >= 2:
            for c in range(columns):
                if before[c]:
                    on(c, functools.partial(serving, c, early(turn - 3) if turn > 2 else lambda block: 0, early(turn - 2)))
        if turn == 0:
            own_load.wait()
        else:
            landed(slabs.at[s], slab_recv.at[s])
            if f == 0:
                slab_pass(d).start()
        high, low = halves(jnp.where(live, slabs[s], 0.0))
        stack[:height] = high
        stack[height:] = low

        @pl.loop(0, pieces)
        def _(q):
            index = lax.broadcasted_iota(jnp.int32, (width, WIDE), 0) + s * width
            chosen = jnp.where(index == order_ref[:, pl.ds(pl.multiple_of(column * width + q * WIDE, WIDE), WIDE)], 1.0, 0.0).astype(jnp.bfloat16)
            both = jnp.dot(stack[...], chosen, preferred_element_type=jnp.float32)
            rest[:, wide(q)] += both[:height] + both[height:]

    def vec_wait(slot, q):
        landed(vec_in.at[slot, :, wide(q)], vec_recv.at[slot, q])

    def part_wait(slot, q):
        landed(part_in.at[slot, :, wide(q)], part_recv.at[slot, q])

    def vec_out(c, n, q):
        u = vec_to[c][n]
        slot = vec_from[u].index(c)
        here, to = (vec, vec_in.at[slot]) if q is None else (vec.at[:, wide(q)], vec_in.at[slot, :, wide(q)])
        return remote(here, to, vec_send.at[n], vec_recv.at[slot, 0 if q is None else q], there(u))

    def vec_outs(c, q, act):
        for n, u in enumerate(vec_to[c]):
            block = [jk for jk in blocks[u] if jk[1] == c][0]

            @pl.when(active(block))
            def _():
                act(vec_out(c, n, q))

    def lift_to(c):
        return [jk for u in range(columns) for jk in blocks[u] if crosses(jk) and jk[1] == c]

    def lift_out(block, r):
        j, k = block
        here, to = (vec, guest.at[a]) if r is None else (vec.at[few(r), :], guest.at[a, few(r), :])
        return remote(here, to, lift_send, guest_recv.at[a, 0 if r is None else r], level(helper(block), target_of(j, k)))

    def lift_back(block, q):
        j, k = block
        slot = part_from[j].index(k)
        here, to = (guest.at[top - 1], part_in.at[slot]) if q is None else (guest.at[top - 1, :, wide(q)], part_in.at[slot, :, wide(q)])
        return remote(here, to, lift_back_send, part_recv.at[slot, 0 if q is None else q], level(helped_level(block), j))

    def take_help(block):
        z = helped_level(block)
        for r in range(rounds):
            landed(guest.at[z, few(r), :], guest_recv.at[z, r])
        high, low = halves(guest[z])
        help_stack[:height] = high
        help_stack[height:] = low

    def help_piece(c, block, q):
        slot = blocks[c].index(block)
        total = jnp.zeros((height, WIDE), jnp.float32)
        for half in range(side):
            total += nt3(help_stack[:, half * part : (half + 1) * part], buf[slot, half, wide(q), :])
        guest[top - 1, :, wide(q)] = total
        lift_back(block, q).start()

    def part_to(block, made, q):
        j, k = block
        slot = part_from[j].index(k)
        here, to = (part_out.at[made], part_in.at[slot]) if q is None else (part_out.at[made, :, wide(q)], part_in.at[slot, :, wide(q)])
        return remote(here, to, part_send.at[made], part_recv.at[slot, 0 if q is None else q], there(j))

    def put(values):
        high, low = halves(values)
        stack[:height] = high
        stack[height:] = low

    def known(k):
        return k in vec_from[heir[k]]

    def guest_out(k, r):
        to = level(k, heir[k])
        j = [j for j, kk in staying if kk == k][0]
        if host_of(j, k) != j:
            to = (jnp.where(a < k, row, to[0]), jnp.where(a < k, j, to[1]))
        return remote(vec.at[few(r), :], guest.at[a, few(r), :], guest_send.at[r], guest_recv.at[a, r], to)

    def relay(j, k, r):
        here = guest.at[a] if r is None else guest.at[a, few(r), :]
        return remote(here, here, relay_send, guest_recv.at[a, 0 if r is None else r], level(k, host_of(j, k)))

    def own_back(j, k, q):
        slot = part_from[j].index(k)
        here, to = (guest_part.at[rounds], part_in.at[slot]) if q is None else (guest_part.at[rounds, :, wide(q)], part_in.at[slot, :, wide(q)])
        return remote(here, to, own_back_send, part_recv.at[slot, 0 if q is None else q], level(k, j))

    def visitors(j, k):
        return [z for z in range(groups) if z > k or z < k and host_of(j, k) == j] + relayed(j, k)

    def relayed(j, k):
        return [] if host_of(j, k) == j else list(range(k))

    def back(j, k, z, r):
        slot = part_from[j].index(k)
        n = visitors(j, k).index(z)
        here = guest_part.at[slice(0, rounds) if r is None else r, n * share : (n + 1) * share, :]
        return remote(here, here if r is None else part_in.at[slot, few(r), :], back_send.at[z], back_recv.at[slot], level(z, j))

    def products(rows, q):
        total = jnp.zeros((rows, WIDE), jnp.float32)
        for half in range(side):
            total += nt3(guest_stack[: 2 * rows, half * part : (half + 1) * part], stay[half, wide(q), :])
        return total

    def host(j, k):
        c = host_of(j, k)
        if c == j:
            stay_in().wait()
        for step in range(1 if c == j else 0, side):
            half = (b + step) % side
            landed(stay.at[half], stay_recv.at[half])
        for block in blocks[c]:

            @pl.loop(0, chunks)
            def _(i):
                side_flows(blocks[c].index(block), block, i, lambda copy: copy.start())

        away = [z for z in visitors(j, k) if z not in relayed(j, k)]
        tall_of = len(away) * share

        @pl.loop(0, rounds)
        def _(r):
            for n, z in enumerate(away):
                landed(guest.at[z, few(r), :], guest_recv.at[z, r])
                high, low = halves(guest[z, few(r), :])
                guest_stack[n * share : (n + 1) * share] = high
                guest_stack[tall_of + n * share : tall_of + (n + 1) * share] = low

            @pl.loop(0, pieces)
            def _(q):
                guest_part[r, :tall_of, wide(q)] = products(tall_of, q)

            for n, z in enumerate(away):
                back(j, k, z, r).start()

        if c == j:
            host_own(j, k)

    def relayed_in(j, k):
        for z in relayed(j, k):
            for r in range(rounds):
                landed(guest.at[z, few(r), :], guest_recv.at[z, r])
            high, low = halves(guest[z])
            help_stack[:height] = high
            help_stack[height:] = low

    def relayed_back(j, k, z, q):
        slot = part_from[j].index(k)
        here = guest.at[z] if q is None else guest.at[z, :, wide(q)]
        there_ref = here if q is None else part_in.at[slot, :, wide(q)]
        return remote(here, there_ref, relayed_send, part_recv.at[slot, 0 if q is None else q], level(z, j))

    def relayed_piece(j, k, q):
        for z in relayed(j, k):
            total = jnp.zeros((height, WIDE), jnp.float32)
            for half in range(side):
                total += nt3(help_stack[:, half * part : (half + 1) * part], stay[half, wide(q), :])
            guest[z, :, wide(q)] = total
            relayed_back(j, k, z, q).start()

    def host_own(j, k):
        c = host_of(j, k)
        if known(k):
            for q in range(pieces):
                vec_wait(vec_from[c].index(k), q)
            own = vec_in.at[vec_from[c].index(k)]
        else:
            for r in range(rounds):
                landed(guest.at[k, few(r), :], guest_recv.at[k, r])
            own = guest.at[k]
        high, low = halves(own[...])
        guest_stack[:height] = high
        guest_stack[height:] = low

        @pl.loop(0, pieces)
        def _(q):
            if c == j:
                part_in[part_from[j].index(k), :, wide(q)] = products(height, q)
            else:
                guest_part[rounds, :, wide(q)] = products(height, q)
                own_back(j, k, q).start()

    def make_part(c, block, q, left):
        slot, made = blocks[c].index(block), part_made[c].index(block)
        for n in range(WIDE // TALL):
            others(slot, block, q * (WIDE // TALL) + n)
        total = jnp.zeros((height, WIDE), jnp.float32)
        for half in range(side):
            total += nt3(left[:, half * part : (half + 1) * part], buf[slot, half, wide(q), :])
        part_out[made, :, wide(q)] = total
        part_to(block, made, q).start()

    per_half = part // WIDE

    def order(n):
        return lax.rem(n + jnp.where(a == 0, b * per_half, 0), pieces)

    def columns_of(o):
        return o // per_half, wide(lax.rem(o, per_half))

    def fold(slot):
        half, where = columns_of(order(pieces - 1))
        for n in range(pieces):
            upto = (n + 1) * WIDE
            high, low = halves(inverse[n * WIDE : upto, :upto])
            right, right_low = halves(buf[slot, half, :upto, where])
            total = jnp.dot(high, right, preferred_element_type=jnp.float32) + jnp.dot(low, right, preferred_element_type=jnp.float32)
            stay[0, n * WIDE : upto, :WIDE] = total + jnp.dot(high, right_low, preferred_element_type=jnp.float32)

    def folded(c):
        return [jk for jk in before[c] if both_down(jk)]

    def take_last(c):
        for block in folded(c):
            coming = vec_from[c].index(block[1])
            last = order(pieces - 1)
            vec_wait(coming, last)
            high, low = halves(vec_in[coming, :, wide(last)])
            stack[:height, :WIDE] = high
            stack[height:, :WIDE] = low
            sums[column] = jnp.zeros((8, height), jnp.float32)

            @pl.loop(0, pieces)
            def _(n):
                done = vec[:, wide(n)] - nt3(stack[:, :WIDE], stay[0, wide(n), :WIDE])
                vec[:, wide(n)] = done
                high, low = halves(done * done)
                sums[column] += nt(ones[...], high) + nt(ones[...], low)

    def take_before(c):
        for block in before[c]:
            j, k = block
            slot, coming = blocks[c].index(block), vec_from[c].index(k)
            if both_down(block):
                serving(c, early(columns - 3), lambda block: chunks)

                @pl.when((a <= k) & (a > 0))
                def _():
                    @pl.loop(0, chunks)
                    def _(i):
                        serve_others(slot, block, i)

                def others_in():
                    @pl.loop(0, chunks)
                    def _(i):
                        others(slot, block, i)

                pl.when(a > 0)(others_in)
                for jj, kk in staying:
                    if jj == c and host_of(jj, kk) != c:

                        @pl.when(a < kk)
                        def _():
                            for r in range(rounds):
                                landed(guest.at[a, few(r), :], guest_recv.at[a, r])
                                relay(jj, kk, r).start()

                for n in range(pieces - 1):
                    if n == per_half:
                        pl.when(a == 0)(others_in)
                        fold(slot)
                    o = order(n)
                    vec_wait(coming, o)
                    high, low = halves(vec_in[coming, :, wide(o)])
                    stack[:height, :WIDE] = high
                    stack[height:, :WIDE] = low
                    half, where = columns_of(o)

                    @pl.loop(0, pieces)
                    def _(m):
                        rest[:, wide(m)] -= nt3(stack[:, :WIDE], buf[slot, half, wide(m), where])
            elif j != c:
                serving(c, early(columns - 3), lambda block: chunks)
                for jj, kk in staying:
                    if host_of(jj, kk) == c:
                        pl.when(a == kk)(functools.partial(host, jj, kk))
                        pl.when(a == kk)(functools.partial(relayed_in, jj, kk))

                def work():
                    for q in range(pieces):
                        vec_wait(coming, q)

                pl.when(active(block) & (a != k) if c == heir[k] else active(block))(work)

                @pl.when(active(block))
                def _():
                    high, low = halves(vec_in[coming])
                    guest_stack[:height] = high
                    guest_stack[height:] = low

                pl.when(helping(block))(functools.partial(take_help, block))
            else:
                serving(c, early(columns - 3), early(columns - 2))
                for q in range(pieces):
                    vec_wait(coming, q)
                put(vec_in[coming])

                @pl.loop(0, pieces)
                def _(q):
                    @pl.when(a != k)
                    def _():
                        serve_ahead(slot, block, q, early(columns - 2)(block))

                    for u in range(columns):
                        for jj, kk in after[u]:
                            if kk == c:

                                @pl.when((a == kk) & (q == (chunks - EARLY[columns - 2] + 1) * TALL // WIDE + 1))
                                def _():
                                    pl.semaphore_signal(gate, inc=1, device_id=there(u), device_id_type=MESH)

                    for n in range(WIDE // TALL):
                        others(slot, block, q * (WIDE // TALL) + n)
                    total = jnp.zeros((height, WIDE), jnp.float32)
                    for half in range(side):
                        total += nt3(stack[:, half * part : (half + 1) * part], buf[slot, half, wide(q), :])
                    rest[:, wide(q)] -= total

    inverse_load.wait()
    for c in range(columns):
        if before[c]:
            on(c, functools.partial(take_before, c))

    squares = jnp.zeros((8, height), jnp.float32)
    for q in range(pieces):
        here = slice(q * WIDE, (q + 1) * WIDE)
        for c in range(columns):
            for block in before[c]:
                if block[0] != c:

                    def give(c=c, block=block):
                        @pl.when(active(block))
                        def _():
                            make_part(c, block, q, guest_stack)

                        @pl.when(helping(block))
                        def _():
                            help_piece(c, block, q)

                        for j, k in staying:
                            if relayed(j, k) and host_of(j, k) == c:
                                pl.when(a == k)(functools.partial(relayed_piece, j, k, q))

                    on(c, give)
            if part_from[c]:

                def work(c=c):
                    for slot, k in enumerate(part_from[c]):
                        if (c, k) not in staying:
                            part_wait(slot, q)
                        else:

                            def back_wait(slot=slot):
                                landed(part_in.at[slot], back_recv.at[slot])

                            if q == 0:
                                pl.when(a != k if host_of(c, k) == c else a > k)(back_wait)
                            if host_of(c, k) != c:
                                pl.when(a <= k)(functools.partial(part_wait, slot, q))

                        rest[:, here] -= part_in[slot, :, here]

                on(c, work)
        high, low = halves(rest[:, here])
        stack[:height, here] = high
        stack[height:, here] = low
        done = nt3(stack[:, : (q + 1) * WIDE], inverse[here, : (q + 1) * WIDE])
        vec[:, here] = done
        high, low = halves(done * done)
        squares += nt(ones[...], high) + nt(ones[...], low)
        for c in range(columns):
            if vec_to[c]:

                on(c, functools.partial(vec_outs, c, q, lambda copy: copy.start()))

    def guest_round(c, r):
        def work():
            if r:
                guest_out(c, r - 1).wait_send()
            if r < rounds:
                guest_out(c, r).start()

        if known(c) or not after[c]:
            pl.when(a != c)(work)
        else:
            work()

    def guests(c):
        for block in lift_to(c):

            @pl.when(jnp.logical_not(active(block)))
            def _():
                for r in range(rounds):
                    lift_out(block, r).start()

        if heir[c] is not None:
            if not known(c) and not after[c]:

                @pl.when(a == c)
                def _():
                    for r in range(rounds):
                        guest_out(c, r).start()
                    for r in range(rounds):
                        guest_out(c, r).wait_send()

            for r in range(1 if after[c] else rounds + 1):
                guest_round(c, r)

    for c in range(columns):
        on(c, functools.partial(guests, c))
    sums[column] = squares
    for c in range(columns):
        if folded(c):
            on(c, functools.partial(take_last, c))
    store = pltpu.make_async_copy(vec, out_ref, out_sem)
    store.start()

    def sum_out(step):
        to = (column + step) % columns
        return remote(sums.at[column], sums.at[column], sum_send.at[step - 1], sum_recv.at[column], there(to))

    for step in range(1, columns):
        sum_out(step).start()

    for j, k in staying:
        if host_of(j, k) != j:

            @pl.when((column == host_of(j, k)) & (a == k))
            def _():
                host_own(j, k)


    def give_after(c):
        for block in after[c]:
            j, k = block
            slot, coming = blocks[c].index(block), vec_from[c].index(k)

            if heir[c] is not None:
                for r in range(1, rounds + 1):
                    guest_round(c, r)

                    @pl.when(a == k)
                    def _():
                        if r == 1:
                            pl.semaphore_wait(gate, 1)

                    @pl.when(active(block))
                    def _():
                        @pl.loop((r - 1) * LATER // rounds, r * LATER // rounds)
                        def _(i):
                            serve(slot, block, i)

            @pl.when(active(block))
            def _():
                for q in range(pieces):
                    vec_wait(coming, q)
                put(vec_in[coming])
                pl.when(helping(block))(functools.partial(take_help, block))

                @pl.loop(0, pieces)
                def _(q):
                    serve_ahead(slot, block, q, LATER)
                    make_part(c, block, q, stack)

                    @pl.when(helping(block))
                    def _():
                        help_piece(c, block, q)

    for c in range(columns):
        if after[c]:
            on(c, functools.partial(give_after, c))

    def sent(copy):
        copy.wait_send()

    for d in range(chips):
        slab_out(d).wait_send()
    for d in range(1, chips):
        slab_pass(d).wait_send()
    for j, k in all_blocks:
        t = target_of(j, k)
        if t is not None and t != j:

            @pl.when((column == j) & (a == k))
            def _():
                entry(blocks[t].index((j, k)), None, t).wait_send()

    for j, k in staying:
        c = host_of(j, k)

        @pl.when((column == j) & (a == k))
        def _():
            for step in range(0 if c != j else 1, side):
                stay_out(step, None, c).wait_send()

        if relayed(j, k):

            @pl.when((column == j) & (a < k))
            def _():
                relay(j, k, None).wait_send()

        @pl.when((column == c) & (a == k))
        def _():
            for z in visitors(j, k):
                if z in relayed(j, k):
                    relayed_back(j, k, z, None).wait_send()
                else:
                    back(j, k, z, None).wait_send()
            if c != j:
                own_back(j, k, None).wait_send()

    for c in range(columns):

        def work(c=c):
            for slot, block in enumerate(blocks[c]):
                line_flows(slot, block, None, sent)
                side_flows(slot, block, None, sent)
                if both_down(block):
                    other_flows(slot, block, None, sent)
            vec_outs(c, None, sent)
            for made, block in enumerate(part_made[c]):

                @pl.when(active(block))
                def _():
                    part_to(block, made, None).wait_send()

                @pl.when(helping(block))
                def _():
                    lift_back(block, None).wait_send()

            for block in lift_to(c):

                @pl.when(jnp.logical_not(active(block)))
                def _():
                    lift_out(block, None).wait_send()

        on(c, work)
    for step in range(1, columns):
        other = (column + step) % columns
        landed(sums.at[other], sum_recv.at[other])
    total = sums[0]
    for c in range(1, columns):
        total += sums[c]
    mean_ref[...] = total[:1] / (width * columns)
    for step in range(1, columns):
        sum_out(step).wait_send()
    store.wait()


def chain_device(slab, factor, block_inverse, pivot_order, row_count):
    height, width = slab.shape
    depth, part = factor.shape
    groups = lax.axis_size("cols")
    side = lax.axis_size("rows") // groups
    column = lax.axis_index("cols")
    slots = max([sum(target_of(j, k) == c for j in range(groups) for k in range(j)) for c in range(groups)])
    chunks, pieces, rounds, chips = depth // TALL, width // WIDE, groups - 1, groups // 2
    sem, space = pltpu.SemaphoreType.DMA, pltpu.VMEM
    f32, bf16 = jnp.float32, jnp.bfloat16
    held = pl.BlockSpec(memory_space=pltpu.VMEM)
    away = pl.BlockSpec(memory_space=pl.ANY)
    vectors, mean = pl.pallas_call(
        functools.partial(chain_kernel, groups, side),
        out_shape=(jax.ShapeDtypeStruct((height, width), f32), jax.ShapeDtypeStruct((1, height), f32)),
        in_specs=[away, away, away, held, pl.BlockSpec(memory_space=pltpu.SMEM)],
        out_specs=(away, held),
        scratch_shapes=[
            space((slots, side, depth, part), f32),
            space((width, width), f32),
            space((groups, height, width), f32),
            space((height, width), f32),
            space((height, width), f32),
            space((2 * height, width), bf16),
            space((1, height, width), f32),
            space((groups - 2, height, width), f32),
            space((1, height, width), f32),
            space((groups, 8, height), f32),
            space((8, WIDE), bf16),
            space((side, depth, part), f32),
            space((groups, height, width), f32),
            space((2 * height, width), bf16),
            space((rounds + 1, height, width), f32),
            space((2 * height, width), bf16),
            sem((chunks,)),
            sem((slots, side, chunks)),
            sem((slots,)),
            sem((slots, side)),
            sem((side - 1, slots)),
            sem(()),
            sem(()),
            sem(()),
            sem((chips,)),
            sem((groups,)),
            sem((chips - 1,)),
            sem((groups - 2,)),
            sem((1, pieces)),
            sem((1,)),
            sem((groups - 2, pieces)),
            sem((groups,)),
            sem((groups,)),
            sem(()),
            sem(()),
            sem((side,)),
            sem((side,)),
            sem((rounds,)),
            sem((groups, rounds)),
            sem((groups,)),
            sem((groups - 2,)),
            sem(()),
            sem(()),
            sem(()),
            sem(()),
            sem(()),
            pltpu.SemaphoreType.REGULAR,
        ],
        compiler_params=pltpu.CompilerParams(collective_id=0, has_side_effects=True, vmem_limit_bytes=57000 * 1024),
    )(slab, factor, block_inverse, pivot_order[None, :], row_count)
    return vectors, mean[0]


def per_device(slab, factor, block_inverse, pivot_order, row_count):
    groups, rows = lax.axis_size("cols"), lax.axis_size("rows")
    depth, part = factor.shape
    fits = groups // 2 == 2 and rows % groups == 0 and rows > groups and part % WIDE == 0 and depth % WIDE == 0 and slab.shape[0] % (8 * (groups - 1)) == 0
    one = chain_device if fits else plain_device
    return one(slab, factor, block_inverse, pivot_order, row_count)


def solution(mesh):
    placed = (P("rows", "cols"), P("cols", "rows"), P("cols", None), P(), P("rows"))
    return jax.shard_map(
        per_device,
        mesh=mesh,
        in_specs=placed,
        out_specs=(P("rows", "cols"), P("rows")),
        check_vma=False,
    )
```

```python
import functools
import jax
import jax.numpy as jnp
from jax import lax
from jax.experimental import pallas as pl
from jax.experimental.pallas import tpu as pltpu
from jax.sharding import PartitionSpec as P

MESH = pl.DeviceIdType.MESH


def times_transposed(left, right):
    return lax.dot_general(
        left,
        right,
        (((1,), (1,)), ((), ())),
        precision=lax.Precision.HIGH,
        preferred_element_type=jnp.float32,
    )


def gather_kernel(groups, side, chunks, part_ref, row_ref, mine, in_sem, keep_sem, right_sem, left_sem, hop_sem, side_sem, cross_sem):
    row, column = lax.axis_index("rows"), lax.axis_index("cols")
    a, b = row // side, row % side
    depth, width = part_ref.shape
    tall = depth // chunks

    def at(a_to, b_to):
        return (a_to * side + b_to, column)

    barrier = pltpu.get_barrier_semaphore()
    for step in (1, groups - 1):
        pl.semaphore_signal(barrier, inc=1, device_id=at((a + step) % groups, b), device_id_type=MESH)
    for step in range(1, side):
        pl.semaphore_signal(barrier, inc=1, device_id=at(a, (b + step) % side), device_id_type=MESH)
    pl.semaphore_wait(barrier, 2 + side - 1)

    def rows_of(i):
        return pl.ds(pl.multiple_of(i * tall, tall), tall)

    def place(k, b_of, i):
        return row_ref.at[k * side + b_of, rows_of(i), :]

    def right(k, i, source):
        return pltpu.make_async_remote_copy(source, place(k, b, i), right_sem.at[k, i], hop_sem.at[k, i], device_id=at(jnp.minimum(a + 1, groups - 1), b), device_id_type=MESH)

    def left(k, i, source):
        return pltpu.make_async_remote_copy(source, place(k, b, i), left_sem.at[k, i], hop_sem.at[k, i], device_id=at(jnp.maximum(a - 1, 0), b), device_id_type=MESH)

    def across(k, step, i, source):
        return pltpu.make_async_remote_copy(source, place(k, b, i), side_sem.at[step - 1, k, i], cross_sem.at[step - 1, k, i], device_id=at(a, (b + step) % side), device_id_type=MESH)

    def load(i):
        return pltpu.make_async_copy(part_ref.at[rows_of(i), :], mine.at[rows_of(i), :], in_sem.at[i])

    def keep(i):
        return pltpu.make_async_copy(mine.at[rows_of(i), :], place(a, b, i), keep_sem.at[i])

    @pl.when(a < column)
    def _():
        @pl.loop(0, chunks)
        def _(i):
            load(i).start()

        @pl.loop(0, chunks)
        def _(i):
            source = mine.at[rows_of(i), :]
            load(i).wait()

            @pl.when(a < groups - 1)
            def _():
                right(a, i, source).start()

            @pl.when(a > 0)
            def _():
                left(a, i, source).start()

            for step in range(1, side):
                across(a, step, i, source).start()
            keep(i).start()

    for hop in range(1, groups):
        @pl.loop(0, chunks)
        def _(i):
            k = a - hop

            @pl.when((k >= 0) & (k < column))
            def _():
                source = place(k, b, i)
                right(k, i, source).wait_recv()

                @pl.when(a < groups - 1)
                def _():
                    right(k, i, source).start()

                for step in range(1, side):
                    across(k, step, i, source).start()

            h = a + hop

            @pl.when((h <= groups - 1) & (h < column))
            def _():
                source = place(h, b, i)
                left(h, i, source).wait_recv()

                @pl.when(a > 0)
                def _():
                    left(h, i, source).start()

                for step in range(1, side):
                    across(h, step, i, source).start()

    for k in range(groups - 1):
        @pl.when(k < column)
        def _():
            @pl.loop(0, chunks)
            def _(i):
                source = place(k, b, i)
                for step in range(1, side):
                    came = place(k, (b + side - step) % side, i)
                    pltpu.make_async_remote_copy(came, came, side_sem.at[step - 1, k, i], cross_sem.at[step - 1, k, i], device_id=at(a, (b + step) % side), device_id_type=MESH).wait_recv()
                    across(k, step, i, source).wait_send()

                @pl.when((k <= a) & (a < groups - 1))
                def _():
                    right(k, i, source).wait_send()

                @pl.when((k >= a) & (a > 0))
                def _():
                    left(k, i, source).wait_send()

                @pl.when(k == a)
                def _():
                    keep(i).wait()


def gather_factor(factor, rows, groups):
    side = rows // groups
    depth, width = factor.shape
    chunks = max(1, depth // 256)
    sem = pltpu.SemaphoreType.DMA
    return pl.pallas_call(
        functools.partial(gather_kernel, groups, side, chunks),
        out_shape=jax.ShapeDtypeStruct(((groups - 1) * side, depth, width), jnp.float32),
        in_specs=[pl.BlockSpec(memory_space=pl.ANY)],
        out_specs=pl.BlockSpec(memory_space=pl.ANY),
        scratch_shapes=[
            pltpu.VMEM((depth, width), jnp.float32),
            sem((chunks,)),
            sem((chunks,)),
            sem((groups, chunks)),
            sem((groups, chunks)),
            sem((groups, chunks)),
            sem((side - 1, groups, chunks)),
            sem((side - 1, groups, chunks)),
        ],
        compiler_params=pltpu.CompilerParams(collective_id=0, has_side_effects=True, vmem_limit_bytes=60000 * 1024),
        cost_estimate=pl.CostEstimate(flops=0, bytes_accessed=600000000, transcendentals=0),
    )(factor)


def plain_device(slab, factor, block_inverse, pivot_order, row_count):
    rows_here, block_width = slab.shape
    row_devices = lax.axis_size("rows")
    column_count = lax.axis_size("cols")
    column = lax.axis_index("cols")
    total_width = block_width * column_count
    side = row_devices // column_count
    chosen = lax.dynamic_slice_in_dim(pivot_order, column * block_width, block_width)
    gathered = lax.all_gather(slab, "cols", axis=1, tiled=True)
    parts = gather_factor(factor, row_devices, column_count)
    gathered, parts = lax.optimization_barrier((gathered, parts))
    ordered = jnp.take(gathered, chosen, axis=1)
    live_rows = jnp.arange(rows_here, dtype=jnp.int32) < row_count[0]
    pending = jnp.where(live_rows[:, None], ordered, jnp.float32(0.0))

    def finish(values):
        return times_transposed(values, block_inverse)

    def nothing(values):
        return jnp.zeros_like(values)

    width = factor.shape[1]
    vectors = jnp.zeros_like(pending)
    for k in range(column_count):
        finished = lax.cond(column == k, finish, nothing, pending)
        vectors = vectors + finished
        if k + 1 < column_count:
            arrived = moving = finished
            for to in range(k + 1, column_count):
                moving = lax.ppermute(moving, "cols", [(to - 1, to)])
                arrived = jnp.where(column == to, moving, arrived)
            update = jnp.zeros_like(pending)
            for b in range(side):
                update += times_transposed(arrived[:, b * width : (b + 1) * width], parts[k * side + b])
            pending = pending - jnp.where(k < column, update, jnp.float32(0.0))
    row_sums = lax.psum(jnp.sum(vectors * vectors, axis=1), "cols")
    return (vectors, row_sums / total_width)


TALL = 128
WIDE = 256
EARLY = (5, 7, 9)
LATER = 4


def target_of(j, k):
    if k == j - 1:
        return j if j % 2 else j - 2
    return j - 1 if j % 2 and k == 0 else None


def host_of(j, k):
    return j - 1 if j % 2 else j


def halves(values):
    high = values.astype(jnp.bfloat16)
    return high, (values - high.astype(jnp.float32)).astype(jnp.bfloat16)


def nt(left, right):
    return lax.dot_general(left, right, (((1,), (1,)), ((), ())), preferred_element_type=jnp.float32)


def nt3(stacked, right):
    rows = stacked.shape[0] // 2
    high, low = halves(right)
    both = nt(stacked, high)
    return both[:rows] + (both[rows:] + nt(stacked[:rows], low))


def chain_kernel(
    groups,
    side,
    slab_ref,
    factor_ref,
    inverse_ref,
    order_ref,
    count_ref,
    out_ref,
    mean_ref,
    buf,
    inverse,
    slabs,
    rest,
    vec,
    stack,
    vec_in,
    part_in,
    part_out,
    sums,
    ones,
    stay,
    guest,
    guest_stack,
    guest_part,
    help_stack,
    load_sem,
    recv_sem,
    up_sem,
    down_sem,
    side_sem,
    entry_sem,
    inverse_sem,
    own_sem,
    slab_send,
    slab_recv,
    pass_send,
    vec_send,
    vec_recv,
    part_send,
    part_recv,
    sum_send,
    sum_recv,
    out_sem,
    stay_load,
    stay_send,
    stay_recv,
    guest_send,
    guest_recv,
    back_send,
    back_recv,
    lift_send,
    lift_back_send,
    relayed_send,
    relay_send,
    own_back_send,
    gate,
):
    columns = groups
    row, column = lax.axis_index("rows"), lax.axis_index("cols")
    a, b = row // side, row % side
    height, width = rest.shape
    depth, part = factor_ref.shape
    chunks = depth // TALL
    pieces = width // WIDE
    rounds = groups - 1
    share = height // rounds
    chips = columns // 2
    chip, core = column // 2, column % 2
    all_blocks = [(j, k) for j in range(1, columns) for k in range(j)]
    moving = [jk for jk in all_blocks if target_of(*jk) is not None]
    staying = [jk for jk in all_blocks if target_of(*jk) is None]
    blocks = [[jk for jk in moving if target_of(*jk) == c] for c in range(columns)]
    before = [[jk for jk in blocks[c] if jk[1] < c] for c in range(columns)]
    after = [[jk for jk in blocks[c] if jk[1] > c] for c in range(columns)]
    heir = [host_of(*[jk for jk in staying if jk[1] == k][0]) if [jk for jk in staying if jk[1] == k] else None for k in range(columns)]
    hosted = [[k for j, k in staying if host_of(j, k) == c] for c in range(columns)]
    vec_from = [sorted({k for _, k in blocks[c] if k != c}) for c in range(columns)]
    vec_to = [[u for u in range(columns) if c in vec_from[u]] for c in range(columns)]
    part_from = [[k for k in range(c) if target_of(c, k) != c] for c in range(columns)]
    part_made = [[jk for jk in blocks[c] if jk[0] != c] for c in range(columns)]

    def there(c):
        return (row, c)

    def level(z, c):
        return (z * side + b, c)

    def beside(step):
        return (a * side + (b + step) % side, column)

    def remote(source, target, send, recv, device):
        return pltpu.make_async_remote_copy(source, target, send, recv, device_id=device, device_id_type=MESH)

    def landed(here, recv):
        remote(here, here, out_sem, recv, there(column)).wait_recv()

    def tall(i):
        return pl.ds(pl.multiple_of(i * TALL, TALL), TALL)

    def wide(q):
        return pl.ds(pl.multiple_of(q * WIDE, WIDE), WIDE)

    def few(r):
        return pl.ds(pl.multiple_of(r * share, share), share)

    def on(c, work):
        pl.when(column == c)(work)

    barrier = pltpu.get_barrier_semaphore()
    for step in range(1, side):
        pl.semaphore_signal(barrier, inc=1, device_id=beside(step), device_id_type=MESH)
        for right_by in range(1, columns):
            pl.semaphore_signal(barrier, inc=1, device_id=(a * side + (b + step) % side, (column + right_by) % columns), device_id_type=MESH)
    for up_by in range(groups):
        for right_by in range(columns):
            if up_by or right_by:
                pl.semaphore_signal(barrier, inc=1, device_id=level((a + up_by) % groups, (column + right_by) % columns), device_id_type=MESH)
    pl.semaphore_wait(barrier, (side - 1) * columns + groups * columns - 1)

    def source_of(d, f):
        return (chip + d) % chips * 2 + (core + f) % 2

    partner = source_of(0, 1)
    own_load = pltpu.make_async_copy(slab_ref, slabs.at[column], own_sem)
    own_load.start()
    inverse_load = pltpu.make_async_copy(inverse_ref, inverse, inverse_sem)

    def slab_out(d):
        to = source_of(d, 0) if d else partner
        return remote(slab_ref, slabs.at[column], slab_send.at[d], slab_recv.at[column], there(to))

    def slab_pass(d):
        place = slabs.at[source_of(d, 0)]
        return remote(place, place, pass_send.at[d - 1], slab_recv.at[source_of(d, 0)], there(partner))

    for d in list(range(1, chips)) + [0]:
        slab_out(d).start()

    def place(slot, half, i):
        return buf.at[slot, half] if i is None else buf.at[slot, half, tall(i), :]

    def came(slot, half, i):
        return recv_sem.at[slot, half, 0 if i is None else i]

    def load(slot, i):
        return pltpu.make_async_copy(factor_ref.at[tall(i), :], place(slot, b, i), load_sem.at[i])

    def entry(slot, i, to):
        return remote(factor_ref if i is None else factor_ref.at[tall(i), :], place(slot, b, i), entry_sem, came(slot, b, i), there(to))

    def up(slot, i):
        return remote(place(slot, b, i), place(slot, b, i), up_sem.at[slot], came(slot, b, i), level(jnp.minimum(a + 1, groups - 1), column))

    def down(slot, half, i):
        return remote(place(slot, half, i), place(slot, half, i), down_sem.at[slot, half], came(slot, half, i), level(jnp.maximum(a - 1, 0), column))

    def across(slot, step, i):
        return remote(place(slot, b, i), place(slot, b, i), side_sem.at[step - 1, slot], came(slot, b, i), beside(step))

    def arrived(slot, half, i):
        landed(place(slot, half, i), recv_sem.at[slot, half, i])

    def both_down(block):
        return block[1] >= 2

    def lifted(block):
        return block[0] % 2 == 0

    top = groups - 1

    def crosses(block):
        return target_of(*block) != block[0]

    def active(block):
        if not crosses(block):
            return a >= 0
        return a >= block[1] if lifted(block) else a < top

    def helper(block):
        return block[1] if lifted(block) else top - 1

    def helped_level(block):
        return block[1] - 1 if lifted(block) else top

    def helping(block):
        return a == helper(block)

    def free_level(block):
        return functools.reduce(jnp.logical_and, [a != k for k in hosted[target_of(*block)]], a >= 0)

    def line_flows(slot, block, i, act):
        k = block[1]

        @pl.when((a >= k) & (a < (top - 1 if crosses(block) and not lifted(block) else top)))
        def _():
            act(up(slot, i))

        if not lifted(block):

            @pl.when((a <= k) & (a > 0))
            def _():
                act(down(slot, b, i))

    def side_flows(slot, block, i, act):
        @pl.when((a >= block[1]) if both_down(block) else active(block))
        def _():
            for step in range(1, side):
                act(across(slot, step, i))

    def other_flows(slot, block, i, act):
        @pl.when((a <= block[1]) & (a > 0))
        def _():
            for step in range(1, side):
                act(down(slot, (b + step) % side, i))

    def serve(slot, block, i):
        j, k = block
        if target_of(j, k) == j:

            @pl.when(a == k)
            def _():
                load(slot, i).wait()

            @pl.when(a != k)
            def _():
                arrived(slot, b, i)
        else:
            arrived(slot, b, i)
        line_flows(slot, block, i, lambda copy: copy.start())

        @pl.when(free_level(block))
        def _():
            side_flows(slot, block, i, lambda copy: copy.start())


    def serve_ahead(slot, block, q, ahead):
        for n in range(WIDE // TALL):
            i = ahead + q * (WIDE // TALL) + n

            @pl.when(i < chunks)
            def _():
                serve(slot, block, i)

    def serve_others(slot, block, i):
        for step in range(1, side):
            arrived(slot, (b + step) % side, i)
        other_flows(slot, block, i, lambda copy: copy.start())

    def others(slot, block, i):
        def work():
            for step in range(1, side):
                arrived(slot, (b + step) % side, i)

        if both_down(block):
            pl.when((a > block[1]) | (a == 0))(work)
        else:
            work()

    def stay_out(step, q, to):
        here = factor_ref if q is None else factor_ref.at[wide(q), :]
        return remote(here, stay.at[b] if q is None else stay.at[b, wide(q), :], stay_send.at[step], stay_recv.at[b], (a * side + (b + step) % side, to))

    def stay_in():
        return pltpu.make_async_copy(factor_ref, stay.at[b], stay_load)

    for j, k in all_blocks:
        t = target_of(j, k)

        @pl.when((column == j) & (a == k))
        def _():
            if t is None:
                for step in range(0 if host_of(j, k) != j else 1, side):
                    for q in range(pieces):
                        stay_out(step, q, host_of(j, k)).start()
                if host_of(j, k) == j:
                    stay_in().start()
            else:
                slot = blocks[t].index((j, k))

                @pl.loop(0, chunks)
                def _(i):
                    if t == j:
                        load(slot, i).start()
                    else:
                        entry(slot, i, t).start()

    inverse_load.start()

    rest[...] = jnp.zeros_like(rest)
    live = lax.broadcasted_iota(jnp.int32, (height, 1), 0) < count_ref[0]
    ones[...] = jnp.ones_like(ones)

    def serving(c, low, high):
        for block in before[c]:

            def work(block=block):
                @pl.loop(low(block), high(block))
                def _(i):
                    serve(blocks[c].index(block), block, i)

            pl.when((a != block[1]) & active(block))(work)

    def early(n):
        return lambda block: jnp.maximum(EARLY[n] - jnp.abs(a - block[1]), 0)

    def serve_source(c):
        for block in before[c]:

            def work(block=block):
                @pl.loop(0, chunks)
                def _(i):
                    serve(blocks[c].index(block), block, i)

            pl.when(a == block[1])(work)

    for c in range(columns):
        if before[c]:
            on(c, functools.partial(serve_source, c))
    for turn in range(columns):
        d, f = turn // 2, turn % 2
        s = source_of(d, f)
        if turn >= 2:
            for c in range(columns):
                if before[c]:
                    on(c, functools.partial(serving, c, early(turn - 3) if turn > 2 else lambda block: 0, early(turn - 2)))
        if turn == 0:
            own_load.wait()
        else:
            landed(slabs.at[s], slab_recv.at[s])
            if f == 0:
                slab_pass(d).start()
        high, low = halves(jnp.where(live, slabs[s], 0.0))
        stack[:height] = high
        stack[height:] = low

        @pl.loop(0, pieces)
        def _(q):
            index = lax.broadcasted_iota(jnp.int32, (width, WIDE), 0) + s * width
            chosen = jnp.where(index == order_ref[:, pl.ds(pl.multiple_of(column * width + q * WIDE, WIDE), WIDE)], 1.0, 0.0).astype(jnp.bfloat16)
            both = jnp.dot(stack[...], chosen, preferred_element_type=jnp.float32)
            rest[:, wide(q)] += both[:height] + both[height:]

    def vec_wait(slot, q):
        landed(vec_in.at[slot, :, wide(q)], vec_recv.at[slot, q])

    def part_wait(slot, q):
        landed(part_in.at[slot, :, wide(q)], part_recv.at[slot, q])

    def vec_out(c, n, q):
        u = vec_to[c][n]
        slot = vec_from[u].index(c)
        here, to = (vec, vec_in.at[slot]) if q is None else (vec.at[:, wide(q)], vec_in.at[slot, :, wide(q)])
        return remote(here, to, vec_send.at[n], vec_recv.at[slot, 0 if q is None else q], there(u))

    def vec_outs(c, q, act):
        for n, u in enumerate(vec_to[c]):
            block = [jk for jk in blocks[u] if jk[1] == c][0]

            @pl.when(active(block))
            def _():
                act(vec_out(c, n, q))

    def lift_to(c):
        return [jk for u in range(columns) for jk in blocks[u] if crosses(jk) and jk[1] == c]

    def lift_out(block, r):
        j, k = block
        here, to = (vec, guest.at[a]) if r is None else (vec.at[few(r), :], guest.at[a, few(r), :])
        return remote(here, to, lift_send, guest_recv.at[a, 0 if r is None else r], level(helper(block), target_of(j, k)))

    def lift_back(block, q):
        j, k = block
        slot = part_from[j].index(k)
        here, to = (guest.at[top - 1], part_in.at[slot]) if q is None else (guest.at[top - 1, :, wide(q)], part_in.at[slot, :, wide(q)])
        return remote(here, to, lift_back_send, part_recv.at[slot, 0 if q is None else q], level(helped_level(block), j))

    def take_help(block):
        z = helped_level(block)
        for r in range(rounds):
            landed(guest.at[z, few(r), :], guest_recv.at[z, r])
        high, low = halves(guest[z])
        help_stack[:height] = high
        help_stack[height:] = low

    def help_piece(c, block, q):
        slot = blocks[c].index(block)
        total = jnp.zeros((height, WIDE), jnp.float32)
        for half in range(side):
            total += nt3(help_stack[:, half * part : (half + 1) * part], buf[slot, half, wide(q), :])
        guest[top - 1, :, wide(q)] = total
        lift_back(block, q).start()

    def part_to(block, made, q):
        j, k = block
        slot = part_from[j].index(k)
        here, to = (part_out.at[made], part_in.at[slot]) if q is None else (part_out.at[made, :, wide(q)], part_in.at[slot, :, wide(q)])
        return remote(here, to, part_send.at[made], part_recv.at[slot, 0 if q is None else q], there(j))

    def put(values):
        high, low = halves(values)
        stack[:height] = high
        stack[height:] = low

    def known(k):
        return k in vec_from[heir[k]]

    def guest_out(k, r):
        to = level(k, heir[k])
        j = [j for j, kk in staying if kk == k][0]
        if host_of(j, k) != j:
            to = (jnp.where(a < k, row, to[0]), jnp.where(a < k, j, to[1]))
        return remote(vec.at[few(r), :], guest.at[a, few(r), :], guest_send.at[r], guest_recv.at[a, r], to)

    def relay(j, k, r):
        here = guest.at[a] if r is None else guest.at[a, few(r), :]
        return remote(here, here, relay_send, guest_recv.at[a, 0 if r is None else r], level(k, host_of(j, k)))

    def own_back(j, k, q):
        slot = part_from[j].index(k)
        here, to = (guest_part.at[rounds], part_in.at[slot]) if q is None else (guest_part.at[rounds, :, wide(q)], part_in.at[slot, :, wide(q)])
        return remote(here, to, own_back_send, part_recv.at[slot, 0 if q is None else q], level(k, j))

    def visitors(j, k):
        return [z for z in range(groups) if z > k or z < k and host_of(j, k) == j] + relayed(j, k)

    def relayed(j, k):
        return [] if host_of(j, k) == j else list(range(k))

    def back(j, k, z, r):
        slot = part_from[j].index(k)
        n = visitors(j, k).index(z)
        here = guest_part.at[slice(0, rounds) if r is None else r, n * share : (n + 1) * share, :]
        return remote(here, here if r is None else part_in.at[slot, few(r), :], back_send.at[z], back_recv.at[slot], level(z, j))

    def products(rows, q):
        total = jnp.zeros((rows, WIDE), jnp.float32)
        for half in range(side):
            total += nt3(guest_stack[: 2 * rows, half * part : (half + 1) * part], stay[half, wide(q), :])
        return total

    def host(j, k):
        c = host_of(j, k)
        if c == j:
            stay_in().wait()
        for step in range(1 if c == j else 0, side):
            half = (b + step) % side
            landed(stay.at[half], stay_recv.at[half])
        for block in blocks[c]:

            @pl.loop(0, chunks)
            def _(i):
                side_flows(blocks[c].index(block), block, i, lambda copy: copy.start())

        away = [z for z in visitors(j, k) if z not in relayed(j, k)]
        tall_of = len(away) * share

        @pl.loop(0, rounds)
        def _(r):
            for n, z in enumerate(away):
                landed(guest.at[z, few(r), :], guest_recv.at[z, r])
                high, low = halves(guest[z, few(r), :])
                guest_stack[n * share : (n + 1) * share] = high
                guest_stack[tall_of + n * share : tall_of + (n + 1) * share] = low

            @pl.loop(0, pieces)
            def _(q):
                guest_part[r, :tall_of, wide(q)] = products(tall_of, q)

            for n, z in enumerate(away):
                back(j, k, z, r).start()

        if c == j:
            host_own(j, k)

    def relayed_in(j, k):
        for z in relayed(j, k):
            for r in range(rounds):
                landed(guest.at[z, few(r), :], guest_recv.at[z, r])
            high, low = halves(guest[z])
            help_stack[:height] = high
            help_stack[height:] = low

    def relayed_back(j, k, z, q):
        slot = part_from[j].index(k)
        here = guest.at[z] if q is None else guest.at[z, :, wide(q)]
        there_ref = here if q is None else part_in.at[slot, :, wide(q)]
        return remote(here, there_ref, relayed_send, part_recv.at[slot, 0 if q is None else q], level(z, j))

    def relayed_piece(j, k, q):
        for z in relayed(j, k):
            total = jnp.zeros((height, WIDE), jnp.float32)
            for half in range(side):
                total += nt3(help_stack[:, half * part : (half + 1) * part], stay[half, wide(q), :])
            guest[z, :, wide(q)] = total
            relayed_back(j, k, z, q).start()

    def host_own(j, k):
        c = host_of(j, k)
        if known(k):
            for q in range(pieces):
                vec_wait(vec_from[c].index(k), q)
            own = vec_in.at[vec_from[c].index(k)]
        else:
            for r in range(rounds):
                landed(guest.at[k, few(r), :], guest_recv.at[k, r])
            own = guest.at[k]
        high, low = halves(own[...])
        guest_stack[:height] = high
        guest_stack[height:] = low

        @pl.loop(0, pieces)
        def _(q):
            if c == j:
                part_in[part_from[j].index(k), :, wide(q)] = products(height, q)
            else:
                guest_part[rounds, :, wide(q)] = products(height, q)
                own_back(j, k, q).start()

    def make_part(c, block, q, left):
        slot, made = blocks[c].index(block), part_made[c].index(block)
        for n in range(WIDE // TALL):
            others(slot, block, q * (WIDE // TALL) + n)
        total = jnp.zeros((height, WIDE), jnp.float32)
        for half in range(side):
            total += nt3(left[:, half * part : (half + 1) * part], buf[slot, half, wide(q), :])
        part_out[made, :, wide(q)] = total
        part_to(block, made, q).start()

    per_half = part // WIDE

    def order(n):
        return lax.rem(n + jnp.where(a == 0, b * per_half, 0), pieces)

    def columns_of(o):
        return o // per_half, wide(lax.rem(o, per_half))

    def fold(slot):
        half, where = columns_of(order(pieces - 1))
        for n in range(pieces):
            upto = (n + 1) * WIDE
            high, low = halves(inverse[n * WIDE : upto, :upto])
            right, right_low = halves(buf[slot, half, :upto, where])
            total = jnp.dot(high, right, preferred_element_type=jnp.float32) + jnp.dot(low, right, preferred_element_type=jnp.float32)
            stay[0, n * WIDE : upto, :WIDE] = total + jnp.dot(high, right_low, preferred_element_type=jnp.float32)

    def folded(c):
        return [jk for jk in before[c] if both_down(jk)]

    def take_last(c):
        for block in folded(c):
            coming = vec_from[c].index(block[1])
            last = order(pieces - 1)
            vec_wait(coming, last)
            high, low = halves(vec_in[coming, :, wide(last)])
            stack[:height, :WIDE] = high
            stack[height:, :WIDE] = low
            total = jnp.zeros((8, height), jnp.float32)
            for n in range(pieces):
                done = vec[:, n * WIDE : (n + 1) * WIDE] - nt3(stack[:, :WIDE], stay[0, n * WIDE : (n + 1) * WIDE, :WIDE])
                vec[:, n * WIDE : (n + 1) * WIDE] = done
                high, low = halves(done * done)
                total += nt(ones[...], high) + nt(ones[...], low)
            sums[column] = total

    def take_before(c):
        for block in before[c]:
            j, k = block
            slot, coming = blocks[c].index(block), vec_from[c].index(k)
            if both_down(block):
                serving(c, early(columns - 3), lambda block: chunks)

                @pl.when((a <= k) & (a > 0))
                def _():
                    @pl.loop(0, chunks)
                    def _(i):
                        serve_others(slot, block, i)

                def others_in():
                    @pl.loop(0, chunks)
                    def _(i):
                        others(slot, block, i)

                pl.when(a > 0)(others_in)
                for jj, kk in staying:
                    if jj == c and host_of(jj, kk) != c:

                        @pl.when(a < kk)
                        def _():
                            for r in range(rounds):
                                landed(guest.at[a, few(r), :], guest_recv.at[a, r])
                                relay(jj, kk, r).start()

                for n in range(pieces - 1):
                    if n == per_half:
                        pl.when(a == 0)(others_in)
                        fold(slot)
                    o = order(n)
                    vec_wait(coming, o)
                    high, low = halves(vec_in[coming, :, wide(o)])
                    stack[:height, :WIDE] = high
                    stack[height:, :WIDE] = low
                    half, where = columns_of(o)

                    @pl.loop(0, pieces)
                    def _(m):
                        rest[:, wide(m)] -= nt3(stack[:, :WIDE], buf[slot, half, wide(m), where])
            elif j != c:
                serving(c, early(columns - 3), lambda block: chunks)
                for jj, kk in staying:
                    if host_of(jj, kk) == c:
                        pl.when(a == kk)(functools.partial(host, jj, kk))
                        pl.when(a == kk)(functools.partial(relayed_in, jj, kk))

                def work():
                    for q in range(pieces):
                        vec_wait(coming, q)

                pl.when(active(block) & (a != k) if c == heir[k] else active(block))(work)

                @pl.when(active(block))
                def _():
                    high, low = halves(vec_in[coming])
                    guest_stack[:height] = high
                    guest_stack[height:] = low

                pl.when(helping(block))(functools.partial(take_help, block))
            else:
                serving(c, early(columns - 3), early(columns - 2))
                for q in range(pieces):
                    vec_wait(coming, q)
                put(vec_in[coming])

                @pl.loop(0, pieces)
                def _(q):
                    @pl.when(a != k)
                    def _():
                        serve_ahead(slot, block, q, early(columns - 2)(block))

                    for u in range(columns):
                        for jj, kk in after[u]:
                            if kk == c:

                                @pl.when((a == kk) & (q == (chunks - EARLY[columns - 2] + 1) * TALL // WIDE + 1))
                                def _():
                                    pl.semaphore_signal(gate, inc=1, device_id=there(u), device_id_type=MESH)

                    for n in range(WIDE // TALL):
                        others(slot, block, q * (WIDE // TALL) + n)
                    total = jnp.zeros((height, WIDE), jnp.float32)
                    for half in range(side):
                        total += nt3(stack[:, half * part : (half + 1) * part], buf[slot, half, wide(q), :])
                    rest[:, wide(q)] -= total

    inverse_load.wait()
    for c in range(columns):
        if before[c]:
            on(c, functools.partial(take_before, c))

    squares = jnp.zeros((8, height), jnp.float32)
    for q in range(pieces):
        here = slice(q * WIDE, (q + 1) * WIDE)
        for c in range(columns):
            for block in before[c]:
                if block[0] != c:

                    def give(c=c, block=block):
                        @pl.when(active(block))
                        def _():
                            make_part(c, block, q, guest_stack)

                        @pl.when(helping(block))
                        def _():
                            help_piece(c, block, q)

                        for j, k in staying:
                            if relayed(j, k) and host_of(j, k) == c:
                                pl.when(a == k)(functools.partial(relayed_piece, j, k, q))

                    on(c, give)
            if part_from[c]:

                def work(c=c):
                    for slot, k in enumerate(part_from[c]):
                        if (c, k) not in staying:
                            part_wait(slot, q)
                        else:

                            def back_wait(slot=slot):
                                landed(part_in.at[slot], back_recv.at[slot])

                            if q == 0:
                                pl.when(a != k if host_of(c, k) == c else a > k)(back_wait)
                            if host_of(c, k) != c:
                                pl.when(a <= k)(functools.partial(part_wait, slot, q))

                        rest[:, here] -= part_in[slot, :, here]

                on(c, work)
        high, low = halves(rest[:, here])
        stack[:height, here] = high
        stack[height:, here] = low
        done = nt3(stack[:, : (q + 1) * WIDE], inverse[here, : (q + 1) * WIDE])
        vec[:, here] = done
        high, low = halves(done * done)
        squares += nt(ones[...], high) + nt(ones[...], low)
        for c in range(columns):
            if vec_to[c]:

                on(c, functools.partial(vec_outs, c, q, lambda copy: copy.start()))

    def guest_round(c, r):
        def work():
            if r:
                guest_out(c, r - 1).wait_send()
            if r < rounds:
                guest_out(c, r).start()

        if known(c) or not after[c]:
            pl.when(a != c)(work)
        else:
            work()

    def guests(c):
        for block in lift_to(c):

            @pl.when(jnp.logical_not(active(block)))
            def _():
                for r in range(rounds):
                    lift_out(block, r).start()

        if heir[c] is not None:
            if not known(c) and not after[c]:

                @pl.when(a == c)
                def _():
                    for r in range(rounds):
                        guest_out(c, r).start()
                    for r in range(rounds):
                        guest_out(c, r).wait_send()

            for r in range(1 if after[c] else rounds + 1):
                guest_round(c, r)

    for c in range(columns):
        on(c, functools.partial(guests, c))
    sums[column] = squares
    for c in range(columns):
        if folded(c):
            on(c, functools.partial(take_last, c))
    store = pltpu.make_async_copy(vec, out_ref, out_sem)
    store.start()

    def sum_out(step):
        to = (column + step) % columns
        return remote(sums.at[column], sums.at[column], sum_send.at[step - 1], sum_recv.at[column], there(to))

    for step in range(1, columns):
        sum_out(step).start()

    for j, k in staying:
        if host_of(j, k) != j:

            @pl.when((column == host_of(j, k)) & (a == k))
            def _():
                host_own(j, k)


    def give_after(c):
        for block in after[c]:
            j, k = block
            slot, coming = blocks[c].index(block), vec_from[c].index(k)

            if heir[c] is not None:
                for r in range(1, rounds + 1):
                    guest_round(c, r)

                    @pl.when(a == k)
                    def _():
                        if r == 1:
                            pl.semaphore_wait(gate, 1)

                    @pl.when(active(block))
                    def _():
                        @pl.loop(*[jnp.where(a == k, min(2 * n, LATER), n * LATER // rounds) for n in (r - 1, r)])
                        def _(i):
                            serve(slot, block, i)

            @pl.when(active(block))
            def _():
                for q in range(pieces):
                    vec_wait(coming, q)
                put(vec_in[coming])
                pl.when(helping(block))(functools.partial(take_help, block))

                @pl.loop(0, pieces)
                def _(q):
                    serve_ahead(slot, block, q, LATER)
                    make_part(c, block, q, stack)

                    @pl.when(helping(block))
                    def _():
                        help_piece(c, block, q)

    for c in range(columns):
        if after[c]:
            on(c, functools.partial(give_after, c))

    def sent(copy):
        copy.wait_send()

    for d in range(chips):
        slab_out(d).wait_send()
    for d in range(1, chips):
        slab_pass(d).wait_send()
    for j, k in all_blocks:
        t = target_of(j, k)
        if t is not None and t != j:

            @pl.when((column == j) & (a == k))
            def _():
                entry(blocks[t].index((j, k)), None, t).wait_send()

    for j, k in staying:
        c = host_of(j, k)

        @pl.when((column == j) & (a == k))
        def _():
            for step in range(0 if c != j else 1, side):
                stay_out(step, None, c).wait_send()

        if relayed(j, k):

            @pl.when((column == j) & (a < k))
            def _():
                relay(j, k, None).wait_send()

        @pl.when((column == c) & (a == k))
        def _():
            for z in visitors(j, k):
                if z in relayed(j, k):
                    relayed_back(j, k, z, None).wait_send()
                else:
                    back(j, k, z, None).wait_send()
            if c != j:
                own_back(j, k, None).wait_send()

    for c in range(columns):

        def work(c=c):
            for slot, block in enumerate(blocks[c]):
                line_flows(slot, block, None, sent)
                side_flows(slot, block, None, sent)
                if both_down(block):
                    other_flows(slot, block, None, sent)
            vec_outs(c, None, sent)
            for made, block in enumerate(part_made[c]):

                @pl.when(active(block))
                def _():
                    part_to(block, made, None).wait_send()

                @pl.when(helping(block))
                def _():
                    lift_back(block, None).wait_send()

            for block in lift_to(c):

                @pl.when(jnp.logical_not(active(block)))
                def _():
                    lift_out(block, None).wait_send()

        on(c, work)
    for step in range(1, columns):
        other = (column + step) % columns
        landed(sums.at[other], sum_recv.at[other])
    total = sums[0]
    for c in range(1, columns):
        total += sums[c]
    mean_ref[...] = total[:1] / (width * columns)
    for step in range(1, columns):
        sum_out(step).wait_send()
    store.wait()


def chain_device(slab, factor, block_inverse, pivot_order, row_count):
    height, width = slab.shape
    depth, part = factor.shape
    groups = lax.axis_size("cols")
    side = lax.axis_size("rows") // groups
    column = lax.axis_index("cols")
    slots = max([sum(target_of(j, k) == c for j in range(groups) for k in range(j)) for c in range(groups)])
    chunks, pieces, rounds, chips = depth // TALL, width // WIDE, groups - 1, groups // 2
    sem, space = pltpu.SemaphoreType.DMA, pltpu.VMEM
    f32, bf16 = jnp.float32, jnp.bfloat16
    held = pl.BlockSpec(memory_space=pltpu.VMEM)
    away = pl.BlockSpec(memory_space=pl.ANY)
    vectors, mean = pl.pallas_call(
        functools.partial(chain_kernel, groups, side),
        out_shape=(jax.ShapeDtypeStruct((height, width), f32), jax.ShapeDtypeStruct((1, height), f32)),
        in_specs=[away, away, away, held, pl.BlockSpec(memory_space=pltpu.SMEM)],
        out_specs=(away, held),
        scratch_shapes=[
            space((slots, side, depth, part), f32),
            space((width, width), f32),
            space((groups, height, width), f32),
            space((height, width), f32),
            space((height, width), f32),
            space((2 * height, width), bf16),
            space((1, height, width), f32),
            space((groups - 2, height, width), f32),
            space((1, height, width), f32),
            space((groups, 8, height), f32),
            space((8, WIDE), bf16),
            space((side, depth, part), f32),
            space((groups, height, width), f32),
            space((2 * height, width), bf16),
            space((rounds + 1, height, width), f32),
            space((2 * height, width), bf16),
            sem((chunks,)),
            sem((slots, side, chunks)),
            sem((slots,)),
            sem((slots, side)),
            sem((side - 1, slots)),
            sem(()),
            sem(()),
            sem(()),
            sem((chips,)),
            sem((groups,)),
            sem((chips - 1,)),
            sem((groups - 2,)),
            sem((1, pieces)),
            sem((1,)),
            sem((groups - 2, pieces)),
            sem((groups,)),
            sem((groups,)),
            sem(()),
            sem(()),
            sem((side,)),
            sem((side,)),
            sem((rounds,)),
            sem((groups, rounds)),
            sem((groups,)),
            sem((groups - 2,)),
            sem(()),
            sem(()),
            sem(()),
            sem(()),
            sem(()),
            pltpu.SemaphoreType.REGULAR,
        ],
        compiler_params=pltpu.CompilerParams(collective_id=0, has_side_effects=True, vmem_limit_bytes=57000 * 1024),
    )(slab, factor, block_inverse, pivot_order[None, :], row_count)
    return vectors, mean[0]


def per_device(slab, factor, block_inverse, pivot_order, row_count):
    groups, rows = lax.axis_size("cols"), lax.axis_size("rows")
    depth, part = factor.shape
    fits = groups // 2 == 2 and rows % groups == 0 and rows > groups and part % WIDE == 0 and depth % WIDE == 0 and slab.shape[0] % (8 * (groups - 1)) == 0
    one = chain_device if fits else plain_device
    return one(slab, factor, block_inverse, pivot_order, row_count)


def solution(mesh):
    placed = (P("rows", "cols"), P("cols", "rows"), P("cols", None), P(), P("rows"))
    return jax.shard_map(
        per_device,
        mesh=mesh,
        in_specs=placed,
        out_specs=(P("rows", "cols"), P("rows")),
        check_vma=False,
    )
```

```python
import functools
import jax
import jax.numpy as jnp
from jax import lax
from jax.experimental import pallas as pl
from jax.experimental.pallas import tpu as pltpu
from jax.sharding import PartitionSpec as P

MESH = pl.DeviceIdType.MESH


def times_transposed(left, right):
    return lax.dot_general(
        left,
        right,
        (((1,), (1,)), ((), ())),
        precision=lax.Precision.HIGH,
        preferred_element_type=jnp.float32,
    )


def gather_kernel(groups, side, chunks, part_ref, row_ref, mine, in_sem, keep_sem, right_sem, left_sem, hop_sem, side_sem, cross_sem):
    row, column = lax.axis_index("rows"), lax.axis_index("cols")
    a, b = row // side, row % side
    depth, width = part_ref.shape
    tall = depth // chunks

    def at(a_to, b_to):
        return (a_to * side + b_to, column)

    barrier = pltpu.get_barrier_semaphore()
    for step in (1, groups - 1):
        pl.semaphore_signal(barrier, inc=1, device_id=at((a + step) % groups, b), device_id_type=MESH)
    for step in range(1, side):
        pl.semaphore_signal(barrier, inc=1, device_id=at(a, (b + step) % side), device_id_type=MESH)
    pl.semaphore_wait(barrier, 2 + side - 1)

    def rows_of(i):
        return pl.ds(pl.multiple_of(i * tall, tall), tall)

    def place(k, b_of, i):
        return row_ref.at[k * side + b_of, rows_of(i), :]

    def right(k, i, source):
        return pltpu.make_async_remote_copy(source, place(k, b, i), right_sem.at[k, i], hop_sem.at[k, i], device_id=at(jnp.minimum(a + 1, groups - 1), b), device_id_type=MESH)

    def left(k, i, source):
        return pltpu.make_async_remote_copy(source, place(k, b, i), left_sem.at[k, i], hop_sem.at[k, i], device_id=at(jnp.maximum(a - 1, 0), b), device_id_type=MESH)

    def across(k, step, i, source):
        return pltpu.make_async_remote_copy(source, place(k, b, i), side_sem.at[step - 1, k, i], cross_sem.at[step - 1, k, i], device_id=at(a, (b + step) % side), device_id_type=MESH)

    def load(i):
        return pltpu.make_async_copy(part_ref.at[rows_of(i), :], mine.at[rows_of(i), :], in_sem.at[i])

    def keep(i):
        return pltpu.make_async_copy(mine.at[rows_of(i), :], place(a, b, i), keep_sem.at[i])

    @pl.when(a < column)
    def _():
        @pl.loop(0, chunks)
        def _(i):
            load(i).start()

        @pl.loop(0, chunks)
        def _(i):
            source = mine.at[rows_of(i), :]
            load(i).wait()

            @pl.when(a < groups - 1)
            def _():
                right(a, i, source).start()

            @pl.when(a > 0)
            def _():
                left(a, i, source).start()

            for step in range(1, side):
                across(a, step, i, source).start()
            keep(i).start()

    for hop in range(1, groups):
        @pl.loop(0, chunks)
        def _(i):
            k = a - hop

            @pl.when((k >= 0) & (k < column))
            def _():
                source = place(k, b, i)
                right(k, i, source).wait_recv()

                @pl.when(a < groups - 1)
                def _():
                    right(k, i, source).start()

                for step in range(1, side):
                    across(k, step, i, source).start()

            h = a + hop

            @pl.when((h <= groups - 1) & (h < column))
            def _():
                source = place(h, b, i)
                left(h, i, source).wait_recv()

                @pl.when(a > 0)
                def _():
                    left(h, i, source).start()

                for step in range(1, side):
                    across(h, step, i, source).start()

    for k in range(groups - 1):
        @pl.when(k < column)
        def _():
            @pl.loop(0, chunks)
            def _(i):
                source = place(k, b, i)
                for step in range(1, side):
                    came = place(k, (b + side - step) % side, i)
                    pltpu.make_async_remote_copy(came, came, side_sem.at[step - 1, k, i], cross_sem.at[step - 1, k, i], device_id=at(a, (b + step) % side), device_id_type=MESH).wait_recv()
                    across(k, step, i, source).wait_send()

                @pl.when((k <= a) & (a < groups - 1))
                def _():
                    right(k, i, source).wait_send()

                @pl.when((k >= a) & (a > 0))
                def _():
                    left(k, i, source).wait_send()

                @pl.when(k == a)
                def _():
                    keep(i).wait()


def gather_factor(factor, rows, groups):
    side = rows // groups
    depth, width = factor.shape
    chunks = max(1, depth // 256)
    sem = pltpu.SemaphoreType.DMA
    return pl.pallas_call(
        functools.partial(gather_kernel, groups, side, chunks),
        out_shape=jax.ShapeDtypeStruct(((groups - 1) * side, depth, width), jnp.float32),
        in_specs=[pl.BlockSpec(memory_space=pl.ANY)],
        out_specs=pl.BlockSpec(memory_space=pl.ANY),
        scratch_shapes=[
            pltpu.VMEM((depth, width), jnp.float32),
            sem((chunks,)),
            sem((chunks,)),
            sem((groups, chunks)),
            sem((groups, chunks)),
            sem((groups, chunks)),
            sem((side - 1, groups, chunks)),
            sem((side - 1, groups, chunks)),
        ],
        compiler_params=pltpu.CompilerParams(collective_id=0, has_side_effects=True, vmem_limit_bytes=60000 * 1024),
        cost_estimate=pl.CostEstimate(flops=0, bytes_accessed=600000000, transcendentals=0),
    )(factor)


def plain_device(slab, factor, block_inverse, pivot_order, row_count):
    rows_here, block_width = slab.shape
    row_devices = lax.axis_size("rows")
    column_count = lax.axis_size("cols")
    column = lax.axis_index("cols")
    total_width = block_width * column_count
    side = row_devices // column_count
    chosen = lax.dynamic_slice_in_dim(pivot_order, column * block_width, block_width)
    gathered = lax.all_gather(slab, "cols", axis=1, tiled=True)
    parts = gather_factor(factor, row_devices, column_count)
    gathered, parts = lax.optimization_barrier((gathered, parts))
    ordered = jnp.take(gathered, chosen, axis=1)
    live_rows = jnp.arange(rows_here, dtype=jnp.int32) < row_count[0]
    pending = jnp.where(live_rows[:, None], ordered, jnp.float32(0.0))

    def finish(values):
        return times_transposed(values, block_inverse)

    def nothing(values):
        return jnp.zeros_like(values)

    width = factor.shape[1]
    vectors = jnp.zeros_like(pending)
    for k in range(column_count):
        finished = lax.cond(column == k, finish, nothing, pending)
        vectors = vectors + finished
        if k + 1 < column_count:
            arrived = moving = finished
            for to in range(k + 1, column_count):
                moving = lax.ppermute(moving, "cols", [(to - 1, to)])
                arrived = jnp.where(column == to, moving, arrived)
            update = jnp.zeros_like(pending)
            for b in range(side):
                update += times_transposed(arrived[:, b * width : (b + 1) * width], parts[k * side + b])
            pending = pending - jnp.where(k < column, update, jnp.float32(0.0))
    row_sums = lax.psum(jnp.sum(vectors * vectors, axis=1), "cols")
    return (vectors, row_sums / total_width)


TALL = 128
WIDE = 256
EARLY = (5, 7, 9)
LATER = 4


def target_of(j, k):
    if k == j - 1:
        return j if j % 2 else j - 2
    return j - 1 if j % 2 and k == 0 else None


def host_of(j, k):
    return j - 1 if j % 2 else j


def halves(values):
    high = values.astype(jnp.bfloat16)
    return high, (values - high.astype(jnp.float32)).astype(jnp.bfloat16)


def nt(left, right):
    return lax.dot_general(left, right, (((1,), (1,)), ((), ())), preferred_element_type=jnp.float32)


def nt3(stacked, right):
    rows = stacked.shape[0] // 2
    high, low = halves(right)
    both = nt(stacked, high)
    return both[:rows] + (both[rows:] + nt(stacked[:rows], low))


def chain_kernel(
    groups,
    side,
    slab_ref,
    factor_ref,
    inverse_ref,
    order_ref,
    count_ref,
    out_ref,
    mean_ref,
    buf,
    inverse,
    slabs,
    rest,
    vec,
    stack,
    vec_in,
    part_in,
    part_out,
    sums,
    ones,
    stay,
    guest,
    guest_stack,
    guest_part,
    help_stack,
    load_sem,
    recv_sem,
    up_sem,
    down_sem,
    side_sem,
    entry_sem,
    inverse_sem,
    own_sem,
    slab_send,
    slab_recv,
    pass_send,
    vec_send,
    vec_recv,
    part_send,
    part_recv,
    sum_send,
    sum_recv,
    out_sem,
    stay_load,
    stay_send,
    stay_recv,
    guest_send,
    guest_recv,
    back_send,
    back_recv,
    lift_send,
    lift_back_send,
    relayed_send,
    relay_send,
    own_back_send,
    gate,
):
    columns = groups
    row, column = lax.axis_index("rows"), lax.axis_index("cols")
    a, b = row // side, row % side
    height, width = rest.shape
    depth, part = factor_ref.shape
    chunks = depth // TALL
    pieces = width // WIDE
    rounds = groups - 1
    share = height // rounds
    chips = columns // 2
    chip, core = column // 2, column % 2
    all_blocks = [(j, k) for j in range(1, columns) for k in range(j)]
    moving = [jk for jk in all_blocks if target_of(*jk) is not None]
    staying = [jk for jk in all_blocks if target_of(*jk) is None]
    blocks = [[jk for jk in moving if target_of(*jk) == c] for c in range(columns)]
    before = [[jk for jk in blocks[c] if jk[1] < c] for c in range(columns)]
    after = [[jk for jk in blocks[c] if jk[1] > c] for c in range(columns)]
    heir = [host_of(*[jk for jk in staying if jk[1] == k][0]) if [jk for jk in staying if jk[1] == k] else None for k in range(columns)]
    hosted = [[k for j, k in staying if host_of(j, k) == c] for c in range(columns)]
    vec_from = [sorted({k for _, k in blocks[c] if k != c}) for c in range(columns)]
    vec_to = [[u for u in range(columns) if c in vec_from[u]] for c in range(columns)]
    part_from = [[k for k in range(c) if target_of(c, k) != c] for c in range(columns)]
    part_made = [[jk for jk in blocks[c] if jk[0] != c] for c in range(columns)]

    def there(c):
        return (row, c)

    def level(z, c):
        return (z * side + b, c)

    def beside(step):
        return (a * side + (b + step) % side, column)

    def remote(source, target, send, recv, device):
        return pltpu.make_async_remote_copy(source, target, send, recv, device_id=device, device_id_type=MESH)

    def landed(here, recv):
        remote(here, here, out_sem, recv, there(column)).wait_recv()

    def tall(i):
        return pl.ds(pl.multiple_of(i * TALL, TALL), TALL)

    def wide(q):
        return pl.ds(pl.multiple_of(q * WIDE, WIDE), WIDE)

    def few(r):
        return pl.ds(pl.multiple_of(r * share, share), share)

    def on(c, work):
        pl.when(column == c)(work)

    barrier = pltpu.get_barrier_semaphore()
    for step in range(1, side):
        pl.semaphore_signal(barrier, inc=1, device_id=beside(step), device_id_type=MESH)
        for right_by in range(1, columns):
            pl.semaphore_signal(barrier, inc=1, device_id=(a * side + (b + step) % side, (column + right_by) % columns), device_id_type=MESH)
    for up_by in range(groups):
        for right_by in range(columns):
            if up_by or right_by:
                pl.semaphore_signal(barrier, inc=1, device_id=level((a + up_by) % groups, (column + right_by) % columns), device_id_type=MESH)
    pl.semaphore_wait(barrier, (side - 1) * columns + groups * columns - 1)

    def source_of(d, f):
        return (chip + d) % chips * 2 + (core + f) % 2

    partner = source_of(0, 1)
    own_load = pltpu.make_async_copy(slab_ref, slabs.at[column], own_sem)
    own_load.start()
    inverse_load = pltpu.make_async_copy(inverse_ref, inverse, inverse_sem)

    def slab_out(d):
        to = source_of(d, 0) if d else partner
        return remote(slab_ref, slabs.at[column], slab_send.at[d], slab_recv.at[column], there(to))

    def slab_pass(d):
        place = slabs.at[source_of(d, 0)]
        return remote(place, place, pass_send.at[d - 1], slab_recv.at[source_of(d, 0)], there(partner))

    for d in list(range(1, chips)) + [0]:
        slab_out(d).start()

    def place(slot, half, i):
        return buf.at[slot, half] if i is None else buf.at[slot, half, tall(i), :]

    def came(slot, half, i):
        return recv_sem.at[slot, half, 0 if i is None else i]

    def load(slot, i):
        return pltpu.make_async_copy(factor_ref.at[tall(i), :], place(slot, b, i), load_sem.at[i])

    def entry(slot, i, to):
        return remote(factor_ref if i is None else factor_ref.at[tall(i), :], place(slot, b, i), entry_sem, came(slot, b, i), there(to))

    def up(slot, i):
        return remote(place(slot, b, i), place(slot, b, i), up_sem.at[slot], came(slot, b, i), level(jnp.minimum(a + 1, groups - 1), column))

    def down(slot, half, i):
        return remote(place(slot, half, i), place(slot, half, i), down_sem.at[slot, half], came(slot, half, i), level(jnp.maximum(a - 1, 0), column))

    def across(slot, step, i):
        return remote(place(slot, b, i), place(slot, b, i), side_sem.at[step - 1, slot], came(slot, b, i), beside(step))

    def arrived(slot, half, i):
        landed(place(slot, half, i), recv_sem.at[slot, half, i])

    def both_down(block):
        return block[1] >= 2

    def lifted(block):
        return block[0] % 2 == 0

    top = groups - 1

    def crosses(block):
        return target_of(*block) != block[0]

    def active(block):
        if not crosses(block):
            return a >= 0
        return a >= block[1] if lifted(block) else a < top

    def helper(block):
        return block[1] if lifted(block) else top - 1

    def helped_level(block):
        return block[1] - 1 if lifted(block) else top

    def helping(block):
        return a == helper(block)

    def free_level(block):
        return functools.reduce(jnp.logical_and, [a != k for k in hosted[target_of(*block)]], a >= 0)

    def line_flows(slot, block, i, act):
        k = block[1]

        @pl.when((a >= k) & (a < (top - 1 if crosses(block) and not lifted(block) else top)))
        def _():
            act(up(slot, i))

        if not lifted(block):

            @pl.when((a <= k) & (a > 0))
            def _():
                act(down(slot, b, i))

    def side_flows(slot, block, i, act):
        @pl.when((a >= block[1]) if both_down(block) else active(block))
        def _():
            for step in range(1, side):
                act(across(slot, step, i))

    def other_flows(slot, block, i, act):
        @pl.when((a <= block[1]) & (a > 0))
        def _():
            for step in range(1, side):
                act(down(slot, (b + step) % side, i))

    def serve(slot, block, i):
        j, k = block
        if target_of(j, k) == j:

            @pl.when(a == k)
            def _():
                load(slot, i).wait()

            @pl.when(a != k)
            def _():
                arrived(slot, b, i)
        else:
            arrived(slot, b, i)
        line_flows(slot, block, i, lambda copy: copy.start())

        @pl.when(free_level(block))
        def _():
            side_flows(slot, block, i, lambda copy: copy.start())


    def serve_ahead(slot, block, q, ahead):
        for n in range(WIDE // TALL):
            i = ahead + q * (WIDE // TALL) + n

            @pl.when(i < chunks)
            def _():
                serve(slot, block, i)

    def serve_others(slot, block, i):
        for step in range(1, side):
            arrived(slot, (b + step) % side, i)
        other_flows(slot, block, i, lambda copy: copy.start())

    def others(slot, block, i):
        def work():
            for step in range(1, side):
                arrived(slot, (b + step) % side, i)

        if both_down(block):
            pl.when((a > block[1]) | (a == 0))(work)
        else:
            work()

    def stay_out(step, q, to):
        here = factor_ref if q is None else factor_ref.at[wide(q), :]
        return remote(here, stay.at[b] if q is None else stay.at[b, wide(q), :], stay_send.at[step], stay_recv.at[b], (a * side + (b + step) % side, to))

    def stay_in():
        return pltpu.make_async_copy(factor_ref, stay.at[b], stay_load)

    for j, k in all_blocks:
        t = target_of(j, k)

        @pl.when((column == j) & (a == k))
        def _():
            if t is None:
                for step in range(0 if host_of(j, k) != j else 1, side):
                    for q in range(pieces):
                        stay_out(step, q, host_of(j, k)).start()
                if host_of(j, k) == j:
                    stay_in().start()
            else:
                slot = blocks[t].index((j, k))

                @pl.loop(0, chunks)
                def _(i):
                    if t == j:
                        load(slot, i).start()
                    else:
                        entry(slot, i, t).start()

    inverse_load.start()

    rest[...] = jnp.zeros_like(rest)
    live = lax.broadcasted_iota(jnp.int32, (height, 1), 0) < count_ref[0]
    ones[...] = jnp.ones_like(ones)

    def serving(c, low, high):
        for block in before[c]:

            def work(block=block):
                @pl.loop(low(block), high(block))
                def _(i):
                    serve(blocks[c].index(block), block, i)

            pl.when((a != block[1]) & active(block))(work)

    def early(n):
        return lambda block: jnp.maximum(EARLY[n] - jnp.abs(a - block[1]), 0)

    def serve_source(c):
        for block in before[c]:

            def work(block=block):
                @pl.loop(0, chunks)
                def _(i):
                    serve(blocks[c].index(block), block, i)

            pl.when(a == block[1])(work)

    for c in range(columns):
        if before[c]:
            on(c, functools.partial(serve_source, c))
    for turn in range(columns):
        d, f = turn // 2, turn % 2
        s = source_of(d, f)
        if turn >= 2:
            for c in range(columns):
                if before[c]:
                    on(c, functools.partial(serving, c, early(turn - 3) if turn > 2 else lambda block: 0, early(turn - 2)))
        if turn == 0:
            own_load.wait()
        else:
            landed(slabs.at[s], slab_recv.at[s])
            if f == 0:
                slab_pass(d).start()
        high, low = halves(jnp.where(live, slabs[s], 0.0))
        stack[:height] = high
        stack[height:] = low

        @pl.loop(0, pieces)
        def _(q):
            index = lax.broadcasted_iota(jnp.int32, (width, WIDE), 0) + s * width
            chosen = jnp.where(index == order_ref[:, pl.ds(pl.multiple_of(column * width + q * WIDE, WIDE), WIDE)], 1.0, 0.0).astype(jnp.bfloat16)
            both = jnp.dot(stack[...], chosen, preferred_element_type=jnp.float32)
            rest[:, wide(q)] += both[:height] + both[height:]

    def vec_wait(slot, q):
        landed(vec_in.at[slot, :, wide(q)], vec_recv.at[slot, q])

    def part_wait(slot, q):
        landed(part_in.at[slot, :, wide(q)], part_recv.at[slot, q])

    def vec_out(c, n, q):
        u = vec_to[c][n]
        slot = vec_from[u].index(c)
        here, to = (vec, vec_in.at[slot]) if q is None else (vec.at[:, wide(q)], vec_in.at[slot, :, wide(q)])
        return remote(here, to, vec_send.at[n], vec_recv.at[slot, 0 if q is None else q], there(u))

    def vec_outs(c, q, act):
        for n, u in enumerate(vec_to[c]):
            block = [jk for jk in blocks[u] if jk[1] == c][0]

            @pl.when(active(block))
            def _():
                act(vec_out(c, n, q))

    def lift_to(c):
        return [jk for u in range(columns) for jk in blocks[u] if crosses(jk) and jk[1] == c]

    def lift_out(block, r):
        j, k = block
        here, to = (vec, guest.at[a]) if r is None else (vec.at[few(r), :], guest.at[a, few(r), :])
        return remote(here, to, lift_send, guest_recv.at[a, 0 if r is None else r], level(helper(block), target_of(j, k)))

    def lift_back(block, q):
        j, k = block
        slot = part_from[j].index(k)
        here, to = (guest.at[top - 1], part_in.at[slot]) if q is None else (guest.at[top - 1, :, wide(q)], part_in.at[slot, :, wide(q)])
        return remote(here, to, lift_back_send, part_recv.at[slot, 0 if q is None else q], level(helped_level(block), j))

    def take_help(block):
        z = helped_level(block)
        for r in range(rounds):
            landed(guest.at[z, few(r), :], guest_recv.at[z, r])
        high, low = halves(guest[z])
        help_stack[:height] = high
        help_stack[height:] = low

    def help_piece(c, block, q):
        slot = blocks[c].index(block)
        total = jnp.zeros((height, WIDE), jnp.float32)
        for half in range(side):
            total += nt3(help_stack[:, half * part : (half + 1) * part], buf[slot, half, wide(q), :])
        guest[top - 1, :, wide(q)] = total
        lift_back(block, q).start()

    def part_to(block, made, q):
        j, k = block
        slot = part_from[j].index(k)
        here, to = (part_out.at[made], part_in.at[slot]) if q is None else (part_out.at[made, :, wide(q)], part_in.at[slot, :, wide(q)])
        return remote(here, to, part_send.at[made], part_recv.at[slot, 0 if q is None else q], there(j))

    def put(values):
        high, low = halves(values)
        stack[:height] = high
        stack[height:] = low

    def known(k):
        return k in vec_from[heir[k]]

    def guest_out(k, r):
        to = level(k, heir[k])
        j = [j for j, kk in staying if kk == k][0]
        if host_of(j, k) != j:
            to = (jnp.where(a < k, row, to[0]), jnp.where(a < k, j, to[1]))
        return remote(vec.at[few(r), :], guest.at[a, few(r), :], guest_send.at[r], guest_recv.at[a, r], to)

    def relay(j, k, r):
        here = guest.at[a] if r is None else guest.at[a, few(r), :]
        return remote(here, here, relay_send, guest_recv.at[a, 0 if r is None else r], level(k, host_of(j, k)))

    def own_back(j, k, q):
        slot = part_from[j].index(k)
        here, to = (guest_part.at[rounds], part_in.at[slot]) if q is None else (guest_part.at[rounds, :, wide(q)], part_in.at[slot, :, wide(q)])
        return remote(here, to, own_back_send, part_recv.at[slot, 0 if q is None else q], level(k, j))

    def visitors(j, k):
        return [z for z in range(groups) if z > k or z < k and host_of(j, k) == j] + relayed(j, k)

    def relayed(j, k):
        return [] if host_of(j, k) == j else list(range(k))

    def back(j, k, z, r):
        slot = part_from[j].index(k)
        n = visitors(j, k).index(z)
        here = guest_part.at[slice(0, rounds) if r is None else r, n * share : (n + 1) * share, :]
        return remote(here, here if r is None else part_in.at[slot, few(r), :], back_send.at[z], back_recv.at[slot], level(z, j))

    def products(rows, q):
        total = jnp.zeros((rows, WIDE), jnp.float32)
        for half in range(side):
            total += nt3(guest_stack[: 2 * rows, half * part : (half + 1) * part], stay[half, wide(q), :])
        return total

    def host(j, k):
        c = host_of(j, k)
        if c == j:
            stay_in().wait()
        for step in range(1 if c == j else 0, side):
            half = (b + step) % side
            landed(stay.at[half], stay_recv.at[half])
        for block in blocks[c]:

            @pl.loop(0, chunks)
            def _(i):
                side_flows(blocks[c].index(block), block, i, lambda copy: copy.start())

        away = [z for z in visitors(j, k) if z not in relayed(j, k)]
        tall_of = len(away) * share

        @pl.loop(0, rounds)
        def _(r):
            for n, z in enumerate(away):
                landed(guest.at[z, few(r), :], guest_recv.at[z, r])
                high, low = halves(guest[z, few(r), :])
                guest_stack[n * share : (n + 1) * share] = high
                guest_stack[tall_of + n * share : tall_of + (n + 1) * share] = low

            @pl.loop(0, pieces)
            def _(q):
                guest_part[r, :tall_of, wide(q)] = products(tall_of, q)

            for n, z in enumerate(away):
                back(j, k, z, r).start()

        if c == j:
            host_own(j, k)

    def relayed_in(j, k):
        for z in relayed(j, k):
            for r in range(rounds):
                landed(guest.at[z, few(r), :], guest_recv.at[z, r])
            high, low = halves(guest[z])
            help_stack[:height] = high
            help_stack[height:] = low

    def relayed_back(j, k, z, q):
        slot = part_from[j].index(k)
        here = guest.at[z] if q is None else guest.at[z, :, wide(q)]
        there_ref = here if q is None else part_in.at[slot, :, wide(q)]
        return remote(here, there_ref, relayed_send, part_recv.at[slot, 0 if q is None else q], level(z, j))

    def relayed_piece(j, k, q):
        for z in relayed(j, k):
            total = jnp.zeros((height, WIDE), jnp.float32)
            for half in range(side):
                total += nt3(help_stack[:, half * part : (half + 1) * part], stay[half, wide(q), :])
            guest[z, :, wide(q)] = total
            relayed_back(j, k, z, q).start()

    def host_own(j, k):
        c = host_of(j, k)
        if known(k):
            for q in range(pieces):
                vec_wait(vec_from[c].index(k), q)
            own = vec_in.at[vec_from[c].index(k)]
        else:
            for r in range(rounds):
                landed(guest.at[k, few(r), :], guest_recv.at[k, r])
            own = guest.at[k]
        high, low = halves(own[...])
        guest_stack[:height] = high
        guest_stack[height:] = low

        @pl.loop(0, pieces)
        def _(q):
            if c == j:
                part_in[part_from[j].index(k), :, wide(q)] = products(height, q)
            else:
                guest_part[rounds, :, wide(q)] = products(height, q)
                own_back(j, k, q).start()

    def make_part(c, block, q, left):
        slot, made = blocks[c].index(block), part_made[c].index(block)
        for n in range(WIDE // TALL):
            others(slot, block, q * (WIDE // TALL) + n)
        total = jnp.zeros((height, WIDE), jnp.float32)
        for half in range(side):
            total += nt3(left[:, half * part : (half + 1) * part], buf[slot, half, wide(q), :])
        part_out[made, :, wide(q)] = total
        part_to(block, made, q).start()

    per_half = part // WIDE

    def order(n):
        return lax.rem(n + jnp.where(a == 0, b * per_half, 0), pieces)

    def columns_of(o):
        return o // per_half, wide(lax.rem(o, per_half))

    def fold(slot):
        half, where = columns_of(order(pieces - 1))
        for n in range(pieces):
            upto = (n + 1) * WIDE
            high, low = halves(inverse[n * WIDE : upto, :upto])
            right, right_low = halves(buf[slot, half, :upto, where])
            total = jnp.dot(high, right, preferred_element_type=jnp.float32) + jnp.dot(low, right, preferred_element_type=jnp.float32)
            stay[0, n * WIDE : upto, :WIDE] = total + jnp.dot(high, right_low, preferred_element_type=jnp.float32)

    def folded(c):
        return [jk for jk in before[c] if both_down(jk)]

    def take_last(c):
        for block in folded(c):
            coming = vec_from[c].index(block[1])
            last = order(pieces - 1)
            vec_wait(coming, last)
            high, low = halves(vec_in[coming, :, wide(last)])
            stack[:height, :WIDE] = high
            stack[height:, :WIDE] = low
            total = jnp.zeros((8, height), jnp.float32)
            for n in range(pieces):
                done = vec[:, n * WIDE : (n + 1) * WIDE] - nt3(stack[:, :WIDE], stay[0, n * WIDE : (n + 1) * WIDE, :WIDE])
                vec[:, n * WIDE : (n + 1) * WIDE] = done
                high, low = halves(done * done)
                total += nt(ones[...], high) + nt(ones[...], low)
            sums[column] = total

    def take_before(c):
        for block in before[c]:
            j, k = block
            slot, coming = blocks[c].index(block), vec_from[c].index(k)
            if both_down(block):
                serving(c, early(columns - 3), lambda block: chunks)

                @pl.when((a <= k) & (a > 0))
                def _():
                    @pl.loop(0, chunks)
                    def _(i):
                        serve_others(slot, block, i)

                def others_in():
                    @pl.loop(0, chunks)
                    def _(i):
                        others(slot, block, i)

                pl.when(a > 0)(others_in)
                for jj, kk in staying:
                    if jj == c and host_of(jj, kk) != c:

                        @pl.when(a < kk)
                        def _():
                            for r in range(rounds):
                                landed(guest.at[a, few(r), :], guest_recv.at[a, r])
                                relay(jj, kk, r).start()

                for n in range(pieces - 1):
                    if n == per_half:
                        pl.when(a == 0)(others_in)
                        fold(slot)
                    o = order(n)
                    vec_wait(coming, o)
                    high, low = halves(vec_in[coming, :, wide(o)])
                    stack[:height, :WIDE] = high
                    stack[height:, :WIDE] = low
                    half, where = columns_of(o)

                    @pl.loop(0, pieces, unroll=2)
                    def _(m):
                        rest[:, wide(m)] -= nt3(stack[:, :WIDE], buf[slot, half, wide(m), where])
            elif j != c:
                serving(c, early(columns - 3), lambda block: chunks)
                for jj, kk in staying:
                    if host_of(jj, kk) == c:
                        pl.when(a == kk)(functools.partial(host, jj, kk))
                        pl.when(a == kk)(functools.partial(relayed_in, jj, kk))

                def work():
                    for q in range(pieces):
                        vec_wait(coming, q)

                pl.when(active(block) & (a != k) if c == heir[k] else active(block))(work)

                @pl.when(active(block))
                def _():
                    high, low = halves(vec_in[coming])
                    guest_stack[:height] = high
                    guest_stack[height:] = low

                pl.when(helping(block))(functools.partial(take_help, block))
            else:
                serving(c, early(columns - 3), early(columns - 2))
                for q in range(pieces):
                    vec_wait(coming, q)
                put(vec_in[coming])

                @pl.loop(0, pieces)
                def _(q):
                    @pl.when(a != k)
                    def _():
                        serve_ahead(slot, block, q, early(columns - 2)(block))

                    for u in range(columns):
                        for jj, kk in after[u]:
                            if kk == c:

                                @pl.when((a == kk) & (q == (chunks - EARLY[columns - 2] + 1) * TALL // WIDE + 1))
                                def _():
                                    pl.semaphore_signal(gate, inc=1, device_id=there(u), device_id_type=MESH)

                    for n in range(WIDE // TALL):
                        others(slot, block, q * (WIDE // TALL) + n)
                    total = jnp.zeros((height, WIDE), jnp.float32)
                    for half in range(side):
                        total += nt3(stack[:, half * part : (half + 1) * part], buf[slot, half, wide(q), :])
                    rest[:, wide(q)] -= total

    inverse_load.wait()
    for c in range(columns):
        if before[c]:
            on(c, functools.partial(take_before, c))

    squares = jnp.zeros((8, height), jnp.float32)
    for q in range(pieces):
        here = slice(q * WIDE, (q + 1) * WIDE)
        for c in range(columns):
            for block in before[c]:
                if block[0] != c:

                    def give(c=c, block=block):
                        @pl.when(active(block))
                        def _():
                            make_part(c, block, q, guest_stack)

                        @pl.when(helping(block))
                        def _():
                            help_piece(c, block, q)

                        for j, k in staying:
                            if relayed(j, k) and host_of(j, k) == c:
                                pl.when(a == k)(functools.partial(relayed_piece, j, k, q))

                    on(c, give)
            if part_from[c]:

                def work(c=c):
                    for slot, k in enumerate(part_from[c]):
                        if (c, k) not in staying:
                            part_wait(slot, q)
                        else:

                            def back_wait(slot=slot):
                                landed(part_in.at[slot], back_recv.at[slot])

                            if q == 0:
                                pl.when(a != k if host_of(c, k) == c else a > k)(back_wait)
                            if host_of(c, k) != c:
                                pl.when(a <= k)(functools.partial(part_wait, slot, q))

                        rest[:, here] -= part_in[slot, :, here]

                on(c, work)
        high, low = halves(rest[:, here])
        stack[:height, here] = high
        stack[height:, here] = low
        done = nt3(stack[:, : (q + 1) * WIDE], inverse[here, : (q + 1) * WIDE])
        vec[:, here] = done
        high, low = halves(done * done)
        squares += nt(ones[...], high) + nt(ones[...], low)
        for c in range(columns):
            if vec_to[c]:

                on(c, functools.partial(vec_outs, c, q, lambda copy: copy.start()))

    def guest_round(c, r):
        def work():
            if r:
                guest_out(c, r - 1).wait_send()
            if r < rounds:
                guest_out(c, r).start()

        if known(c) or not after[c]:
            pl.when(a != c)(work)
        else:
            work()

    def guests(c):
        for block in lift_to(c):

            @pl.when(jnp.logical_not(active(block)))
            def _():
                for r in range(rounds):
                    lift_out(block, r).start()

        if heir[c] is not None:
            if not known(c) and not after[c]:

                @pl.when(a == c)
                def _():
                    for r in range(rounds):
                        guest_out(c, r).start()
                    for r in range(rounds):
                        guest_out(c, r).wait_send()

            for r in range(1 if after[c] else rounds + 1):
                guest_round(c, r)

    for c in range(columns):
        on(c, functools.partial(guests, c))
    sums[column] = squares
    for c in range(columns):
        if folded(c):
            on(c, functools.partial(take_last, c))
    store = pltpu.make_async_copy(vec, out_ref, out_sem)
    store.start()

    def sum_out(step):
        to = (column + step) % columns
        return remote(sums.at[column], sums.at[column], sum_send.at[step - 1], sum_recv.at[column], there(to))

    for step in range(1, columns):
        sum_out(step).start()

    for j, k in staying:
        if host_of(j, k) != j:

            @pl.when((column == host_of(j, k)) & (a == k))
            def _():
                host_own(j, k)


    def give_after(c):
        for block in after[c]:
            j, k = block
            slot, coming = blocks[c].index(block), vec_from[c].index(k)

            if heir[c] is not None:
                for r in range(1, rounds + 1):
                    guest_round(c, r)

                    @pl.when(a == k)
                    def _():
                        if r == 1:
                            pl.semaphore_wait(gate, 1)

                    @pl.when(active(block))
                    def _():
                        @pl.loop(*[jnp.where(a == k, min(2 * n, LATER), n * LATER // rounds) for n in (r - 1, r)])
                        def _(i):
                            serve(slot, block, i)

            @pl.when(active(block))
            def _():
                for q in range(pieces):
                    vec_wait(coming, q)
                put(vec_in[coming])
                pl.when(helping(block))(functools.partial(take_help, block))

                @pl.loop(0, pieces)
                def _(q):
                    serve_ahead(slot, block, q, LATER)
                    make_part(c, block, q, stack)

                    @pl.when(helping(block))
                    def _():
                        help_piece(c, block, q)

    for c in range(columns):
        if after[c]:
            on(c, functools.partial(give_after, c))

    def sent(copy):
        copy.wait_send()

    for d in range(chips):
        slab_out(d).wait_send()
    for d in range(1, chips):
        slab_pass(d).wait_send()
    for j, k in all_blocks:
        t = target_of(j, k)
        if t is not None and t != j:

            @pl.when((column == j) & (a == k))
            def _():
                entry(blocks[t].index((j, k)), None, t).wait_send()

    for j, k in staying:
        c = host_of(j, k)

        @pl.when((column == j) & (a == k))
        def _():
            for step in range(0 if c != j else 1, side):
                stay_out(step, None, c).wait_send()

        if relayed(j, k):

            @pl.when((column == j) & (a < k))
            def _():
                relay(j, k, None).wait_send()

        @pl.when((column == c) & (a == k))
        def _():
            for z in visitors(j, k):
                if z in relayed(j, k):
                    relayed_back(j, k, z, None).wait_send()
                else:
                    back(j, k, z, None).wait_send()
            if c != j:
                own_back(j, k, None).wait_send()

    for c in range(columns):

        def work(c=c):
            for slot, block in enumerate(blocks[c]):
                line_flows(slot, block, None, sent)
                side_flows(slot, block, None, sent)
                if both_down(block):
                    other_flows(slot, block, None, sent)
            vec_outs(c, None, sent)
            for made, block in enumerate(part_made[c]):

                @pl.when(active(block))
                def _():
                    part_to(block, made, None).wait_send()

                @pl.when(helping(block))
                def _():
                    lift_back(block, None).wait_send()

            for block in lift_to(c):

                @pl.when(jnp.logical_not(active(block)))
                def _():
                    lift_out(block, None).wait_send()

        on(c, work)
    for step in range(1, columns):
        other = (column + step) % columns
        landed(sums.at[other], sum_recv.at[other])
    total = sums[0]
    for c in range(1, columns):
        total += sums[c]
    mean_ref[...] = total[:1] / (width * columns)
    for step in range(1, columns):
        sum_out(step).wait_send()
    store.wait()


def chain_device(slab, factor, block_inverse, pivot_order, row_count):
    height, width = slab.shape
    depth, part = factor.shape
    groups = lax.axis_size("cols")
    side = lax.axis_size("rows") // groups
    column = lax.axis_index("cols")
    slots = max([sum(target_of(j, k) == c for j in range(groups) for k in range(j)) for c in range(groups)])
    chunks, pieces, rounds, chips = depth // TALL, width // WIDE, groups - 1, groups // 2
    sem, space = pltpu.SemaphoreType.DMA, pltpu.VMEM
    f32, bf16 = jnp.float32, jnp.bfloat16
    held = pl.BlockSpec(memory_space=pltpu.VMEM)
    away = pl.BlockSpec(memory_space=pl.ANY)
    vectors, mean = pl.pallas_call(
        functools.partial(chain_kernel, groups, side),
        out_shape=(jax.ShapeDtypeStruct((height, width), f32), jax.ShapeDtypeStruct((1, height), f32)),
        in_specs=[away, away, away, held, pl.BlockSpec(memory_space=pltpu.SMEM)],
        out_specs=(away, held),
        scratch_shapes=[
            space((slots, side, depth, part), f32),
            space((width, width), f32),
            space((groups, height, width), f32),
            space((height, width), f32),
            space((height, width), f32),
            space((2 * height, width), bf16),
            space((1, height, width), f32),
            space((groups - 2, height, width), f32),
            space((1, height, width), f32),
            space((groups, 8, height), f32),
            space((8, WIDE), bf16),
            space((side, depth, part), f32),
            space((groups, height, width), f32),
            space((2 * height, width), bf16),
            space((rounds + 1, height, width), f32),
            space((2 * height, width), bf16),
            sem((chunks,)),
            sem((slots, side, chunks)),
            sem((slots,)),
            sem((slots, side)),
            sem((side - 1, slots)),
            sem(()),
            sem(()),
            sem(()),
            sem((chips,)),
            sem((groups,)),
            sem((chips - 1,)),
            sem((groups - 2,)),
            sem((1, pieces)),
            sem((1,)),
            sem((groups - 2, pieces)),
            sem((groups,)),
            sem((groups,)),
            sem(()),
            sem(()),
            sem((side,)),
            sem((side,)),
            sem((rounds,)),
            sem((groups, rounds)),
            sem((groups,)),
            sem((groups - 2,)),
            sem(()),
            sem(()),
            sem(()),
            sem(()),
            sem(()),
            pltpu.SemaphoreType.REGULAR,
        ],
        compiler_params=pltpu.CompilerParams(collective_id=0, has_side_effects=True, vmem_limit_bytes=57000 * 1024),
    )(slab, factor, block_inverse, pivot_order[None, :], row_count)
    return vectors, mean[0]


def per_device(slab, factor, block_inverse, pivot_order, row_count):
    groups, rows = lax.axis_size("cols"), lax.axis_size("rows")
    depth, part = factor.shape
    fits = groups // 2 == 2 and rows % groups == 0 and rows > groups and part % WIDE == 0 and depth % WIDE == 0 and slab.shape[0] % (8 * (groups - 1)) == 0
    one = chain_device if fits else plain_device
    return one(slab, factor, block_inverse, pivot_order, row_count)


def solution(mesh):
    placed = (P("rows", "cols"), P("cols", "rows"), P("cols", None), P(), P("rows"))
    return jax.shard_map(
        per_device,
        mesh=mesh,
        in_specs=placed,
        out_specs=(P("rows", "cols"), P("rows")),
        check_vma=False,
    )
```
